8 devices in a mesh: w: 2 (over z, y), h: 4 (over x, core).
Axes of the slice: x: 2, y: 2, z: 1, core: 2. Of those that a mesh axis runs over, the one named last changes fastest.
Arguments:
- x: bfloat16 [1, 64, 512, 640], P(None, 'h', 'w')
- w1: bfloat16 [3, 3, 640, 640], replicated
- gamma: float32 [640], replicated
- beta: float32 [640], replicated
- w2: bfloat16 [3, 3, 640, 640], replicated
- g: bfloat16 [1, 64, 512, 640], P(None, 'h', 'w')
Outputs:
- output 1: bfloat16 [1, 64, 512, 640], P(None, 'h', 'w')
- output 2: bfloat16 [1, 64, 512, 640], P(None, 'h', 'w')
- output 3: float32 [3, 3, 640, 640], replicated
- output 4: float32 [3, 3, 640, 640], replicated
- output 5: float32 [640], replicated
- output 6: float32 [640], replicated
All inputs are finite; a program needn't handle non-finite values.
Results may differ from the reference program's by a relative error of at most 0.00136865.
Values are sent between devices in bfloat16 or wider.
A program may use at most 1 GiB of HBM per device.

```python
import jax
import jax.numpy as jnp
from jax import lax

B = 1
C = 640
GROUPS = 32
TH = 16
TW = 256
HT = 4
WT = 2
HS = HT * TH
WS = WT * TW
DN = ('NHWC', 'HWIO', 'NHWC')


def setup_inputs(seed: int = 0) -> dict:
    ks = jax.random.split(jax.random.PRNGKey(seed), 6)
    rows = jnp.arange(HS)
    cols = jnp.arange(WS)
    xs = (0.5 + 1.5 * rows / HS)[None, :, None, None]
    x = (jax.random.normal(ks[0], (B, HS, WS, C), jnp.float32) * xs).astype(jnp.bfloat16)
    std = (9 * C) ** -0.5
    w1 = (jax.random.normal(ks[1], (3, 3, C, C), jnp.float32) * std).astype(jnp.bfloat16)
    gamma = 1.0 + 0.3 * jax.random.normal(ks[2], (C,), jnp.float32)
    beta = 0.3 * jax.random.normal(ks[3], (C,), jnp.float32)
    w2 = (jax.random.normal(ks[4], (3, 3, C, C), jnp.float32) * std).astype(jnp.bfloat16)
    edge = ((rows % TH == 0) | (rows % TH == TH - 1))[:, None] | ((cols % TW == 0) | (cols % TW == TW - 1))[None, :]
    gs = jnp.where(edge, 3.0, 1.0)[None, :, :, None]
    g = (jax.random.normal(ks[5], (B, HS, WS, C), jnp.float32) * gs).astype(jnp.bfloat16)
    return {'x': x, 'w1': w1, 'gamma': gamma, 'beta': beta, 'w2': w2, 'g': g}


def _conv(u, w):
    return lax.conv_general_dilated(u.astype(jnp.float32), w.astype(jnp.float32), (1, 1), 'SAME', dimension_numbers=DN)


def _conv_t(v, w):
    return _conv(v, jnp.flip(w, (0, 1)).transpose(0, 1, 3, 2))


def _wgrad(u, v):
    up = jnp.pad(u.astype(jnp.float32), ((0, 0), (1, 1), (1, 1), (0, 0)))
    v32 = v.astype(jnp.float32)
    h, w = v.shape[1], v.shape[2]
    return jnp.stack([jnp.stack([jnp.einsum('bhwc,bhwo->co', up[:, a:a + h, b:b + w], v32) for b in range(3)]) for a in range(3)])


def _norm_act(a, gamma, beta):
    nb, h, w, c = a.shape
    ag = a.reshape(nb, h, w, GROUPS, c // GROUPS)
    mean = ag.mean(axis=(1, 2, 4), keepdims=True)
    var = ((ag - mean) ** 2).mean(axis=(1, 2, 4), keepdims=True)
    n = ((ag - mean) * lax.rsqrt(var + 1e-5)).reshape(a.shape) * gamma + beta
    return jax.nn.gelu(n, approximate=True)


def reference(x, w1, gamma, beta, w2, g):
    a = _conv(x, w1).astype(jnp.bfloat16).astype(jnp.float32)
    zf, vjp = jax.vjp(_norm_act, a, gamma, beta)
    z = zf.astype(jnp.bfloat16)
    y = (_conv(z, w2) + x.astype(jnp.float32)).astype(jnp.bfloat16)
    dz = _conv_t(g, w2)
    dw2 = _wgrad(z, g)
    da, dgamma, dbeta = vjp(dz)
    da = da.astype(jnp.bfloat16)
    dx = (_conv_t(da, w1) + g.astype(jnp.float32)).astype(jnp.bfloat16)
    dw1 = _wgrad(x, da)
    return y, dx, dw1, dw2, dgamma, dbeta
```

```python
import functools

import jax
import jax.numpy as jnp
from jax import lax
from jax.experimental import pallas as pl
from jax.experimental.pallas import tpu as pltpu
from jax.sharding import Mesh
from jax.sharding import PartitionSpec as P


GROUPS = 32
EPS = 1e-5
F32 = jnp.float32
BF16 = jnp.bfloat16
MESH = pl.DeviceIdType.MESH
EB = 16
VMEM_LIMIT = 61 * 1024 * 1024
ANY = pl.BlockSpec(memory_space=pl.ANY)
VM = pl.BlockSpec(memory_space=pltpu.VMEM)
GELU_C = 0.7978845608028654
GELU_A = 0.044715


def _gelu_parts(n):
    n2 = n * n
    t = jnp.tanh(GELU_C * (n + GELU_A * n * n2))
    return n2, t


def _gelu(n):
    _, t = _gelu_parts(n)
    return 0.5 * n * (1.0 + t)


def _gelu_grad(n):
    n2, t = _gelu_parts(n)
    return 0.5 * (1.0 + t) + 0.5 * n * (1.0 - t * t) * (GELU_C * (1.0 + 3.0 * GELU_A * n2))


def _halo_kernel(nh, nw, n_arr, *refs):
    ins = refs[:n_arr]
    outs = refs[n_arr:4 * n_arr]
    send, recv = refs[4 * n_arr:]
    th, tw, c = ins[0].shape
    w = lax.axis_index("w")
    h = lax.axis_index("x") * 2 + lax.axis_index("c")

    def dev(dh, dw):
        hh = h + dh
        return (w + dw, hh // 2, hh % 2)

    def has(dh, dw):
        ok = None
        for cond in ([h > 0] if dh < 0 else [h < nh - 1] if dh > 0 else []) + ([w > 0] if dw < 0 else [w < nw - 1] if dw > 0 else []):
            ok = cond if ok is None else jnp.logical_and(ok, cond)
        return ok

    dirs = [(dh, dw) for dh in (-1, 0, 1) for dw in (-1, 0, 1) if (dh, dw) != (0, 0)]
    barrier = pltpu.get_barrier_semaphore()
    for d in dirs:
        @pl.when(has(*d))
        def _(d=d):
            pl.semaphore_signal(barrier, inc=1, device_id=dev(*d), device_id_type=MESH)
    one = jnp.int32(1)
    zero = jnp.int32(0)
    nv = one + jnp.where(h > 0, one, zero) + jnp.where(h < nh - 1, one, zero)
    nz = one + jnp.where(w > 0, one, zero) + jnp.where(w < nw - 1, one, zero)
    pl.semaphore_wait(barrier, nv * nz - 1)

    def parts(k, dh, dw):
        u = ins[k]
        rows, cl, cr = outs[3 * k:3 * k + 3]
        r = 0 if dh < 0 else th - 1
        to = 1 if dh < 0 else 0
        to18 = th + 1 if dh < 0 else 0
        cs = slice(0, EB) if dw < 0 else slice(tw - EB, tw)
        side = cr if dw < 0 else cl
        if dw == 0:
            return u.at[r], rows.at[to]
        if dh == 0:
            return u.at[:, cs, :], side.at[1:th + 1]
        return u.at[r, cs, :], side.at[to18]

    def copy(k, i, dh, dw):
        src, dst = parts(k, dh, dw)
        return pltpu.make_async_remote_copy(src_ref=src, dst_ref=dst, send_sem=send.at[k * 8 + i], recv_sem=recv.at[k * 8 + i],
                                            device_id=dev(dh, dw), device_id_type=MESH)

    for k in range(n_arr):
        for i, d in enumerate(dirs):
            @pl.when(has(*d))
            def _(k=k, i=i, d=d):
                copy(k, i, *d).start()
    for k in range(n_arr):
        rows, cl, cr = outs[3 * k:3 * k + 3]
        for dh, dw in dirs:
            @pl.when(jnp.logical_not(has(-dh, -dw)))
            def _(rows=rows, cl=cl, cr=cr, dh=dh, dw=dw):
                to = 1 if dh < 0 else 0
                to18 = th + 1 if dh < 0 else 0
                side = cr if dw < 0 else cl
                if dw == 0:
                    rows[to] = jnp.zeros((tw, c), BF16)
                elif dh == 0:
                    side[1:th + 1] = jnp.zeros((th, EB, c), BF16)
                else:
                    side[to18] = jnp.zeros((EB, c), BF16)
    for k in range(n_arr):
        for i, (dh, dw) in enumerate(dirs):
            @pl.when(has(dh, dw))
            def _(k=k, i=i, dh=dh, dw=dw):
                copy(k, i, dh, dw).wait_send()

            @pl.when(has(-dh, -dw))
            def _(k=k, i=i, dh=dh, dw=dw):
                copy(k, i, dh, dw).wait_recv()


def _halo(nh, nw, cid, *us):
    th, tw, c = us[0].shape
    n = len(us)
    out = []
    for _ in us:
        out += [jax.ShapeDtypeStruct((2, tw, c), BF16), jax.ShapeDtypeStruct((th + 2, EB, c), BF16), jax.ShapeDtypeStruct((th + 2, EB, c), BF16)]
    res = pl.pallas_call(
        functools.partial(_halo_kernel, nh, nw, n), out_shape=out, in_specs=[ANY] * n, out_specs=[VM] * (3 * n),
        scratch_shapes=[pltpu.SemaphoreType.DMA((8 * n,)), pltpu.SemaphoreType.DMA((8 * n,))],
        compiler_params=pltpu.CompilerParams(collective_id=cid, has_side_effects=True, vmem_limit_bytes=VMEM_LIMIT),
    )(*us)
    return [tuple(res[3 * k:3 * k + 3]) for k in range(n)]


def _allsum_kernel(nh, nw, cnt, mode, part_ref, par_ref, out_ref, mine, buf, lsem, send, recv):
    n = nh * nw
    w = lax.axis_index("w")
    h = lax.axis_index("x") * 2 + lax.axis_index("c")
    me = w * nh + h

    def dev(j):
        hh = j % nh
        return (j // nh, hh // 2, hh % 2)

    local = pltpu.make_async_copy(part_ref, mine, lsem)
    local.start()
    barrier = pltpu.get_barrier_semaphore()
    for k in range(1, n):
        pl.semaphore_signal(barrier, inc=1, device_id=dev(lax.rem(me + k, n)), device_id_type=MESH)
    local.wait()
    pl.semaphore_wait(barrier, n - 1)
    copies = []
    for k in range(1, n):
        cp = pltpu.make_async_remote_copy(src_ref=mine, dst_ref=buf.at[k - 1], send_sem=send.at[k - 1], recv_sem=recv.at[k - 1],
                                          device_id=dev(lax.rem(me + k, n)), device_id_type=MESH)
        cp.start()
        copies.append(cp)
    for cp in copies:
        cp.wait()
    total = None
    vals = [mine[...]] + [buf[k] for k in range(n - 1)]
    for j in range(n):
        t = jnp.zeros_like(vals[0])
        off = lax.rem(me - j + n, n)
        for k in range(n):
            t = t + jnp.where(off == k, vals[k], 0.0)
        total = t if total is None else total + t
    c = total.shape[-1]
    gi = jnp.floor((lax.broadcasted_iota(jnp.int32, (c, c), 0).astype(F32) + 0.5) * (GROUPS / c))
    gj = jnp.floor((lax.broadcasted_iota(jnp.int32, (c, c), 1).astype(F32) + 0.5) * (GROUPS / c))
    same = jnp.where(gi == gj, 1.0, 0.0).astype(F32)
    row = lax.broadcasted_iota(jnp.int32, (8, c), 0)
    if mode == 0:
        m = jnp.dot(total, same, precision=lax.Precision.HIGHEST, preferred_element_type=F32) / cnt
        mean, sq = m[0:1], m[1:2]
        rstd = lax.rsqrt(sq - mean * mean + EPS)
        out_ref[...] = jnp.where(row == 0, mean, jnp.where(row == 1, rstd, par_ref[...]))
    else:
        u = jnp.dot(total * par_ref[2:3], same, precision=lax.Precision.HIGHEST, preferred_element_type=F32) / cnt
        out_ref[...] = jnp.where(row == 0, total[0:1], jnp.where(row == 1, total[1:2], jnp.where(row == 2, u[0:1], u[1:2])))


def _allsum(nh, nw, cnt, mode, cid, part, par):
    c = part.shape[-1]
    n = nh * nw
    return pl.pallas_call(
        functools.partial(_allsum_kernel, nh, nw, cnt, mode), out_shape=jax.ShapeDtypeStruct((8, c), F32),
        in_specs=[ANY, VM], out_specs=VM,
        scratch_shapes=[pltpu.VMEM((8, c), F32), pltpu.VMEM((n - 1, 8, c), F32), pltpu.SemaphoreType.DMA,
                        pltpu.SemaphoreType.DMA((n - 1,)), pltpu.SemaphoreType.DMA((n - 1,))],
        compiler_params=pltpu.CompilerParams(collective_id=cid, has_side_effects=True, vmem_limit_bytes=VMEM_LIMIT),
    )(part, par)


def _load_patches(u_ref, rows_ref, p, sems):
    th, c = u_ref.shape[0], u_ref.shape[2]
    cps = [pltpu.make_async_copy(u_ref, p.at[1:th + 1, :, c:2 * c], sems.at[0]),
           pltpu.make_async_copy(rows_ref.at[0], p.at[0, :, c:2 * c], sems.at[1]),
           pltpu.make_async_copy(rows_ref.at[1], p.at[th + 1, :, c:2 * c], sems.at[2])]
    for cp in cps:
        cp.start()
    return cps


def _shift_patches(p, cl_ref, cr_ref):
    n, tw, c3 = p.shape
    c = c3 // 3
    ck = 128

    def row(r, _):
        idx = lax.broadcasted_iota(jnp.int32, (tw, ck), 0)
        for k in range(c // ck):
            f = p[r, :, c + k * ck:c + (k + 1) * ck].astype(F32)
            lo = cl_ref[r, :, k * ck:(k + 1) * ck].astype(F32)[EB - 1:EB]
            hi = cr_ref[r, :, k * ck:(k + 1) * ck].astype(F32)[0:1]
            p[r, :, k * ck:(k + 1) * ck] = jnp.where(idx == 0, lo, pltpu.roll(f, 1, 0)).astype(BF16)
            p[r, :, 2 * c + k * ck:2 * c + (k + 1) * ck] = jnp.where(idx == tw - 1, hi, pltpu.roll(f, tw - 1, 0)).astype(BF16)
        return 0

    lax.fori_loop(0, n, row, 0)


def _conv_kernel(transposed, rb, n_extra, epilogue, u_ref, rows_ref, cl_ref, cr_ref, w_ref, *refs):
    extra = refs[:n_extra]
    outs = refs[n_extra:-4]
    p, wb, psem, wsem = refs[-4:]
    c = u_ref.shape[2]
    i = pl.program_id(0)

    @pl.when(i == 0)
    def _():
        cps = _load_patches(u_ref, rows_ref, p, psem)
        ws = []
        for a in range(3):
            for b in range(3):
                if transposed:
                    ws.append(pltpu.make_async_copy(w_ref.at[2 - a, 2 - b], wb.at[a, :, b * c:(b + 1) * c], wsem.at[a * 3 + b]))
                else:
                    ws.append(pltpu.make_async_copy(w_ref.at[a, b], wb.at[a, b * c:(b + 1) * c, :], wsem.at[a * 3 + b]))
        for cp in ws:
            cp.start()
        for cp in cps:
            cp.wait()
        _shift_patches(p, cl_ref, cr_ref)
        for cp in ws:
            cp.wait()

    tw = p.shape[1]
    acc = None
    for a in range(3):
        lhs = p[pl.ds(i * rb + a, rb)].reshape(rb * tw, 3 * c)
        dims = (((1,), (1,)), ((), ())) if transposed else (((1,), (0,)), ((), ()))
        d = lax.dot_general(lhs, wb[a], dims, preferred_element_type=F32)
        acc = d if acc is None else acc + d
    epilogue(i, acc, extra, outs)


def _conv(transposed, epilogue, u, halo, w, extra, extra_specs, outs, out_specs, rb=2):
    th, tw, c = u.shape
    full = pl.BlockSpec((th + 2, EB, c), lambda i: (0, 0, 0), pipeline_mode=pl.Buffered(1))
    return pl.pallas_call(
        functools.partial(_conv_kernel, transposed, rb, len(extra), epilogue),
        grid=(th // rb,), out_shape=outs, in_specs=[ANY, ANY, full, full, ANY] + extra_specs, out_specs=out_specs,
        scratch_shapes=[pltpu.VMEM((th + 2, tw, 3 * c), BF16), pltpu.VMEM((3, c, 3 * c) if transposed else (3, 3 * c, c), BF16),
                        pltpu.SemaphoreType.DMA((3,)), pltpu.SemaphoreType.DMA((9,))],
        compiler_params=pltpu.CompilerParams(dimension_semantics=("arbitrary",), vmem_limit_bytes=VMEM_LIMIT),
        cost_estimate=pl.CostEstimate(flops=2 * 9 * th * tw * c * c, bytes_accessed=4 * th * tw * c + 18 * c * c, transcendentals=0),
    )(u, *halo, w, *extra)


def _ep_conv1(i, acc, extra, outs):
    a_ref, s_ref = outs
    a16 = acc.astype(BF16)
    a_ref[...] = a16.reshape(a_ref.shape)
    a = a16.astype(F32)
    s0 = a.sum(0, keepdims=True)
    s1 = (a * a).sum(0, keepdims=True)
    row = lax.broadcasted_iota(jnp.int32, s_ref.shape, 0)
    s = jnp.where(row == 0, s0, jnp.where(row == 1, s1, 0.0))

    @pl.when(i == 0)
    def _():
        s_ref[...] = s

    @pl.when(i > 0)
    def _():
        s_ref[...] += s


def _ep_residual(i, acc, extra, outs):
    o_ref = outs[0]
    r = extra[0][...].astype(F32).reshape(acc.shape)
    o_ref[...] = (acc + r).astype(BF16).reshape(o_ref.shape)


def _ep_dz(i, acc, extra, outs):
    a_ref, st_ref = extra
    dn_ref, s_ref = outs
    st = st_ref[...]
    xhat = (a_ref[...].astype(F32).reshape(acc.shape) - st[0:1]) * st[1:2]
    dn = acc * _gelu_grad(xhat * st[2:3] + st[3:4])
    dn_ref[...] = dn.reshape(dn_ref.shape)
    s0 = (dn * xhat).sum(0, keepdims=True)
    s1 = dn.sum(0, keepdims=True)
    row = lax.broadcasted_iota(jnp.int32, s_ref.shape, 0)
    s = jnp.where(row == 0, s0, jnp.where(row == 1, s1, 0.0))

    @pl.when(i == 0)
    def _():
        s_ref[...] = s

    @pl.when(i > 0)
    def _():
        s_ref[...] += s


def _z_kernel(a_ref, st_ref, z_ref):
    st = st_ref[...]
    xhat = (a_ref[...].astype(F32) - st[0:1]) * st[1:2]
    z_ref[...] = _gelu(xhat * st[2:3] + st[3:4]).astype(BF16)


def _da_kernel(dn_ref, a_ref, st_ref, t_ref, o_ref):
    st = st_ref[...]
    t = t_ref[...]
    xhat = (a_ref[...].astype(F32) - st[0:1]) * st[1:2]
    o_ref[...] = (st[1:2] * (dn_ref[...] * st[2:3] - t[3:4] - xhat * t[2:3])).astype(BF16)


def _wgrad_kernel(u_ref, rows_ref, cl_ref, cr_ref, v_ref, o_ref, p, vt, psem):
    a = pl.program_id(0)
    th, tw, c = v_ref.shape

    @pl.when(a == 0)
    def _():
        cps = _load_patches(u_ref, rows_ref, p, psem)

        def tr(r, _):
            vt[:, pl.ds(pl.multiple_of(r * tw, tw), tw)] = v_ref[r].T
            return 0

        lax.fori_loop(0, th, tr, 0)
        for cp in cps:
            cp.wait()
        _shift_patches(p, cl_ref, cr_ref)

    n = 3 * c
    k = 0
    while k < n:
        m = min(512, n - k)
        rhs = p[pl.ds(a, th), :, k:k + m].reshape(th * tw, m)
        d = jnp.dot(vt[...], rhs, preferred_element_type=F32)
        o_ref[0, k:k + m, :] = d.T
        k += m


def _wgrad(u, halo, v):
    th, tw, c = u.shape
    full = pl.BlockSpec((th + 2, EB, c), lambda i: (0, 0, 0), pipeline_mode=pl.Buffered(1))
    fv = pl.BlockSpec((th, tw, c), lambda i: (0, 0, 0), pipeline_mode=pl.Buffered(1))
    return pl.pallas_call(
        _wgrad_kernel, grid=(3,), out_shape=jax.ShapeDtypeStruct((3, 3 * c, c), F32),
        in_specs=[ANY, ANY, full, full, fv], out_specs=pl.BlockSpec((1, 3 * c, c), lambda a: (a, 0, 0)),
        scratch_shapes=[pltpu.VMEM((th + 2, tw, 3 * c), BF16), pltpu.VMEM((c, th * tw), BF16), pltpu.SemaphoreType.DMA((3,))],
        compiler_params=pltpu.CompilerParams(dimension_semantics=("arbitrary",), vmem_limit_bytes=VMEM_LIMIT),
        cost_estimate=pl.CostEstimate(flops=2 * 9 * th * tw * c * c, bytes_accessed=4 * th * tw * c + 36 * c * c, transcendentals=0),
    )(u, *halo, v)


def _reduce_all(d):
    r, k, c = d.shape
    s = lax.psum_scatter(d.reshape(r * k, c), ("c", "w", "x"), scatter_dimension=0, tiled=True)
    s = lax.all_gather(s, ("w", "x"), axis=0, tiled=True)
    return lax.all_gather(s, "c", axis=0, tiled=True).reshape(3, 3, c, c)


def solution(mesh):
    nh, nw = mesh.shape["h"], mesh.shape["w"]
    mesh3 = Mesh(mesh.devices.reshape(nw, nh // 2, 2), ("w", "x", "c"))
    tile = P(None, ("x", "c"), "w", None)

    def body(x, w1, gamma, beta, w2, g):
        _, th, tw, c = x.shape
        x, g = x[0], g[0]
        cnt = float(th * nh * tw * nw * (c // GROUPS))
        rb = 2
        blk = pl.BlockSpec((rb, tw, c), lambda i: (i, 0, 0))
        small = pl.BlockSpec((8, c), lambda i: (0, 0))
        img16 = jax.ShapeDtypeStruct((th, tw, c), BF16)
        img32 = jax.ShapeDtypeStruct((th, tw, c), F32)
        sums = jax.ShapeDtypeStruct((8, c), F32)
        par = jnp.concatenate([jnp.zeros((2, c), F32), gamma[None], beta[None], jnp.zeros((4, c), F32)])

        xh, gh = _halo(nh, nw, 0, x, g)
        a, s = _conv(False, _ep_conv1, x, xh, w1, [], [], [img16, sums], [blk, small])
        st = _allsum(nh, nw, cnt, 0, 1, s, par)
        z = pl.pallas_call(_z_kernel, grid=(th // rb,), out_shape=img16, in_specs=[blk, small], out_specs=blk, name="act")(a, st)
        (zh,) = _halo(nh, nw, 2, z)
        d2 = _wgrad(z, zh, g)
        g_late, d2 = lax.optimization_barrier((g, d2))
        dw2 = _reduce_all(d2)
        dn, t = _conv(True, _ep_dz, g_late, gh, w2, [a, st], [blk, small], [img32, sums], [blk, small])
        t = _allsum(nh, nw, cnt, 1, 3, t, st)
        da = pl.pallas_call(_da_kernel, grid=(th // rb,), out_shape=img16, in_specs=[blk, blk, small, small], out_specs=blk, name="da")(dn, a, st, t)
        (dah,) = _halo(nh, nw, 4, da)
        d1 = _wgrad(x, xh, da)
        z_late, da_late, d1 = lax.optimization_barrier((z, da, d1))
        dw1 = _reduce_all(d1)
        (y,) = _conv(False, _ep_residual, z_late, zh, w2, [x], [blk], [img16], [blk])
        (dx,) = _conv(True, _ep_residual, da_late, dah, w1, [g], [blk], [img16], [blk])
        return y[None], dx[None], dw1, dw2, t[0], t[1]

    return jax.shard_map(body, mesh=mesh3, in_specs=(tile, P(), P(), P(), P(), tile), out_specs=(tile, tile, P(), P(), P(), P()), check_vma=False)
```

```python
import functools

import jax
import jax.numpy as jnp
from jax import lax
from jax.experimental import pallas as pl
from jax.experimental.pallas import tpu as pltpu
from jax.sharding import Mesh
from jax.sharding import PartitionSpec as P


GROUPS = 32
EPS = 1e-5
F32 = jnp.float32
BF16 = jnp.bfloat16
MESH = pl.DeviceIdType.MESH
VMEM_LIMIT = 61 * 1024 * 1024
ANY = pl.BlockSpec(memory_space=pl.ANY)
VM = pl.BlockSpec(memory_space=pltpu.VMEM)
GELU_C = 0.7978845608028654
GELU_A = 0.044715


def _gelu_parts(n):
    n2 = n * n
    t = jnp.tanh(GELU_C * (n + GELU_A * n * n2))
    return n2, t


def _gelu(n):
    _, t = _gelu_parts(n)
    return 0.5 * n * (1.0 + t)


def _gelu_grad(n):
    n2, t = _gelu_parts(n)
    return 0.5 * (1.0 + t) + 0.5 * n * (1.0 - t * t) * (GELU_C * (1.0 + 3.0 * GELU_A * n2))


def _halo_kernel(nh, nw, n_arr, *refs):
    ins = refs[:3 * n_arr]
    outs = refs[3 * n_arr:6 * n_arr]
    send, recv = refs[6 * n_arr:]
    th, tw, c = ins[0].shape
    w = lax.axis_index("w")
    h = lax.axis_index("x") * 2 + lax.axis_index("c")

    def dev(dh, dw):
        hh = h + dh
        return (w + dw, hh // 2, hh % 2)

    def has(dh, dw):
        ok = None
        for cond in ([h > 0] if dh < 0 else [h < nh - 1] if dh > 0 else []) + ([w > 0] if dw < 0 else [w < nw - 1] if dw > 0 else []):
            ok = cond if ok is None else jnp.logical_and(ok, cond)
        return ok

    dirs = [(dh, dw) for dh in (-1, 0, 1) for dw in (-1, 0, 1) if (dh, dw) != (0, 0)]
    barrier = pltpu.get_barrier_semaphore()
    for d in dirs:
        @pl.when(has(*d))
        def _(d=d):
            pl.semaphore_signal(barrier, inc=1, device_id=dev(*d), device_id_type=MESH)
    one = jnp.int32(1)
    zero = jnp.int32(0)
    nv = one + jnp.where(h > 0, one, zero) + jnp.where(h < nh - 1, one, zero)
    nz = one + jnp.where(w > 0, one, zero) + jnp.where(w < nw - 1, one, zero)
    pl.semaphore_wait(barrier, nv * nz - 1)

    def parts(k, dh, dw):
        u, first, last = ins[3 * k:3 * k + 3]
        rows, cl, cr = outs[3 * k:3 * k + 3]
        r = 0 if dh < 0 else th - 1
        to = 1 if dh < 0 else 0
        to18 = th + 1 if dh < 0 else 0
        edge, side = (first, cr) if dw < 0 else (last, cl)
        if dw == 0:
            return u.at[r], rows.at[to]
        if dh == 0:
            return edge, side.at[1:th + 1]
        return edge.at[r], side.at[to18]

    def copy(k, i, dh, dw):
        src, dst = parts(k, dh, dw)
        return pltpu.make_async_remote_copy(src_ref=src, dst_ref=dst, send_sem=send.at[k * 8 + i], recv_sem=recv.at[k * 8 + i],
                                            device_id=dev(dh, dw), device_id_type=MESH)

    for k in range(n_arr):
        for i, d in enumerate(dirs):
            @pl.when(has(*d))
            def _(k=k, i=i, d=d):
                copy(k, i, *d).start()
    for k in range(n_arr):
        rows, cl, cr = outs[3 * k:3 * k + 3]
        for dh, dw in dirs:
            @pl.when(jnp.logical_not(has(-dh, -dw)))
            def _(rows=rows, cl=cl, cr=cr, dh=dh, dw=dw):
                to = 1 if dh < 0 else 0
                to18 = th + 1 if dh < 0 else 0
                side = cr if dw < 0 else cl
                if dw == 0:
                    rows[to] = jnp.zeros((tw, c), BF16)
                elif dh == 0:
                    side[1:th + 1] = jnp.zeros((th, 1, c), F32)
                else:
                    side[to18] = jnp.zeros((1, c), F32)
    for k in range(n_arr):
        for i, (dh, dw) in enumerate(dirs):
            @pl.when(has(dh, dw))
            def _(k=k, i=i, dh=dh, dw=dw):
                copy(k, i, dh, dw).wait_send()

            @pl.when(has(-dh, -dw))
            def _(k=k, i=i, dh=dh, dw=dw):
                copy(k, i, dh, dw).wait_recv()


def _halo(nh, nw, cid, *us):
    th, tw, c = us[0].shape
    n = len(us) // 3
    out = []
    for _ in range(n):
        out += [jax.ShapeDtypeStruct((2, tw, c), BF16), jax.ShapeDtypeStruct((th + 2, 1, c), F32), jax.ShapeDtypeStruct((th + 2, 1, c), F32)]
    res = pl.pallas_call(
        functools.partial(_halo_kernel, nh, nw, n), out_shape=out, in_specs=[ANY] * (3 * n), out_specs=[VM] * (3 * n),
        scratch_shapes=[pltpu.SemaphoreType.DMA((8 * n,)), pltpu.SemaphoreType.DMA((8 * n,))],
        compiler_params=pltpu.CompilerParams(collective_id=cid, has_side_effects=True, vmem_limit_bytes=VMEM_LIMIT),
    )(*us)
    return [tuple(res[3 * k:3 * k + 3]) for k in range(n)]


def _allsum_kernel(nh, nw, cnt, mode, part_ref, par_ref, out_ref, mine, buf, lsem, send, recv):
    n = nh * nw
    w = lax.axis_index("w")
    h = lax.axis_index("x") * 2 + lax.axis_index("c")
    me = w * nh + h

    def dev(j):
        hh = j % nh
        return (j // nh, hh // 2, hh % 2)

    local = pltpu.make_async_copy(part_ref, mine, lsem)
    local.start()
    barrier = pltpu.get_barrier_semaphore()
    for k in range(1, n):
        pl.semaphore_signal(barrier, inc=1, device_id=dev(lax.rem(me + k, n)), device_id_type=MESH)
    local.wait()
    pl.semaphore_wait(barrier, n - 1)
    copies = []
    for k in range(1, n):
        cp = pltpu.make_async_remote_copy(src_ref=mine, dst_ref=buf.at[k - 1], send_sem=send.at[k - 1], recv_sem=recv.at[k - 1],
                                          device_id=dev(lax.rem(me + k, n)), device_id_type=MESH)
        cp.start()
        copies.append(cp)
    for cp in copies:
        cp.wait()
    total = None
    vals = [mine[...]] + [buf[k] for k in range(n - 1)]
    for j in range(n):
        t = jnp.zeros_like(vals[0])
        off = lax.rem(me - j + n, n)
        for k in range(n):
            t = t + jnp.where(off == k, vals[k], 0.0)
        total = t if total is None else total + t
    c = total.shape[-1]
    gi = jnp.floor((lax.broadcasted_iota(jnp.int32, (c, c), 0).astype(F32) + 0.5) * (GROUPS / c))
    gj = jnp.floor((lax.broadcasted_iota(jnp.int32, (c, c), 1).astype(F32) + 0.5) * (GROUPS / c))
    same = jnp.where(gi == gj, 1.0, 0.0).astype(F32)
    row = lax.broadcasted_iota(jnp.int32, (8, c), 0)
    if mode == 0:
        m = jnp.dot(total, same, precision=lax.Precision.HIGHEST, preferred_element_type=F32) / cnt
        mean, sq = m[0:1], m[1:2]
        rstd = lax.rsqrt(sq - mean * mean + EPS)
        out_ref[...] = jnp.where(row == 0, mean, jnp.where(row == 1, rstd, par_ref[...]))
    else:
        u = jnp.dot(total * par_ref[2:3], same, precision=lax.Precision.HIGHEST, preferred_element_type=F32) / cnt
        out_ref[...] = jnp.where(row == 0, total[0:1], jnp.where(row == 1, total[1:2], jnp.where(row == 2, u[0:1], u[1:2])))


def _allsum(nh, nw, cnt, mode, cid, part, par):
    c = part.shape[-1]
    n = nh * nw
    return pl.pallas_call(
        functools.partial(_allsum_kernel, nh, nw, cnt, mode), out_shape=jax.ShapeDtypeStruct((8, c), F32),
        in_specs=[ANY, VM], out_specs=VM,
        scratch_shapes=[pltpu.VMEM((8, c), F32), pltpu.VMEM((n - 1, 8, c), F32), pltpu.SemaphoreType.DMA,
                        pltpu.SemaphoreType.DMA((n - 1,)), pltpu.SemaphoreType.DMA((n - 1,))],
        compiler_params=pltpu.CompilerParams(collective_id=cid, has_side_effects=True, vmem_limit_bytes=VMEM_LIMIT),
    )(part, par)


def _load_patches(u_ref, rows_ref, p, sems):
    th, c = u_ref.shape[0], u_ref.shape[2]
    cps = [pltpu.make_async_copy(u_ref, p.at[1:th + 1, :, c:2 * c], sems.at[0]),
           pltpu.make_async_copy(rows_ref.at[0], p.at[0, :, c:2 * c], sems.at[1]),
           pltpu.make_async_copy(rows_ref.at[1], p.at[th + 1, :, c:2 * c], sems.at[2])]
    for cp in cps:
        cp.start()
    return cps


def _shift_patches(p, cl_ref, cr_ref):
    n, tw, c3 = p.shape
    c = c3 // 3
    ck = 128

    def row(r, _):
        idx = lax.broadcasted_iota(jnp.int32, (tw, ck), 0)
        for k in range(c // ck):
            f = p[r, :, c + k * ck:c + (k + 1) * ck].astype(F32)
            lo = cl_ref[r, :, k * ck:(k + 1) * ck]
            hi = cr_ref[r, :, k * ck:(k + 1) * ck]
            p[r, :, k * ck:(k + 1) * ck] = jnp.where(idx == 0, lo, pltpu.roll(f, 1, 0)).astype(BF16)
            p[r, :, 2 * c + k * ck:2 * c + (k + 1) * ck] = jnp.where(idx == tw - 1, hi, pltpu.roll(f, tw - 1, 0)).astype(BF16)
        return 0

    lax.fori_loop(0, n, row, 0)


def _conv_kernel(transposed, rb, n_extra, epilogue, u_ref, rows_ref, cl_ref, cr_ref, w_ref, *refs):
    extra = refs[:n_extra]
    outs = refs[n_extra:-4]
    p, wb, psem, wsem = refs[-4:]
    c = u_ref.shape[2]
    i = pl.program_id(0)

    @pl.when(i == 0)
    def _():
        cps = _load_patches(u_ref, rows_ref, p, psem)
        ws = []
        for a in range(3):
            for b in range(3):
                if transposed:
                    ws.append(pltpu.make_async_copy(w_ref.at[2 - a, 2 - b], wb.at[a, :, b * c:(b + 1) * c], wsem.at[a * 3 + b]))
                else:
                    ws.append(pltpu.make_async_copy(w_ref.at[a, b], wb.at[a, b * c:(b + 1) * c, :], wsem.at[a * 3 + b]))
        for cp in ws:
            cp.start()
        for cp in cps:
            cp.wait()
        _shift_patches(p, cl_ref, cr_ref)
        for cp in ws:
            cp.wait()

    tw = p.shape[1]
    acc = None
    for a in range(3):
        lhs = p[pl.ds(i * rb + a, rb)].reshape(rb * tw, 3 * c)
        dims = (((1,), (1,)), ((), ())) if transposed else (((1,), (0,)), ((), ()))
        d = lax.dot_general(lhs, wb[a], dims, preferred_element_type=F32)
        acc = d if acc is None else acc + d
    epilogue(i, acc, extra, outs)


def _conv(transposed, epilogue, u, halo, w, extra, extra_specs, outs, out_specs, rb=2):
    th, tw, c = u.shape
    full = pl.BlockSpec((th + 2, 1, c), lambda i: (0, 0, 0), pipeline_mode=pl.Buffered(1))
    return pl.pallas_call(
        functools.partial(_conv_kernel, transposed, rb, len(extra), epilogue),
        grid=(th // rb,), out_shape=outs, in_specs=[ANY, ANY, full, full, ANY] + extra_specs, out_specs=out_specs,
        scratch_shapes=[pltpu.VMEM((th + 2, tw, 3 * c), BF16), pltpu.VMEM((3, c, 3 * c) if transposed else (3, 3 * c, c), BF16),
                        pltpu.SemaphoreType.DMA((3,)), pltpu.SemaphoreType.DMA((9,))],
        compiler_params=pltpu.CompilerParams(dimension_semantics=("arbitrary",), vmem_limit_bytes=VMEM_LIMIT),
        cost_estimate=pl.CostEstimate(flops=2 * 9 * th * tw * c * c, bytes_accessed=4 * th * tw * c + 18 * c * c, transcendentals=0),
    )(u, *halo, w, *extra)


def _ep_conv1(i, acc, extra, outs):
    a_ref, s_ref = outs
    a16 = acc.astype(BF16)
    a_ref[...] = a16.reshape(a_ref.shape)
    a = a16.astype(F32)
    s0 = a.sum(0, keepdims=True)
    s1 = (a * a).sum(0, keepdims=True)
    row = lax.broadcasted_iota(jnp.int32, s_ref.shape, 0)
    s = jnp.where(row == 0, s0, jnp.where(row == 1, s1, 0.0))

    @pl.when(i == 0)
    def _():
        s_ref[...] = s

    @pl.when(i > 0)
    def _():
        s_ref[...] += s


def _ep_dz(i, acc, extra, outs):
    a_ref, st_ref = extra
    dn_ref, s_ref = outs
    st = st_ref[...]
    xhat = (a_ref[...].astype(F32).reshape(acc.shape) - st[0:1]) * st[1:2]
    dn = acc * _gelu_grad(xhat * st[2:3] + st[3:4])
    dn_ref[...] = dn.reshape(dn_ref.shape)
    s0 = (dn * xhat).sum(0, keepdims=True)
    s1 = dn.sum(0, keepdims=True)
    row = lax.broadcasted_iota(jnp.int32, s_ref.shape, 0)
    s = jnp.where(row == 0, s0, jnp.where(row == 1, s1, 0.0))

    @pl.when(i == 0)
    def _():
        s_ref[...] = s

    @pl.when(i > 0)
    def _():
        s_ref[...] += s


def _edges(v, first_ref, last_ref):
    first_ref[...] = v[:, 0:1, :]
    last_ref[...] = v[:, v.shape[1] - 1:, :]


def _z_kernel(a_ref, st_ref, z_ref, first_ref, last_ref):
    st = st_ref[...]
    xhat = (a_ref[...].astype(F32) - st[0:1]) * st[1:2]
    z = _gelu(xhat * st[2:3] + st[3:4]).astype(BF16)
    z_ref[...] = z
    _edges(z.astype(F32), first_ref, last_ref)


def _da_kernel(dn_ref, a_ref, st_ref, t_ref, o_ref, first_ref, last_ref):
    st = st_ref[...]
    t = t_ref[...]
    xhat = (a_ref[...].astype(F32) - st[0:1]) * st[1:2]
    da = (st[1:2] * (dn_ref[...] * st[2:3] - t[3:4] - xhat * t[2:3])).astype(BF16)
    o_ref[...] = da
    _edges(da.astype(F32), first_ref, last_ref)


def _wgrad_kernel(u_ref, rows_ref, cl_ref, cr_ref, v_ref, o_ref, p, vt, psem):
    a = pl.program_id(0)
    th, tw, c = v_ref.shape

    @pl.when(a == 0)
    def _():
        cps = _load_patches(u_ref, rows_ref, p, psem)

        def tr(r, _):
            vt[:, pl.ds(pl.multiple_of(r * tw, tw), tw)] = v_ref[r].T
            return 0

        lax.fori_loop(0, th, tr, 0)
        for cp in cps:
            cp.wait()
        _shift_patches(p, cl_ref, cr_ref)

    n = 3 * c
    k = 0
    while k < n:
        m = min(512, n - k)
        rhs = p[pl.ds(a, th), :, k:k + m].reshape(th * tw, m)
        d = jnp.dot(vt[...], rhs, preferred_element_type=F32)
        o_ref[0, k:k + m, :] = d.T
        k += m


def _wgrad(u, halo, v):
    th, tw, c = u.shape
    full = pl.BlockSpec((th + 2, 1, c), lambda i: (0, 0, 0), pipeline_mode=pl.Buffered(1))
    fv = pl.BlockSpec((th, tw, c), lambda i: (0, 0, 0), pipeline_mode=pl.Buffered(1))
    return pl.pallas_call(
        _wgrad_kernel, grid=(3,), out_shape=jax.ShapeDtypeStruct((3, 3 * c, c), F32),
        in_specs=[ANY, ANY, full, full, fv], out_specs=pl.BlockSpec((1, 3 * c, c), lambda a: (a, 0, 0)),
        scratch_shapes=[pltpu.VMEM((th + 2, tw, 3 * c), BF16), pltpu.VMEM((c, th * tw), BF16), pltpu.SemaphoreType.DMA((3,))],
        compiler_params=pltpu.CompilerParams(dimension_semantics=("arbitrary",), vmem_limit_bytes=VMEM_LIMIT),
        cost_estimate=pl.CostEstimate(flops=2 * 9 * th * tw * c * c, bytes_accessed=4 * th * tw * c + 36 * c * c, transcendentals=0),
    )(u, *halo, v)


TICKS = (2, 3, 4, 6, 8, 9, 11, 13, 15, 17, 18, 20, 21, 22)


def _tail_kernel(u_ref, urows, ucl, ucr, v_ref, vrows, vcl, vcr, z_ref, zrows, zcl, zcr, w1_ref, w2_ref, xb_ref, gb_ref,
                 y_ref, dx_ref, dw_ref, p, vt, wb, dsend, hown, recv0, recv1, recv2, psem, wsem, vsem, send, recv, lsem):
    i = pl.program_id(0)
    th, tw, c = u_ref.shape
    nt = 9
    half, q, e, sub = c // 2, c // 4, c // 8, c // 16
    wi, xi, ci = lax.axis_index("w"), lax.axis_index("x"), lax.axis_index("c")
    mate, xn, yn = (wi, xi, 1 - ci), (wi, 1 - xi, ci), (1 - wi, xi, ci)
    pa, pb = xi * e, q + wi * e
    fa, fb = pa + wi * sub, pb + xi * sub

    def rows(start, n):
        return pl.ds(pl.multiple_of(start, 8), n)

    def rc(stage, t, src, dst, dev):
        return pltpu.make_async_remote_copy(src_ref=src, dst_ref=dst, send_sem=send.at[stage, t], recv_sem=recv.at[stage, t],
                                            device_id=dev, device_id_type=MESH)

    def base(t):
        return t * c + ci * half

    def s0(t):
        return [rc(0, t, dsend.at[lax.rem(t, 2)], recv0.at[lax.rem(t, 2)], mate)]

    def s1(t):
        return [rc(1, t, hown.at[t, rows((1 - xi) * e, e)], recv1.at[t, 0], xn),
                rc(2, t, hown.at[t, rows(q + (1 - wi) * e, e)], recv1.at[t, 1], yn)]

    def s2(t):
        return [rc(3, t, hown.at[t, rows(pa + (1 - wi) * sub, sub)], recv2.at[t, 0], yn),
                rc(4, t, hown.at[t, rows(pb + (1 - xi) * sub, sub)], recv2.at[t, 1], xn)]

    def s3(t):
        return [rc(5, t, hown.at[t, rows(fa, sub)], dw_ref.at[rows(base(t) + fa, sub)], yn),
                rc(6, t, hown.at[t, rows(fb, sub)], dw_ref.at[rows(base(t) + fb, sub)], xn)]

    def keep(t):
        return [pltpu.make_async_copy(hown.at[t, rows(fa, sub)], dw_ref.at[rows(base(t) + fa, sub)], lsem.at[0, t]),
                pltpu.make_async_copy(hown.at[t, rows(fb, sub)], dw_ref.at[rows(base(t) + fb, sub)], lsem.at[1, t])]

    def s4(t):
        return [rc(7, t, dw_ref.at[rows(base(t) + pa, e)], dw_ref.at[rows(base(t) + pa, e)], xn),
                rc(8, t, dw_ref.at[rows(base(t) + pb, e)], dw_ref.at[rows(base(t) + pb, e)], yn)]

    def s5(t):
        return [rc(9, t, dw_ref.at[rows(base(t), half)], dw_ref.at[rows(base(t), half)], mate)]

    def start(cps):
        for cp in cps:
            cp.start()

    def when_chunk(t, f):
        @pl.when(jnp.logical_and(t >= 0, t < nt))
        def _():
            f(t)

    def tick(j):
        def t2(t):
            for cp in s1(t):
                cp.wait_recv()
            hown[t, rows(pa, e), :] += recv1[t, 0]
            hown[t, rows(pb, e), :] += recv1[t, 1]

        def t3(t):
            for cp in s2(t):
                cp.wait_recv()
            hown[t, rows(fa, sub), :] += recv2[t, 0]
            hown[t, rows(fb, sub), :] += recv2[t, 1]

        def t4(t):
            for cp in s3(t):
                cp.wait_recv()
            for cp in keep(t):
                cp.wait()
            start(s4(t))

        def t5(t):
            for cp in s4(t):
                cp.wait_recv()
            start(s5(t))

        def t6(t):
            for cp in s5(t):
                cp.wait_recv()
            for cp in s1(t) + s2(t) + s3(t) + s4(t) + s5(t):
                cp.wait_send()

        when_chunk(j, lambda t: start(s1(t)))
        when_chunk(j - 1, t2)
        when_chunk(j - 2, t3)
        when_chunk(j - 3, t4)
        when_chunk(j - 4, t5)
        when_chunk(j - 1, lambda t: start(s2(t)))
        when_chunk(j - 2, lambda t: start(s3(t) + keep(t)))
        when_chunk(j - 5, t6)

    @pl.when(i == 0)
    def _():
        vc = pltpu.make_async_copy(v_ref, p.at[1:th + 1, :, 0:c], vsem)
        vc.start()
        cps = _load_patches(u_ref, urows, p, psem)
        pltpu.make_async_copy(w2_ref, wb, wsem.at[0]).start()
        barrier = pltpu.get_barrier_semaphore()
        for d in (mate, xn, yn):
            pl.semaphore_signal(barrier, inc=1, device_id=d, device_id_type=MESH)
        pl.semaphore_wait(barrier, 3)
        vc.wait()

        def tr(r, _):
            vt[:, pl.ds(pl.multiple_of(r * tw, tw), tw)] = p[r + 1, :, 0:c].T
            return 0

        lax.fori_loop(0, th, tr, 0)
        for cp in cps:
            cp.wait()
        _shift_patches(p, ucl, ucr)

    @pl.when(jnp.logical_and(i >= 2, i < nt + 2))
    def _():
        t = i - 2
        for cp in s0(t):
            cp.wait()
        hown[t] += recv0[lax.rem(t, 2)]

    @pl.when(jnp.logical_and(i >= 1, i < nt + 1))
    def _():
        start(s0(i - 1))

    @pl.when(i == nt)
    def _():
        cps = _load_patches(z_ref, zrows, p, psem)
        pltpu.make_async_copy(w2_ref, wb, wsem.at[0]).wait()
        for cp in cps:
            cp.wait()
        _shift_patches(p, zcl, zcr)

    @pl.when(i == nt + 8)
    def _():
        cps = _load_patches(v_ref, vrows, p, psem)
        ws = [pltpu.make_async_copy(w1_ref.at[8 - k], wb.at[k], wsem.at[k]) for k in range(9)]
        start(ws)
        for cp in cps:
            cp.wait()
        _shift_patches(p, vcl, vcr)
        for cp in ws:
            cp.wait()

    j = jnp.int32(-1)
    now = jnp.int32(0)
    for s in TICKS:
        j = j + jnp.where(i >= s, 1, 0)
        now = now + jnp.where(i == s, 1, 0)

    @pl.when(now > 0)
    def _():
        tick(j)

    @pl.when(i < nt)
    def _():
        a = lax.div(i, 3)
        b = lax.rem(i, 3)
        rhs = p[pl.ds(a, th), :, pl.ds(pl.multiple_of(b * c, 128), c)].reshape(th * tw, c)
        d = jnp.dot(vt[...], rhs, preferred_element_type=F32).T
        hown[i] = jnp.where(ci == 0, d[:half], d[half:])
        dsend[lax.rem(i, 2)] = jnp.where(ci == 0, d[half:], d[:half])

    def conv(ib, transposed, r_ref, o_ref):
        acc = None
        for a in range(3):
            lhs = p[pl.ds(ib * 2 + a, 2)].reshape(2 * tw, 3 * c)
            if transposed:
                rhs = jnp.concatenate([wb[3 * a], wb[3 * a + 1], wb[3 * a + 2]], axis=1)
                d = lax.dot_general(lhs, rhs, (((1,), (1,)), ((), ())), preferred_element_type=F32)
            else:
                d = jnp.dot(lhs, wb[3 * a:3 * a + 3].reshape(3 * c, c), preferred_element_type=F32)
            acc = d if acc is None else acc + d
        r = r_ref[...].astype(F32).reshape(acc.shape)
        o_ref[...] = (acc + r).astype(BF16).reshape(o_ref.shape)

    @pl.when(jnp.logical_and(i >= nt, i < nt + 8))
    def _():
        conv(i - nt, False, xb_ref, y_ref)

    @pl.when(i >= nt + 8)
    def _():
        conv(i - nt - 8, True, gb_ref, dx_ref)


def _tail(x, xh, da, dah, z, zh, w1, w2, g):
    th, tw, c = x.shape
    nt, half = 9, c // 2
    full = pl.BlockSpec((th + 2, 1, c), lambda i: (0, 0, 0), pipeline_mode=pl.Buffered(1))
    yb = pl.BlockSpec((2, tw, c), lambda i: (jnp.minimum(jnp.maximum(i - nt, 0), 7), 0, 0))
    xb = pl.BlockSpec((2, tw, c), lambda i: (jnp.maximum(i - nt - 8, 0), 0, 0))
    img = [ANY, ANY, full, full]
    dma = pltpu.SemaphoreType.DMA
    return pl.pallas_call(
        _tail_kernel, grid=(nt + 16,),
        out_shape=[jax.ShapeDtypeStruct((th, tw, c), BF16), jax.ShapeDtypeStruct((th, tw, c), BF16), jax.ShapeDtypeStruct((nt * c, c), F32)],
        in_specs=img * 3 + [ANY, ANY, yb, xb], out_specs=[yb, xb, ANY],
        scratch_shapes=[pltpu.VMEM((th + 2, tw, 3 * c), BF16), pltpu.VMEM((c, th * tw), BF16), pltpu.VMEM((9, c, c), BF16),
                        pltpu.VMEM((2, half, c), F32), pltpu.VMEM((nt, half, c), F32), pltpu.VMEM((2, half, c), F32),
                        pltpu.VMEM((nt, 2, c // 8, c), F32), pltpu.VMEM((nt, 2, c // 16, c), F32),
                        dma((3,)), dma((9,)), dma, dma((10, nt)), dma((10, nt)), dma((2, nt))],
        compiler_params=pltpu.CompilerParams(dimension_semantics=("arbitrary",), vmem_limit_bytes=VMEM_LIMIT, collective_id=5, has_side_effects=True),
        cost_estimate=pl.CostEstimate(flops=3 * 2 * 9 * th * tw * c * c, bytes_accessed=16 * th * tw * c, transcendentals=0),
        name="tail",
    )(x, *xh, da, *dah, z, *zh, w1.reshape(9, c, c), w2.reshape(9, c, c), x, g)


def _reduce_all(d):
    r, k, c = d.shape
    s = lax.psum_scatter(d.reshape(r * k, c), ("c", "w", "x"), scatter_dimension=0, tiled=True)
    return lax.all_gather(s, ("c", "w", "x"), axis=0, tiled=True).reshape(3, 3, c, c)


def solution(mesh):
    nh, nw = mesh.shape["h"], mesh.shape["w"]
    mesh3 = Mesh(mesh.devices.reshape(nw, nh // 2, 2), ("w", "x", "c"))
    tile = P(None, ("x", "c"), "w", None)

    def body(x, w1, gamma, beta, w2, g):
        _, th, tw, c = x.shape
        x, g = x[0], g[0]
        cnt = float(th * nh * tw * nw * (c // GROUPS))
        rb = 2
        blk = pl.BlockSpec((rb, tw, c), lambda i: (i, 0, 0))
        small = pl.BlockSpec((8, c), lambda i: (0, 0))
        img16 = jax.ShapeDtypeStruct((th, tw, c), BF16)
        img32 = jax.ShapeDtypeStruct((th, tw, c), F32)
        sums = jax.ShapeDtypeStruct((8, c), F32)
        par = jnp.concatenate([jnp.zeros((2, c), F32), gamma[None], beta[None], jnp.zeros((4, c), F32)])

        edge = jax.ShapeDtypeStruct((th, 1, c), F32)
        eblk = pl.BlockSpec((rb, 1, c), lambda i: (i, 0, 0))

        def with_edges(u):
            return u, u[:, 0:1, :].astype(F32), u[:, tw - 1:, :].astype(F32)

        xh, gh = _halo(nh, nw, 0, *with_edges(x), *with_edges(g))
        a, s = _conv(False, _ep_conv1, x, xh, w1, [], [], [img16, sums], [blk, small])
        st = _allsum(nh, nw, cnt, 0, 1, s, par)
        z, z0, z1 = pl.pallas_call(_z_kernel, grid=(th // rb,), out_shape=[img16, edge, edge], in_specs=[blk, small], out_specs=[blk, eblk, eblk], name="act")(a, st)
        (zh,) = _halo(nh, nw, 2, z, z0, z1)
        d2 = _wgrad(z, zh, g)
        g_late, d2 = lax.optimization_barrier((g, d2))
        dw2 = _reduce_all(d2)
        dn, t = _conv(True, _ep_dz, g_late, gh, w2, [a, st], [blk, small], [img32, sums], [blk, small])
        t = _allsum(nh, nw, cnt, 1, 3, t, st)
        da, da0, da1 = pl.pallas_call(_da_kernel, grid=(th // rb,), out_shape=[img16, edge, edge], in_specs=[blk, blk, small, small], out_specs=[blk, eblk, eblk], name="da")(dn, a, st, t)
        (dah,) = _halo(nh, nw, 4, da, da0, da1)
        y, dx, dw1 = _tail(x, xh, da, dah, z, zh, w1, w2, g)
        return y[None], dx[None], dw1.reshape(3, 3, c, c), dw2, t[0], t[1]

    return jax.shard_map(body, mesh=mesh3, in_specs=(tile, P(), P(), P(), P(), tile), out_specs=(tile, tile, P(), P(), P(), P()), check_vma=False)
```

```python
import functools

import jax
import jax.numpy as jnp
from jax import lax
from jax.experimental import pallas as pl
from jax.experimental.pallas import tpu as pltpu
from jax.sharding import Mesh
from jax.sharding import PartitionSpec as P

GROUPS = 32
EPS = 1e-5
F32 = jnp.float32
BF16 = jnp.bfloat16
MESH = pl.DeviceIdType.MESH
VMEM_LIMIT = 61 * 1024 * 1024
ANY = pl.BlockSpec(memory_space=pl.ANY)
VM = pl.BlockSpec(memory_space=pltpu.VMEM)
GELU_C = 0.7978845608028654
GELU_A = 0.044715


def _gelu_parts(n):
    n2 = n * n
    t = jnp.tanh(GELU_C * (n + GELU_A * n * n2))
    return n2, t


def _gelu(n):
    _, t = _gelu_parts(n)
    return 0.5 * n * (1.0 + t)


def _gelu_grad(n):
    n2, t = _gelu_parts(n)
    return 0.5 * (1.0 + t) + 0.5 * n * (1.0 - t * t) * (GELU_C * (1.0 + 3.0 * GELU_A * n2))


def _halo_kernel(nh, nw, n_arr, *refs):
    ins = refs[:3 * n_arr]
    outs = refs[3 * n_arr:6 * n_arr]
    send, recv = refs[6 * n_arr:]
    th, tw, c = ins[0].shape
    w = lax.axis_index("w")
    h = lax.axis_index("x") * 2 + lax.axis_index("c")

    def dev(dh, dw):
        hh = h + dh
        return (w + dw, hh // 2, hh % 2)

    def has(dh, dw):
        ok = None
        for cond in ([h > 0] if dh < 0 else [h < nh - 1] if dh > 0 else []) + ([w > 0] if dw < 0 else [w < nw - 1] if dw > 0 else []):
            ok = cond if ok is None else jnp.logical_and(ok, cond)
        return ok

    dirs = [(dh, dw) for dh in (-1, 0, 1) for dw in (-1, 0, 1) if (dh, dw) != (0, 0)]
    barrier = pltpu.get_barrier_semaphore()
    for d in dirs:
        @pl.when(has(*d))
        def _(d=d):
            pl.semaphore_signal(barrier, inc=1, device_id=dev(*d), device_id_type=MESH)
    one = jnp.int32(1)
    zero = jnp.int32(0)
    nv = one + jnp.where(h > 0, one, zero) + jnp.where(h < nh - 1, one, zero)
    nz = one + jnp.where(w > 0, one, zero) + jnp.where(w < nw - 1, one, zero)
    pl.semaphore_wait(barrier, nv * nz - 1)

    def parts(k, dh, dw):
        u, first, last = ins[3 * k:3 * k + 3]
        rows, cl, cr = outs[3 * k:3 * k + 3]
        r = 0 if dh < 0 else th - 1
        to = 1 if dh < 0 else 0
        to18 = th + 1 if dh < 0 else 0
        edge, side = (first, cr) if dw < 0 else (last, cl)
        if dw == 0:
            return u.at[r], rows.at[to]
        if dh == 0:
            return edge, side.at[1:th + 1]
        return edge.at[r], side.at[to18]

    def copy(k, i, dh, dw):
        src, dst = parts(k, dh, dw)
        return pltpu.make_async_remote_copy(src_ref=src, dst_ref=dst, send_sem=send.at[k * 8 + i], recv_sem=recv.at[k * 8 + i],
                                            device_id=dev(dh, dw), device_id_type=MESH)

    for k in range(n_arr):
        for i, d in enumerate(dirs):
            @pl.when(has(*d))
            def _(k=k, i=i, d=d):
                copy(k, i, *d).start()
    for k in range(n_arr):
        rows, cl, cr = outs[3 * k:3 * k + 3]
        for i, (dh, dw) in enumerate(dirs):
            @pl.when(jnp.logical_not(has(-dh, -dw)))
            def _(rows=rows, cl=cl, cr=cr, dh=dh, dw=dw):
                to = 1 if dh < 0 else 0
                to18 = th + 1 if dh < 0 else 0
                side = cr if dw < 0 else cl
                if dw == 0:
                    rows[to] = jnp.zeros((tw, c), BF16)
                elif dh == 0:
                    side[1:th + 1] = jnp.zeros((th, 1, c), F32)
                else:
                    side[to18] = jnp.zeros((1, c), F32)
    for k in range(n_arr):
        for i, (dh, dw) in enumerate(dirs):
            @pl.when(has(dh, dw))
            def _(k=k, i=i, dh=dh, dw=dw):
                copy(k, i, dh, dw).wait_send()

            @pl.when(has(-dh, -dw))
            def _(k=k, i=i, dh=dh, dw=dw):
                copy(k, i, dh, dw).wait_recv()


def _halo(nh, nw, cid, *us):
    th, tw, c = us[0].shape
    n = len(us) // 3
    out = []
    for _ in range(n):
        out += [jax.ShapeDtypeStruct((2, tw, c), BF16), jax.ShapeDtypeStruct((th + 2, 1, c), F32), jax.ShapeDtypeStruct((th + 2, 1, c), F32)]
    res = pl.pallas_call(
        functools.partial(_halo_kernel, nh, nw, n), out_shape=out, in_specs=[ANY] * (3 * n), out_specs=[VM] * (3 * n),
        scratch_shapes=[pltpu.SemaphoreType.DMA((8 * n,)), pltpu.SemaphoreType.DMA((8 * n,))],
        compiler_params=pltpu.CompilerParams(collective_id=cid, has_side_effects=True, vmem_limit_bytes=VMEM_LIMIT),
        name=f"halo{cid}",
    )(*us)
    return [tuple(res[3 * k:3 * k + 3]) for k in range(n)]


def _allsum_kernel(nh, nw, cnt, mode, part_ref, par_ref, out_ref, mine, buf, lsem, send, recv):
    n = nh * nw
    w = lax.axis_index("w")
    h = lax.axis_index("x") * 2 + lax.axis_index("c")
    me = w * nh + h

    def dev(j):
        hh = j % nh
        return (j // nh, hh // 2, hh % 2)

    local = pltpu.make_async_copy(part_ref, mine, lsem)
    local.start()
    barrier = pltpu.get_barrier_semaphore()
    for k in range(1, n):
        pl.semaphore_signal(barrier, inc=1, device_id=dev(lax.rem(me + k, n)), device_id_type=MESH)
    local.wait()
    pl.semaphore_wait(barrier, n - 1)
    copies = []
    for k in range(1, n):
        cp = pltpu.make_async_remote_copy(src_ref=mine, dst_ref=buf.at[k - 1], send_sem=send.at[k - 1], recv_sem=recv.at[k - 1],
                                          device_id=dev(lax.rem(me + k, n)), device_id_type=MESH)
        cp.start()
        copies.append(cp)
    for cp in copies:
        cp.wait()
    total = None
    vals = [mine[...]] + [buf[k] for k in range(n - 1)]
    for j in range(n):
        t = jnp.zeros_like(vals[0])
        off = lax.rem(me - j + n, n)
        for k in range(n):
            t = t + jnp.where(off == k, vals[k], 0.0)
        total = t if total is None else total + t
    c = total.shape[-1]
    gi = jnp.floor((lax.broadcasted_iota(jnp.int32, (c, c), 0).astype(F32) + 0.5) * (GROUPS / c))
    gj = jnp.floor((lax.broadcasted_iota(jnp.int32, (c, c), 1).astype(F32) + 0.5) * (GROUPS / c))
    same = jnp.where(gi == gj, 1.0, 0.0).astype(F32)
    row = lax.broadcasted_iota(jnp.int32, (8, c), 0)
    if mode == 0:
        m = jnp.dot(total, same, precision=lax.Precision.HIGHEST, preferred_element_type=F32) / cnt
        mean, sq = m[0:1], m[1:2]
        rstd = lax.rsqrt(sq - mean * mean + EPS)
        out_ref[...] = jnp.where(row == 0, mean, jnp.where(row == 1, rstd, par_ref[...]))
    else:
        u = jnp.dot(total * par_ref[2:3], same, precision=lax.Precision.HIGHEST, preferred_element_type=F32) / cnt
        out_ref[...] = jnp.where(row == 0, total[0:1], jnp.where(row == 1, total[1:2], jnp.where(row == 2, u[0:1], u[1:2])))


def _allsum(nh, nw, cnt, mode, cid, part, par):
    c = part.shape[-1]
    n = nh * nw
    return pl.pallas_call(
        functools.partial(_allsum_kernel, nh, nw, cnt, mode), out_shape=jax.ShapeDtypeStruct((8, c), F32),
        in_specs=[ANY, VM], out_specs=VM,
        scratch_shapes=[pltpu.VMEM((8, c), F32), pltpu.VMEM((n - 1, 8, c), F32), pltpu.SemaphoreType.DMA,
                        pltpu.SemaphoreType.DMA((n - 1,)), pltpu.SemaphoreType.DMA((n - 1,))],
        compiler_params=pltpu.CompilerParams(collective_id=cid, has_side_effects=True, vmem_limit_bytes=VMEM_LIMIT),
        name=f"allsum{cid}",
    )(part, par)


def _load_patches(u_ref, rows_ref, p, sems):
    th, c = u_ref.shape[0], u_ref.shape[2]
    cps = [pltpu.make_async_copy(u_ref, p.at[1:th + 1, :, c:2 * c], sems.at[0]),
           pltpu.make_async_copy(rows_ref.at[0], p.at[0, :, c:2 * c], sems.at[1]),
           pltpu.make_async_copy(rows_ref.at[1], p.at[th + 1, :, c:2 * c], sems.at[2])]
    for cp in cps:
        cp.start()
    return cps


def _shift_patches(p, cl_ref, cr_ref):
    n, tw, c3 = p.shape
    c = c3 // 3
    ck = 128

    def row(r, _):
        idx = lax.broadcasted_iota(jnp.int32, (tw, ck), 0)
        for k in range(c // ck):
            f = p[r, :, c + k * ck:c + (k + 1) * ck].astype(F32)
            lo = cl_ref[r, :, k * ck:(k + 1) * ck]
            hi = cr_ref[r, :, k * ck:(k + 1) * ck]
            p[r, :, k * ck:(k + 1) * ck] = jnp.where(idx == 0, lo, pltpu.roll(f, 1, 0)).astype(BF16)
            p[r, :, 2 * c + k * ck:2 * c + (k + 1) * ck] = jnp.where(idx == tw - 1, hi, pltpu.roll(f, tw - 1, 0)).astype(BF16)
        return 0

    lax.fori_loop(0, n, row, 0)


def _conv_kernel(rb, epilogue, u_ref, rows_ref, cl_ref, cr_ref, w_ref, *refs):
    outs = refs[:-4]
    p, wb, psem, wsem = refs[-4:]
    c = u_ref.shape[2]
    i = pl.program_id(0)

    @pl.when(i == 0)
    def _():
        cps = _load_patches(u_ref, rows_ref, p, psem)
        wc = pltpu.make_async_copy(w_ref, wb, wsem)
        wc.start()
        for cp in cps:
            cp.wait()
        _shift_patches(p, cl_ref, cr_ref)
        wc.wait()

    tw = p.shape[1]
    acc = None
    for a in range(3):
        lhs = p[pl.ds(i * rb + a, rb)].reshape(rb * tw, 3 * c)
        d = jnp.dot(lhs, wb[a], preferred_element_type=F32)
        acc = d if acc is None else acc + d
    epilogue(i, acc, (), outs)


def _conv(name, epilogue, u, halo, w, outs, out_specs, rb=2):
    th, tw, c = u.shape
    full = pl.BlockSpec((th + 2, 1, c), lambda i: (0, 0, 0), pipeline_mode=pl.Buffered(1))
    wshape = (3, 3 * c, c)
    return pl.pallas_call(
        functools.partial(_conv_kernel, rb, epilogue),
        grid=(th // rb,), out_shape=outs, in_specs=[ANY, ANY, full, full, ANY], out_specs=out_specs,
        scratch_shapes=[pltpu.VMEM((th + 2, tw, 3 * c), BF16), pltpu.VMEM(wshape, BF16), pltpu.SemaphoreType.DMA((3,)), pltpu.SemaphoreType.DMA],
        compiler_params=pltpu.CompilerParams(dimension_semantics=("arbitrary",), vmem_limit_bytes=VMEM_LIMIT),
        name=name,
    )(u, *halo, w.reshape(wshape))


def _add_sums(i, s0, s1, s_ref):
    row = lax.broadcasted_iota(jnp.int32, s_ref.shape, 0)
    s = jnp.where(row == 0, s0, jnp.where(row == 1, s1, 0.0))

    @pl.when(i == 0)
    def _():
        s_ref[...] = s

    @pl.when(i > 0)
    def _():
        s_ref[...] += s


def _ep_conv1(i, acc, extra, outs):
    a_ref, s_ref = outs
    a16 = acc.astype(BF16)
    a_ref[...] = a16.reshape(a_ref.shape)
    a = a16.astype(F32)
    s0 = a.sum(0, keepdims=True)
    s1 = (a * a).sum(0, keepdims=True)
    _add_sums(i, s0, s1, s_ref)


def _ep_residual(i, acc, extra, outs):
    o_ref = outs[0]
    r = extra[0][...].astype(F32).reshape(acc.shape)
    o_ref[...] = (acc + r).astype(BF16).reshape(o_ref.shape)


def _ep_dz(i, acc, extra, outs):
    a_ref, st_ref = extra
    dn_ref, s_ref = outs
    st = st_ref[...]
    xhat = (a_ref[...].astype(F32).reshape(acc.shape) - st[0:1]) * st[1:2]
    dn = acc * _gelu_grad(xhat * st[2:3] + st[3:4])
    dn_ref[...] = dn.reshape(dn_ref.shape)
    s0 = (dn * xhat).sum(0, keepdims=True)
    s1 = dn.sum(0, keepdims=True)
    _add_sums(i, s0, s1, s_ref)


def _edges(v, first_ref, last_ref):
    first_ref[...] = v[:, 0:1, :]
    last_ref[...] = v[:, v.shape[1] - 1:, :]


def _z_kernel(a_ref, st_ref, z_ref, first_ref, last_ref):
    st = st_ref[...]
    xhat = (a_ref[...].astype(F32) - st[0:1]) * st[1:2]
    z = _gelu(xhat * st[2:3] + st[3:4]).astype(BF16)
    z_ref[...] = z
    _edges(z.astype(F32), first_ref, last_ref)


def _da_kernel(dn_ref, a_ref, st_ref, t_ref, o_ref, first_ref, last_ref):
    st = st_ref[...]
    t = t_ref[...]
    xhat = (a_ref[...].astype(F32) - st[0:1]) * st[1:2]
    da = (st[1:2] * (dn_ref[...] * st[2:3] - t[3:4] - xhat * t[2:3])).astype(BF16)
    o_ref[...] = da
    _edges(da.astype(F32), first_ref, last_ref)


def _fused_kernel(ticks, nu, ep_u, ep_v, n_xu, n_xv, n_ov, u_ref, urows, ucl, ucr, v_ref, vrows, vcl, vcr, w_ref, *refs):
    xu, refs = refs[:n_xu], refs[n_xu:]
    xv, refs = refs[:n_xv], refs[n_xv:]
    ou, refs = (refs[:1], refs[1:]) if nu else ((), refs)
    ov, refs = refs[:n_ov], refs[n_ov:]
    dw_ref, p, vt, wb, dsend, hown, recv0, recv1, recv2, psem, wsem, vsem, send, recv, lsem = refs
    i = pl.program_id(0)
    th, tw, c = u_ref.shape
    nt = w_ref.shape[0]
    half, q, e, sub = c // 2, c // 4, c // 8, c // 16
    wi, xi, ci = lax.axis_index("w"), lax.axis_index("x"), lax.axis_index("c")
    mate, xn, yn = (wi, xi, 1 - ci), (wi, 1 - xi, ci), (1 - wi, xi, ci)
    pa, pb = xi * e, q + wi * e
    fa, fb = pa + wi * sub, pb + xi * sub

    def rows(start, n):
        return pl.ds(pl.multiple_of(start, 8), n)

    def rc(stage, t, src, dst, dev):
        return pltpu.make_async_remote_copy(src_ref=src, dst_ref=dst, send_sem=send.at[stage, t], recv_sem=recv.at[stage, t],
                                            device_id=dev, device_id_type=MESH)

    def base(t):
        return t * c + ci * half

    def s0(t):
        return [rc(0, t, dsend.at[lax.rem(t, 2)], recv0.at[lax.rem(t, 2)], mate)]

    def s1(t):
        return [rc(1, t, hown.at[t, rows((1 - xi) * e, e)], recv1.at[t, 0], xn),
                rc(2, t, hown.at[t, rows(q + (1 - wi) * e, e)], recv1.at[t, 1], yn)]

    def s2(t):
        return [rc(3, t, hown.at[t, rows(pa + (1 - wi) * sub, sub)], recv2.at[t, 0], yn),
                rc(4, t, hown.at[t, rows(pb + (1 - xi) * sub, sub)], recv2.at[t, 1], xn)]

    def s3(t):
        return [rc(5, t, hown.at[t, rows(fa, sub)], dw_ref.at[rows(base(t) + fa, sub)], yn),
                rc(6, t, hown.at[t, rows(fb, sub)], dw_ref.at[rows(base(t) + fb, sub)], xn)]

    def keep(t):
        return [pltpu.make_async_copy(hown.at[t, rows(fa, sub)], dw_ref.at[rows(base(t) + fa, sub)], lsem.at[0, t]),
                pltpu.make_async_copy(hown.at[t, rows(fb, sub)], dw_ref.at[rows(base(t) + fb, sub)], lsem.at[1, t])]

    def s4(t):
        return [rc(7, t, dw_ref.at[rows(base(t) + pa, e)], dw_ref.at[rows(base(t) + pa, e)], xn),
                rc(8, t, dw_ref.at[rows(base(t) + pb, e)], dw_ref.at[rows(base(t) + pb, e)], yn)]

    def s5(t):
        return [rc(9, t, dw_ref.at[rows(base(t), half)], dw_ref.at[rows(base(t), half)], mate)]

    def start(cps):
        for cp in cps:
            cp.start()

    def when_chunk(t, f):
        @pl.when(jnp.logical_and(t >= 0, t < nt))
        def _():
            f(t)

    def tick(j):
        def t2(t):
            for cp in s1(t):
                cp.wait_recv()
            hown[t, rows(pa, e), :] += recv1[t, 0]
            hown[t, rows(pb, e), :] += recv1[t, 1]

        def t3(t):
            for cp in s2(t):
                cp.wait_recv()
            hown[t, rows(fa, sub), :] += recv2[t, 0]
            hown[t, rows(fb, sub), :] += recv2[t, 1]

        def t4(t):
            for cp in s3(t):
                cp.wait_recv()
            for cp in keep(t):
                cp.wait()
            start(s4(t))

        def t5(t):
            for cp in s4(t):
                cp.wait_recv()
            start(s5(t))

        def t6(t):
            for cp in s5(t):
                cp.wait_recv()
            for cp in s1(t) + s2(t) + s3(t) + s4(t) + s5(t):
                cp.wait_send()

        when_chunk(j, lambda t: start(s1(t)))
        when_chunk(j - 1, t2)
        when_chunk(j - 2, t3)
        when_chunk(j - 3, t4)
        when_chunk(j - 4, t5)
        when_chunk(j - 1, lambda t: start(s2(t)))
        when_chunk(j - 2, lambda t: start(s3(t) + keep(t)))
        when_chunk(j - 5, t6)

    wcp = pltpu.make_async_copy(w_ref, wb, wsem)

    @pl.when(i == 0)
    def _():
        vc = pltpu.make_async_copy(v_ref, p.at[1:th + 1, :, 0:c], vsem)
        vc.start()
        cps = _load_patches(u_ref, urows, p, psem)
        wcp.start()
        barrier = pltpu.get_barrier_semaphore()
        for d in (mate, xn, yn):
            pl.semaphore_signal(barrier, inc=1, device_id=d, device_id_type=MESH)
        pl.semaphore_wait(barrier, 3)
        vc.wait()

        def tr(r, _):
            vt[:, pl.ds(pl.multiple_of(r * tw, tw), tw)] = p[r + 1, :, 0:c].T
            return 0

        lax.fori_loop(0, th, tr, 0)
        for cp in cps:
            cp.wait()
        _shift_patches(p, ucl, ucr)

    @pl.when(jnp.logical_and(i >= 2, i < nt + 2))
    def _():
        t = i - 2
        for cp in s0(t):
            cp.wait()
        hown[t] += recv0[lax.rem(t, 2)]

    @pl.when(jnp.logical_and(i >= 1, i < nt + 1))
    def _():
        start(s0(i - 1))

    @pl.when(i == nt)
    def _():
        wcp.wait()

    @pl.when(i == nt + nu)
    def _():
        cps = _load_patches(v_ref, vrows, p, psem)
        for cp in cps:
            cp.wait()
        _shift_patches(p, vcl, vcr)

    j = jnp.int32(-1)
    now = jnp.int32(0)
    for s in ticks:
        j = j + jnp.where(i >= s, 1, 0)
        now = now + jnp.where(i == s, 1, 0)

    @pl.when(now > 0)
    def _():
        tick(j)

    @pl.when(i < nt)
    def _():
        a = lax.div(i, 3)
        b = lax.rem(i, 3)
        rhs = p[pl.ds(a, th), :, pl.ds(pl.multiple_of(b * c, 128), c)].reshape(th * tw, c)
        d = jnp.dot(vt[...], rhs, preferred_element_type=F32).T
        hown[i] = jnp.where(ci == 0, d[:half], d[half:])
        dsend[lax.rem(i, 2)] = jnp.where(ci == 0, d[half:], d[:half])

    def conv(ib, transposed):
        acc = None
        for a in range(3):
            lhs = p[pl.ds(ib * 2 + a, 2)].reshape(2 * tw, 3 * c)
            if transposed:
                k = nt - 1 - 3 * a
                rhs = jnp.concatenate([wb[k], wb[k - 1], wb[k - 2]], axis=1)
                d = lax.dot_general(lhs, rhs, (((1,), (1,)), ((), ())), preferred_element_type=F32)
            else:
                d = jnp.dot(lhs, wb[3 * a:3 * a + 3].reshape(3 * c, c), preferred_element_type=F32)
            acc = d if acc is None else acc + d
        return acc

    if nu:
        @pl.when(jnp.logical_and(i >= nt, i < nt + nu))
        def _():
            ep_u(i - nt, conv(i - nt, False), xu, ou)

    @pl.when(jnp.logical_and(i >= nt + nu, i < nt + nu + th // 2))
    def _():
        ib = i - nt - nu
        ep_v(ib, conv(ib, True), xv, ov)


def _fused(name, cid, steps, ticks, u, uh, v, vh, w, nu, ep_u, xu, ep_v, xv, outs_v):
    th, tw, c = u.shape
    nt, half = 9, c // 2
    last = th // 2 - 1
    full = pl.BlockSpec((th + 2, 1, c), lambda i: (0, 0, 0), pipeline_mode=pl.Buffered(1))
    small = pl.BlockSpec((8, c), lambda i: (0, 0))
    ub = pl.BlockSpec((2, tw, c), lambda i: (jnp.minimum(jnp.maximum(i - nt, 0), nu - 1), 0, 0))
    vb = pl.BlockSpec((2, tw, c), lambda i: (jnp.minimum(jnp.maximum(i - nt - nu, 0), last), 0, 0))
    img = [ANY, ANY, full, full]
    dma = pltpu.SemaphoreType.DMA
    out_u = [jax.ShapeDtypeStruct((2 * nu, tw, c), BF16)] if nu else []
    call = pl.pallas_call(
        functools.partial(_fused_kernel, ticks, nu, ep_u, ep_v, len(xu), len(xv), len(outs_v)), grid=(steps,),
        out_shape=out_u + [o for o, _ in outs_v] + [jax.ShapeDtypeStruct((nt * c, c), F32)],
        in_specs=img + img + [ANY] + [ub for _ in xu] + [vb if b else small for _, b in xv],
        out_specs=[ub for _ in out_u] + [vb if b else small for _, b in outs_v] + [ANY],
        scratch_shapes=[pltpu.VMEM((th + 2, tw, 3 * c), BF16), pltpu.VMEM((c, th * tw), BF16), pltpu.VMEM((nt, c, c), BF16),
                        pltpu.VMEM((2, half, c), F32), pltpu.VMEM((nt, half, c), F32), pltpu.VMEM((2, half, c), F32),
                        pltpu.VMEM((nt, 2, c // 8, c), F32), pltpu.VMEM((nt, 2, c // 16, c), F32),
                        dma((3,)), dma, dma, dma((10, nt)), dma((10, nt)), dma((2, nt))],
        compiler_params=pltpu.CompilerParams(dimension_semantics=("arbitrary",), vmem_limit_bytes=VMEM_LIMIT, collective_id=cid, has_side_effects=True),
        name=name,
    )
    return call(u, *uh, v, *vh, w.reshape(nt, c, c), *[x for x, _ in xu], *[x for x, _ in xv])


def solution(mesh):
    nh, nw = mesh.shape["h"], mesh.shape["w"]
    mesh3 = Mesh(mesh.devices.reshape(nw, nh // 2, 2), ("w", "x", "c"))
    tile = P(None, ("x", "c"), "w", None)

    def body(x, w1, gamma, beta, w2, g):
        _, th, tw, c = x.shape
        x, g = x[0], g[0]
        cnt = float(th * nh * tw * nw * (c // GROUPS))
        rb = 2
        blk = pl.BlockSpec((rb, tw, c), lambda i: (i, 0, 0))
        small = pl.BlockSpec((8, c), lambda i: (0, 0))
        img16 = jax.ShapeDtypeStruct((th, tw, c), BF16)
        img32 = jax.ShapeDtypeStruct((th, tw, c), F32)
        sums = jax.ShapeDtypeStruct((8, c), F32)
        par = jnp.concatenate([jnp.zeros((2, c), F32), gamma[None], beta[None], jnp.zeros((4, c), F32)])

        edge = jax.ShapeDtypeStruct((th, 1, c), F32)
        eblk = pl.BlockSpec((rb, 1, c), lambda i: (i, 0, 0))

        def with_edges(u):
            return u, u[:, 0:1, :].astype(F32), u[:, tw - 1:, :].astype(F32)

        xh, gh = _halo(nh, nw, 0, *with_edges(x), *with_edges(g))
        a, s = _conv("conv1", _ep_conv1, x, xh, w1, [img16, sums], [blk, small])
        st = _allsum(nh, nw, cnt, 0, 1, s, par)
        z, z0, z1 = pl.pallas_call(_z_kernel, grid=(th // rb,), out_shape=[img16, edge, edge], in_specs=[blk, small], out_specs=[blk, eblk, eblk], name="act")(a, st)
        (zh,) = _halo(nh, nw, 2, z, z0, z1)
        y, dn, t, dw2 = _fused("mid", 5, 25, (2, 3, 4, 6, 8, 9, 11, 13, 15, 17, 18, 20, 21, 22), z, zh, g, gh, w2, 8, _ep_residual, [(x, True)],
                               _ep_dz, [(a, True), (st, False)], [(img32, True), (sums, False)])
        t = _allsum(nh, nw, cnt, 1, 3, t, st)
        da, da0, da1 = pl.pallas_call(_da_kernel, grid=(th // rb,), out_shape=[img16, edge, edge], in_specs=[blk, blk, small, small], out_specs=[blk, eblk, eblk], name="da")(dn, a, st, t)
        (dah,) = _halo(nh, nw, 4, da, da0, da1)
        dx, dw1 = _fused("tail", 6, 21, (2, 3, 4, 5, 7, 9, 11, 13, 15, 16, 17, 18, 19, 20), x, xh, da, dah, w1, 0, None, [],
                         _ep_residual, [(g, True)], [(img16, True)])
        return y[None], dx[None], dw1.reshape(w1.shape), dw2.reshape(w2.shape), t[0], t[1]

    return jax.shard_map(body, mesh=mesh3, in_specs=(tile, P(), P(), P(), P(), tile), out_specs=(tile, tile, P(), P(), P(), P()), check_vma=False)
```

```python
import functools

import jax
import jax.numpy as jnp
from jax import lax
from jax.experimental import pallas as pl
from jax.experimental.pallas import tpu as pltpu
from jax.sharding import Mesh
from jax.sharding import PartitionSpec as P

GROUPS = 32
EPS = 1e-5
F32 = jnp.float32
BF16 = jnp.bfloat16
MESH = pl.DeviceIdType.MESH
VMEM_LIMIT = 61 * 1024 * 1024
ANY = pl.BlockSpec(memory_space=pl.ANY)
VM = pl.BlockSpec(memory_space=pltpu.VMEM)
GELU_C = 0.7978845608028654
GELU_A = 0.044715


def _gelu_parts(n):
    n2 = n * n
    t = jnp.tanh(GELU_C * (n + GELU_A * n * n2))
    return n2, t


def _gelu(n):
    _, t = _gelu_parts(n)
    return 0.5 * n * (1.0 + t)


def _gelu_grad(n):
    n2, t = _gelu_parts(n)
    return 0.5 * (1.0 + t) + 0.5 * n * (1.0 - t * t) * (GELU_C * (1.0 + 3.0 * GELU_A * n2))


def _halo_kernel(nh, nw, n_arr, *refs):
    ins = refs[:3 * n_arr]
    outs = refs[3 * n_arr:6 * n_arr]
    send, recv = refs[6 * n_arr:]
    th, tw, c = ins[0].shape
    w = lax.axis_index("w")
    h = lax.axis_index("x") * 2 + lax.axis_index("c")

    def dev(dh, dw):
        hh = h + dh
        return (w + dw, hh // 2, hh % 2)

    def has(dh, dw):
        ok = None
        for cond in ([h > 0] if dh < 0 else [h < nh - 1] if dh > 0 else []) + ([w > 0] if dw < 0 else [w < nw - 1] if dw > 0 else []):
            ok = cond if ok is None else jnp.logical_and(ok, cond)
        return ok

    dirs = [(dh, dw) for dh in (-1, 0, 1) for dw in (-1, 0, 1) if (dh, dw) != (0, 0)]
    barrier = pltpu.get_barrier_semaphore()
    for d in dirs:
        @pl.when(has(*d))
        def _(d=d):
            pl.semaphore_signal(barrier, inc=1, device_id=dev(*d), device_id_type=MESH)
    one = jnp.int32(1)
    zero = jnp.int32(0)
    nv = one + jnp.where(h > 0, one, zero) + jnp.where(h < nh - 1, one, zero)
    nz = one + jnp.where(w > 0, one, zero) + jnp.where(w < nw - 1, one, zero)
    pl.semaphore_wait(barrier, nv * nz - 1)

    def parts(k, dh, dw):
        u, first, last = ins[3 * k:3 * k + 3]
        rows, cl, cr = outs[3 * k:3 * k + 3]
        r = 0 if dh < 0 else th - 1
        to = 1 if dh < 0 else 0
        to18 = th + 1 if dh < 0 else 0
        edge, side = (first, cr) if dw < 0 else (last, cl)
        if dw == 0:
            return u.at[r], rows.at[to]
        if dh == 0:
            return edge, side.at[1:th + 1]
        return edge.at[r], side.at[to18]

    def copy(k, i, dh, dw):
        src, dst = parts(k, dh, dw)
        return pltpu.make_async_remote_copy(src_ref=src, dst_ref=dst, send_sem=send.at[k * 8 + i], recv_sem=recv.at[k * 8 + i],
                                            device_id=dev(dh, dw), device_id_type=MESH)

    for k in range(n_arr):
        for i, d in enumerate(dirs):
            @pl.when(has(*d))
            def _(k=k, i=i, d=d):
                copy(k, i, *d).start()
    for k in range(n_arr):
        rows, cl, cr = outs[3 * k:3 * k + 3]
        for i, (dh, dw) in enumerate(dirs):
            @pl.when(jnp.logical_not(has(-dh, -dw)))
            def _(rows=rows, cl=cl, cr=cr, dh=dh, dw=dw):
                to = 1 if dh < 0 else 0
                to18 = th + 1 if dh < 0 else 0
                side = cr if dw < 0 else cl
                if dw == 0:
                    rows[to] = jnp.zeros((tw, c), BF16)
                elif dh == 0:
                    side[1:th + 1] = jnp.zeros((th, 1, c), F32)
                else:
                    side[to18] = jnp.zeros((1, c), F32)
    for k in range(n_arr):
        for i, (dh, dw) in enumerate(dirs):
            @pl.when(has(dh, dw))
            def _(k=k, i=i, dh=dh, dw=dw):
                copy(k, i, dh, dw).wait_send()

            @pl.when(has(-dh, -dw))
            def _(k=k, i=i, dh=dh, dw=dw):
                copy(k, i, dh, dw).wait_recv()


def _halo(nh, nw, cid, *us):
    th, tw, c = us[0].shape
    n = len(us) // 3
    out = []
    for _ in range(n):
        out += [jax.ShapeDtypeStruct((2, tw, c), BF16), jax.ShapeDtypeStruct((th + 2, 1, c), F32), jax.ShapeDtypeStruct((th + 2, 1, c), F32)]
    res = pl.pallas_call(
        functools.partial(_halo_kernel, nh, nw, n), out_shape=out, in_specs=[ANY] * (3 * n), out_specs=[VM] * (3 * n),
        scratch_shapes=[pltpu.SemaphoreType.DMA((8 * n,)), pltpu.SemaphoreType.DMA((8 * n,))],
        compiler_params=pltpu.CompilerParams(collective_id=cid, has_side_effects=True, vmem_limit_bytes=VMEM_LIMIT),
        name=f"halo{cid}",
    )(*us)
    return [tuple(res[3 * k:3 * k + 3]) for k in range(n)]


def _allsum_kernel(nh, nw, cnt, mode, part_ref, par_ref, out_ref, mine, buf, lsem, send, recv):
    n = nh * nw
    w = lax.axis_index("w")
    h = lax.axis_index("x") * 2 + lax.axis_index("c")
    me = w * nh + h

    def dev(j):
        hh = j % nh
        return (j // nh, hh // 2, hh % 2)

    local = pltpu.make_async_copy(part_ref, mine, lsem)
    local.start()
    barrier = pltpu.get_barrier_semaphore()
    for k in range(1, n):
        pl.semaphore_signal(barrier, inc=1, device_id=dev(lax.rem(me + k, n)), device_id_type=MESH)
    local.wait()
    pl.semaphore_wait(barrier, n - 1)
    copies = []
    for k in range(1, n):
        cp = pltpu.make_async_remote_copy(src_ref=mine, dst_ref=buf.at[k - 1], send_sem=send.at[k - 1], recv_sem=recv.at[k - 1],
                                          device_id=dev(lax.rem(me + k, n)), device_id_type=MESH)
        cp.start()
        copies.append(cp)
    for cp in copies:
        cp.wait()
    total = None
    vals = [mine[...]] + [buf[k] for k in range(n - 1)]
    for j in range(n):
        t = jnp.zeros_like(vals[0])
        off = lax.rem(me - j + n, n)
        for k in range(n):
            t = t + jnp.where(off == k, vals[k], 0.0)
        total = t if total is None else total + t
    c = total.shape[-1]
    gi = jnp.floor((lax.broadcasted_iota(jnp.int32, (c, c), 0).astype(F32) + 0.5) * (GROUPS / c))
    gj = jnp.floor((lax.broadcasted_iota(jnp.int32, (c, c), 1).astype(F32) + 0.5) * (GROUPS / c))
    same = jnp.where(gi == gj, 1.0, 0.0).astype(F32)
    row = lax.broadcasted_iota(jnp.int32, (8, c), 0)
    if mode == 0:
        m = jnp.dot(total, same, precision=lax.Precision.HIGHEST, preferred_element_type=F32) / cnt
        mean, sq = m[0:1], m[1:2]
        rstd = lax.rsqrt(sq - mean * mean + EPS)
        out_ref[...] = jnp.where(row == 0, mean, jnp.where(row == 1, rstd, par_ref[...]))
    else:
        u = jnp.dot(total * par_ref[2:3], same, precision=lax.Precision.HIGHEST, preferred_element_type=F32) / cnt
        out_ref[...] = jnp.where(row == 0, total[0:1], jnp.where(row == 1, total[1:2], jnp.where(row == 2, u[0:1], u[1:2])))


def _allsum(nh, nw, cnt, mode, cid, part, par):
    c = part.shape[-1]
    n = nh * nw
    return pl.pallas_call(
        functools.partial(_allsum_kernel, nh, nw, cnt, mode), out_shape=jax.ShapeDtypeStruct((8, c), F32),
        in_specs=[ANY, VM], out_specs=VM,
        scratch_shapes=[pltpu.VMEM((8, c), F32), pltpu.VMEM((n - 1, 8, c), F32), pltpu.SemaphoreType.DMA,
                        pltpu.SemaphoreType.DMA((n - 1,)), pltpu.SemaphoreType.DMA((n - 1,))],
        compiler_params=pltpu.CompilerParams(collective_id=cid, has_side_effects=True, vmem_limit_bytes=VMEM_LIMIT),
        name=f"allsum{cid}",
    )(part, par)


def _load_patches(u_ref, rows_ref, p, sems):
    th, c = u_ref.shape[0], u_ref.shape[2]
    cps = [pltpu.make_async_copy(u_ref, p.at[1:th + 1, :, c:2 * c], sems.at[0]),
           pltpu.make_async_copy(rows_ref.at[0], p.at[0, :, c:2 * c], sems.at[1]),
           pltpu.make_async_copy(rows_ref.at[1], p.at[th + 1, :, c:2 * c], sems.at[2])]
    for cp in cps:
        cp.start()
    return cps


def _shift_patches(p, cl_ref, cr_ref, r0=0):
    n, tw, c3 = p.shape
    c = c3 // 3
    ck = 128

    def row(r, _):
        idx = lax.broadcasted_iota(jnp.int32, (tw, ck), 0)
        for k in range(c // ck):
            f = p[r, :, c + k * ck:c + (k + 1) * ck].astype(F32)
            lo = cl_ref[r0 + r, :, k * ck:(k + 1) * ck]
            hi = cr_ref[r0 + r, :, k * ck:(k + 1) * ck]
            p[r, :, k * ck:(k + 1) * ck] = jnp.where(idx == 0, lo, pltpu.roll(f, 1, 0)).astype(BF16)
            p[r, :, 2 * c + k * ck:2 * c + (k + 1) * ck] = jnp.where(idx == tw - 1, hi, pltpu.roll(f, tw - 1, 0)).astype(BF16)
        return 0

    lax.fori_loop(0, n, row, 0)


def _conv_kernel(rb, epilogue, u_ref, rows_ref, cl_ref, cr_ref, w_ref, *refs):
    outs = refs[:-4]
    p, wb, psem, wsem = refs[-4:]
    c = u_ref.shape[2]
    i = pl.program_id(0)

    @pl.when(i == 0)
    def _():
        cps = _load_patches(u_ref, rows_ref, p, psem)
        wc = pltpu.make_async_copy(w_ref, wb, wsem)
        wc.start()
        for cp in cps:
            cp.wait()
        _shift_patches(p, cl_ref, cr_ref)
        wc.wait()

    tw = p.shape[1]
    acc = None
    for a in range(3):
        lhs = p[pl.ds(i * rb + a, rb)].reshape(rb * tw, 3 * c)
        d = jnp.dot(lhs, wb[a], preferred_element_type=F32)
        acc = d if acc is None else acc + d
    epilogue(i, acc, (), outs)


def _conv(name, epilogue, u, halo, w, outs, out_specs, rb=2):
    th, tw, c = u.shape
    full = pl.BlockSpec((th + 2, 1, c), lambda i: (0, 0, 0), pipeline_mode=pl.Buffered(1))
    wshape = (3, 3 * c, c)
    return pl.pallas_call(
        functools.partial(_conv_kernel, rb, epilogue),
        grid=(th // rb,), out_shape=outs, in_specs=[ANY, ANY, full, full, ANY], out_specs=out_specs,
        scratch_shapes=[pltpu.VMEM((th + 2, tw, 3 * c), BF16), pltpu.VMEM(wshape, BF16), pltpu.SemaphoreType.DMA((3,)), pltpu.SemaphoreType.DMA],
        compiler_params=pltpu.CompilerParams(dimension_semantics=("arbitrary",), vmem_limit_bytes=VMEM_LIMIT),
        name=name,
    )(u, *halo, w.reshape(wshape))


def _add_sums(i, s0, s1, s_ref):
    row = lax.broadcasted_iota(jnp.int32, s_ref.shape, 0)
    s = jnp.where(row == 0, s0, jnp.where(row == 1, s1, 0.0))

    @pl.when(i == 0)
    def _():
        s_ref[...] = s

    @pl.when(i > 0)
    def _():
        s_ref[...] += s


def _ep_conv1(i, acc, extra, outs):
    a_ref, s_ref = outs
    a16 = acc.astype(BF16)
    a_ref[...] = a16.reshape(a_ref.shape)
    a = a16.astype(F32)
    s0 = a.sum(0, keepdims=True)
    s1 = (a * a).sum(0, keepdims=True)
    _add_sums(i, s0, s1, s_ref)


def _ep_residual(i, acc, extra, outs):
    o_ref = outs[0]
    r = extra[0][...].astype(F32).reshape(acc.shape)
    o_ref[...] = (acc + r).astype(BF16).reshape(o_ref.shape)


def _ep_dz(i, acc, extra, outs):
    a_ref, st_ref = extra
    dn_ref, s_ref = outs
    mean, rstd, gamma, beta = _params(st_ref)
    xhat = (a_ref[...].astype(F32).reshape(acc.shape) - mean) * rstd
    dn = acc * _gelu_grad(xhat * gamma + beta)
    dn_ref[...] = dn.reshape(dn_ref.shape)
    s0 = (dn * xhat).sum(0, keepdims=True)
    s1 = dn.sum(0, keepdims=True)
    _add_sums(i, s0, s1, s_ref)


def _params(st_ref):
    st = st_ref[...]
    return [st[k:k + 1] for k in range(4)]


def _edges(v, first_ref, last_ref):
    first_ref[...] = v[:, 0:1, :]
    last_ref[...] = v[:, v.shape[1] - 1:, :]


def _z_kernel(a_ref, st_ref, z_ref, first_ref, last_ref):
    mean, rstd, gamma, beta = _params(st_ref)
    xhat = (a_ref[...].astype(F32) - mean) * rstd
    z = _gelu(xhat * gamma + beta).astype(BF16)
    z_ref[...] = z
    _edges(z.astype(F32), first_ref, last_ref)


def _da_kernel(dn_ref, a_ref, st_ref, t_ref, o_ref, first_ref, last_ref):
    mean, rstd, gamma, _ = _params(st_ref)
    _, _, u0, u1 = _params(t_ref)
    xhat = (a_ref[...].astype(F32) - mean) * rstd
    da = (rstd * (dn_ref[...] * gamma - u1 - xhat * u0)).astype(BF16)
    o_ref[...] = da
    _edges(da.astype(F32), first_ref, last_ref)


def _fused_kernel(ticks, nu, ep_u, ep_v, n_xu, n_xv, n_ov, u_ref, urows, ucl, ucr, v_ref, vrows, vcl, vcr, w_ref, *refs):
    xu, refs = refs[:n_xu], refs[n_xu:]
    xv, refs = refs[:n_xv], refs[n_xv:]
    ou, refs = (refs[:1], refs[1:]) if nu else ((), refs)
    ov, refs = refs[:n_ov], refs[n_ov:]
    dw_ref, p, vt, wb, dsend, hown, recv0, recv1, recv2, psem, wsem, vsem, send, recv, lsem = refs
    i = pl.program_id(0)
    th, tw, c = u_ref.shape
    nt = w_ref.shape[0]
    half, q, e, sub = c // 2, c // 4, c // 8, c // 16
    wi, xi, ci = lax.axis_index("w"), lax.axis_index("x"), lax.axis_index("c")
    mate, xn, yn = (wi, xi, 1 - ci), (wi, 1 - xi, ci), (1 - wi, xi, ci)
    pa, pb = xi * e, q + wi * e
    fa, fb = pa + wi * sub, pb + xi * sub

    def rows(start, n):
        return pl.ds(pl.multiple_of(start, 8), n)

    def rc(stage, t, src, dst, dev):
        return pltpu.make_async_remote_copy(src_ref=src, dst_ref=dst, send_sem=send.at[stage, t], recv_sem=recv.at[stage, t],
                                            device_id=dev, device_id_type=MESH)

    def base(t):
        return t * c + ci * half

    def s0(t):
        return [rc(0, t, dsend.at[lax.rem(t, 2)], recv0.at[lax.rem(t, 2)], mate)]

    def s1(t):
        return [rc(1, t, hown.at[t, rows((1 - xi) * e, e)], recv1.at[t, 0], xn),
                rc(2, t, hown.at[t, rows(q + (1 - wi) * e, e)], recv1.at[t, 1], yn)]

    def s2(t):
        return [rc(3, t, hown.at[t, rows(pa + (1 - wi) * sub, sub)], recv2.at[t, 0], yn),
                rc(4, t, hown.at[t, rows(pb + (1 - xi) * sub, sub)], recv2.at[t, 1], xn)]

    def s3(t):
        return [rc(5, t, hown.at[t, rows(fa, sub)], dw_ref.at[rows(base(t) + fa, sub)], yn),
                rc(6, t, hown.at[t, rows(fb, sub)], dw_ref.at[rows(base(t) + fb, sub)], xn)]

    def keep(t):
        return [pltpu.make_async_copy(hown.at[t, rows(fa, sub)], dw_ref.at[rows(base(t) + fa, sub)], lsem.at[0, t]),
                pltpu.make_async_copy(hown.at[t, rows(fb, sub)], dw_ref.at[rows(base(t) + fb, sub)], lsem.at[1, t])]

    def s4(t):
        return [rc(7, t, dw_ref.at[rows(base(t) + pa, e)], dw_ref.at[rows(base(t) + pa, e)], xn),
                rc(8, t, dw_ref.at[rows(base(t) + pb, e)], dw_ref.at[rows(base(t) + pb, e)], yn)]

    def s5(t):
        return [rc(9, t, dw_ref.at[rows(base(t), half)], dw_ref.at[rows(base(t), half)], mate)]

    def start(cps):
        for cp in cps:
            cp.start()

    def when_chunk(t, f):
        @pl.when(jnp.logical_and(t >= 0, t < nt))
        def _():
            f(t)

    def tick(j):
        def t2(t):
            for cp in s1(t):
                cp.wait_recv()
            hown[t, rows(pa, e), :] += recv1[t, 0]
            hown[t, rows(pb, e), :] += recv1[t, 1]

        def t3(t):
            for cp in s2(t):
                cp.wait_recv()
            hown[t, rows(fa, sub), :] += recv2[t, 0]
            hown[t, rows(fb, sub), :] += recv2[t, 1]

        def t4(t):
            for cp in s3(t):
                cp.wait_recv()
            for cp in keep(t):
                cp.wait()
            start(s4(t))

        def t5(t):
            for cp in s4(t):
                cp.wait_recv()
            start(s5(t))

        def t6(t):
            for cp in s5(t):
                cp.wait_recv()
            for cp in s1(t) + s2(t) + s3(t) + s4(t) + s5(t):
                cp.wait_send()

        lag = 2
        when_chunk(j, lambda t: start(s1(t)))
        when_chunk(j - lag, t2)
        when_chunk(j - 2 * lag, t3)
        when_chunk(j - 3 * lag, t4)
        when_chunk(j - 4 * lag, t5)
        when_chunk(j - lag, lambda t: start(s2(t)))
        when_chunk(j - 2 * lag, lambda t: start(s3(t) + keep(t)))
        when_chunk(j - 5 * lag, t6)

    wcp = pltpu.make_async_copy(w_ref, wb, wsem)

    @pl.when(i == 0)
    def _():
        vc = pltpu.make_async_copy(v_ref, p.at[1:th + 1, :, 0:c], vsem)
        vc.start()
        cps = _load_patches(u_ref, urows, p, psem)
        wcp.start()
        barrier = pltpu.get_barrier_semaphore()
        for d in (mate, xn, yn):
            pl.semaphore_signal(barrier, inc=1, device_id=d, device_id_type=MESH)
        pl.semaphore_wait(barrier, 3)
        vc.wait()

        def tr(r, _):
            vt[:, pl.ds(pl.multiple_of(r * tw, tw), tw)] = p[r + 1, :, 0:c].T
            return 0

        lax.fori_loop(0, th, tr, 0)
        for cp in cps:
            cp.wait()
        _shift_patches(p, ucl, ucr)

    @pl.when(jnp.logical_and(i >= 2, i < nt + 2))
    def _():
        t = i - 2
        for cp in s0(t):
            cp.wait()
        hown[t] += recv0[lax.rem(t, 2)]

    @pl.when(jnp.logical_and(i >= 1, i < nt + 1))
    def _():
        start(s0(i - 1))

    @pl.when(i == nt)
    def _():
        wcp.wait()

    @pl.when(i == nt + nu)
    def _():
        cps = _load_patches(v_ref, vrows, p, psem)
        for cp in cps:
            cp.wait()
        _shift_patches(p, vcl, vcr)

    j = jnp.int32(-1)
    now = jnp.int32(0)
    for s in ticks:
        j = j + jnp.where(i >= s, 1, 0)
        now = now + jnp.where(i == s, 1, 0)

    @pl.when(now > 0)
    def _():
        tick(j)

    @pl.when(i < nt)
    def _():
        a = lax.div(i, 3)
        b = lax.rem(i, 3)
        rhs = p[pl.ds(a, th), :, pl.ds(pl.multiple_of(b * c, 128), c)].reshape(th * tw, c)
        d = jnp.dot(vt[...], rhs, preferred_element_type=F32).T
        hown[i] = jnp.where(ci == 0, d[:half], d[half:])
        dsend[lax.rem(i, 2)] = jnp.where(ci == 0, d[half:], d[:half])

    def conv(ib, transposed):
        acc = None
        for a in range(3):
            lhs = p[pl.ds(ib * 2 + a, 2)].reshape(2 * tw, 3 * c)
            if transposed:
                k = nt - 1 - 3 * a
                rhs = jnp.concatenate([wb[k], wb[k - 1], wb[k - 2]], axis=1)
                d = lax.dot_general(lhs, rhs, (((1,), (1,)), ((), ())), preferred_element_type=F32)
            else:
                d = jnp.dot(lhs, wb[3 * a:3 * a + 3].reshape(3 * c, c), preferred_element_type=F32)
            acc = d if acc is None else acc + d
        return acc

    if nu:
        @pl.when(jnp.logical_and(i >= nt, i < nt + nu))
        def _():
            ep_u(i - nt, conv(i - nt, False), xu, ou)

    @pl.when(jnp.logical_and(i >= nt + nu, i < nt + nu + th // 2))
    def _():
        ib = i - nt - nu
        ep_v(ib, conv(ib, True), xv, ov)


def _fused(name, cid, steps, ticks, u, uh, v, vh, w, nu, ep_u, xu, ep_v, xv, outs_v):
    th, tw, c = u.shape
    nt, half = 9, c // 2
    last = th // 2 - 1
    full = pl.BlockSpec((th + 2, 1, c), lambda i: (0, 0, 0), pipeline_mode=pl.Buffered(1))
    small = pl.BlockSpec((8, c), lambda i: (0, 0))
    ub = pl.BlockSpec((2, tw, c), lambda i: (jnp.minimum(jnp.maximum(i - nt, 0), nu - 1), 0, 0))
    vb = pl.BlockSpec((2, tw, c), lambda i: (jnp.minimum(jnp.maximum(i - nt - nu, 0), last), 0, 0))
    img = [ANY, ANY, full, full]
    dma = pltpu.SemaphoreType.DMA
    out_u = [jax.ShapeDtypeStruct((2 * nu, tw, c), BF16)] if nu else []
    call = pl.pallas_call(
        functools.partial(_fused_kernel, ticks, nu, ep_u, ep_v, len(xu), len(xv), len(outs_v)), grid=(steps,),
        out_shape=out_u + [o for o, _ in outs_v] + [jax.ShapeDtypeStruct((nt * c, c), F32)],
        in_specs=img + img + [ANY] + [ub for _ in xu] + [vb if b else small for _, b in xv],
        out_specs=[ub for _ in out_u] + [vb if b else small for _, b in outs_v] + [ANY],
        scratch_shapes=[pltpu.VMEM((th + 2, tw, 3 * c), BF16), pltpu.VMEM((c, th * tw), BF16), pltpu.VMEM((nt, c, c), BF16),
                        pltpu.VMEM((2, half, c), F32), pltpu.VMEM((nt, half, c), F32), pltpu.VMEM((2, half, c), F32),
                        pltpu.VMEM((nt, 2, c // 8, c), F32), pltpu.VMEM((nt, 2, c // 16, c), F32),
                        dma((3,)), dma, dma, dma((10, nt)), dma((10, nt)), dma((2, nt))],
        compiler_params=pltpu.CompilerParams(dimension_semantics=("arbitrary",), vmem_limit_bytes=VMEM_LIMIT, collective_id=cid, has_side_effects=True),
        name=name,
    )
    return call(u, *uh, v, *vh, w.reshape(nt, c, c), *[x for x, _ in xu], *[x for x, _ in xv])


def _finish_kernel(u_ref, rows_ref, cl_ref, cr_ref, w_ref, x_ref, y0_ref, dx0_ref, d1_ref, d2_ref,
                   y_ref, dx_ref, dw1_ref, dw2_ref, p, wb, yb, by, bx, b1, b2, psem, wsem, ysem, insem, outsem):
    i = pl.program_id(0)
    steps = pl.num_programs(0)
    th, tw, c = u_ref.shape
    r0 = th - steps
    slot = lax.rem(i, 2)
    moves = [(y0_ref, by, y_ref), (dx0_ref, bx, dx_ref), (d1_ref, b1, dw1_ref), (d2_ref, b2, dw2_ref)]

    def ins(k):
        out = []
        for m, (src, buf, _) in enumerate(moves):
            n = buf.shape[1]
            out.append(pltpu.make_async_copy(src.at[pl.ds(k * n, n)], buf.at[lax.rem(k, 2)], insem.at[m, lax.rem(k, 2)]))
        return out

    def outs(k):
        out = []
        for m, (_, buf, dst) in enumerate(moves):
            n = buf.shape[1]
            out.append(pltpu.make_async_copy(buf.at[lax.rem(k, 2)], dst.at[pl.ds(k * n, n)], outsem.at[m, lax.rem(k, 2)]))
        return out

    def yout(k):
        return pltpu.make_async_copy(yb.at[lax.rem(k, 2)], y_ref.at[r0 + k], ysem.at[lax.rem(k, 2)])

    def each(cps, f):
        for cp in cps:
            f(cp)

    start, wait = (lambda cp: cp.start()), (lambda cp: cp.wait())

    @pl.when(i == 0)
    def _():
        n = th - r0 + 1
        cps = [pltpu.make_async_copy(u_ref.at[r0 - 1:], p.at[:n, :, c:2 * c], psem.at[0]),
               pltpu.make_async_copy(rows_ref.at[1], p.at[n, :, c:2 * c], psem.at[1])]
        wc = pltpu.make_async_copy(w_ref, wb, wsem)
        each(cps + [wc], start)
        each(ins(i), start)
        each(cps, wait)
        _shift_patches(p, cl_ref, cr_ref, r0)
        wc.wait()

    each(ins(i), wait)
    each(outs(i), start)

    @pl.when(i > 0)
    def _():
        each(outs(i - 1), wait)

    @pl.when(i + 1 < steps)
    def _():
        each(ins(i + 1), start)

    acc = None
    for a in range(3):
        d = jnp.dot(p[i + a], wb[a], preferred_element_type=F32)
        acc = d if acc is None else acc + d

    @pl.when(i > 1)
    def _():
        yout(i - 2).wait()

    yb[slot] = (acc + x_ref[0].astype(F32)).astype(BF16)
    yout(i).start()

    @pl.when(i == steps - 1)
    def _():
        yout(i - 1).wait()
        yout(i).wait()
        each(outs(i), wait)


def _finish(u, halo, w, x, y0, dx0, d1, d2):
    th, tw, c = u.shape
    r0 = y0.shape[0]
    steps = th - r0
    full = pl.BlockSpec((th + 2, 1, c), lambda i: (0, 0, 0), pipeline_mode=pl.Buffered(1))
    wshape = (3, 3 * c, c)
    dma = pltpu.SemaphoreType.DMA
    raw = (y0, dx0, d1, d2)

    def buf(v):
        return pltpu.VMEM((2, v.shape[0] // steps) + v.shape[1:], v.dtype)

    return pl.pallas_call(
        _finish_kernel, grid=(steps,),
        out_shape=[jax.ShapeDtypeStruct((th, tw, c), BF16)] + [jax.ShapeDtypeStruct(v.shape, v.dtype) for v in raw[1:]],
        in_specs=[ANY, ANY, full, full, ANY, pl.BlockSpec((1, tw, c), lambda i: (r0 + i, 0, 0))] + [ANY] * 4, out_specs=[ANY] * 4,
        scratch_shapes=[pltpu.VMEM((steps + 2, tw, 3 * c), BF16), pltpu.VMEM(wshape, BF16), pltpu.VMEM((2, tw, c), BF16)] + [buf(v) for v in raw]
        + [dma((2,)), dma, dma((2,)), dma((4, 2)), dma((4, 2))],
        compiler_params=pltpu.CompilerParams(dimension_semantics=("arbitrary",), vmem_limit_bytes=VMEM_LIMIT),
        name="finish",
    )(u, *halo, w.reshape(wshape), x, *raw)


def solution(mesh):
    nh, nw = mesh.shape["h"], mesh.shape["w"]
    mesh3 = Mesh(mesh.devices.reshape(nw, nh // 2, 2), ("w", "x", "c"))
    tile = P(None, ("x", "c"), "w", None)

    def body(x, w1, gamma, beta, w2, g):
        _, th, tw, c = x.shape
        x, g = x[0], g[0]
        cnt = float(th * nh * tw * nw * (c // GROUPS))
        rb = 2
        blk = pl.BlockSpec((rb, tw, c), lambda i: (i, 0, 0))
        small = pl.BlockSpec((8, c), lambda i: (0, 0))
        img16 = jax.ShapeDtypeStruct((th, tw, c), BF16)
        img32 = jax.ShapeDtypeStruct((th, tw, c), F32)
        sums = jax.ShapeDtypeStruct((8, c), F32)
        par = jnp.concatenate([jnp.zeros((2, c), F32), gamma[None], beta[None], jnp.zeros((4, c), F32)])

        edge = jax.ShapeDtypeStruct((th, 1, c), F32)
        eblk = pl.BlockSpec((rb, 1, c), lambda i: (i, 0, 0))

        def with_edges(u):
            return u, u[:, 0:1, :].astype(F32), u[:, tw - 1:, :].astype(F32)

        xh, gh = _halo(nh, nw, 0, *with_edges(x), *with_edges(g))
        a, s = _conv("conv1", _ep_conv1, x, xh, w1, [img16, sums], [blk, small])
        st = _allsum(nh, nw, cnt, 0, 1, s, par)
        z, z0, z1 = pl.pallas_call(_z_kernel, grid=(th // rb,), out_shape=[img16, edge, edge], in_specs=[blk, small], out_specs=[blk, eblk, eblk], name="act")(a, st)
        (zh,) = _halo(nh, nw, 2, z, z0, z1)
        y, dn, t, dw2 = _fused("mid", 5, 24, (*range(2, 9), *range(10, 15, 2), *range(15, 24)), z, zh, g, gh, w2, 4, _ep_residual, [(x, True)],
                               _ep_dz, [(a, True), (st, False)], [(img32, True), (sums, False)])
        t = _allsum(nh, nw, cnt, 1, 3, t, st)
        da, da0, da1 = pl.pallas_call(_da_kernel, grid=(th // rb,), out_shape=[img16, edge, edge], in_specs=[blk, blk, small, small], out_specs=[blk, eblk, eblk], name="da")(dn, a, st, t)
        (dah,) = _halo(nh, nw, 4, da, da0, da1)
        dx, dw1 = _fused("tail", 6, 25, (*range(2, 9), *range(10, 15, 2), *range(16, 25)), x, xh, da, dah, w1, 0, None, [],
                         _ep_residual, [(g, True)], [(img16, True)])
        y, dx, dw1, dw2 = _finish(z, zh, w2, x, y, dx, dw1, dw2)
        return y[None], dx[None], dw1.reshape(w1.shape), dw2.reshape(w2.shape), t[0], t[1]

    return jax.shard_map(body, mesh=mesh3, in_specs=(tile, P(), P(), P(), P(), tile), out_specs=(tile, tile, P(), P(), P(), P()), check_vma=False)
```

```python
import functools

import jax
import jax.numpy as jnp
from jax import lax
from jax.experimental import pallas as pl
from jax.experimental.pallas import tpu as pltpu
from jax.sharding import Mesh
from jax.sharding import PartitionSpec as P

GROUPS = 32
EPS = 1e-5
F32 = jnp.float32
BF16 = jnp.bfloat16
MESH = pl.DeviceIdType.MESH
VMEM_LIMIT = 61 * 1024 * 1024
ANY = pl.BlockSpec(memory_space=pl.ANY)
VM = pl.BlockSpec(memory_space=pltpu.VMEM)
GELU_C = 0.7978845608028654
GELU_A = 0.044715


def _gelu_parts(n):
    n2 = n * n
    t = jnp.tanh(GELU_C * (n + GELU_A * n * n2))
    return n2, t


def _gelu(n):
    _, t = _gelu_parts(n)
    return 0.5 * n * (1.0 + t)


def _gelu_grad(n):
    n2, t = _gelu_parts(n)
    return 0.5 * (1.0 + t) + 0.5 * n * (1.0 - t * t) * (GELU_C * (1.0 + 3.0 * GELU_A * n2))


def _exchange(nh, nw, arrays, send, recv):
    th, tw, c = arrays[0][0].shape
    w = lax.axis_index("w")
    h = lax.axis_index("x") * 2 + lax.axis_index("c")
    dirs = [(dh, dw) for dh in (-1, 0, 1) for dw in (-1, 0, 1) if (dh, dw) != (0, 0)]
    sends = [(k, i, dh, dw) for k in range(len(arrays)) for i, (dh, dw) in enumerate(dirs)]

    def dev(dh, dw):
        hh = h + dh
        return (w + dw, hh // 2, hh % 2)

    def has(dh, dw):
        ok = None
        for cond in ([h > 0] if dh < 0 else [h < nh - 1] if dh > 0 else []) + ([w > 0] if dw < 0 else [w < nw - 1] if dw > 0 else []):
            ok = cond if ok is None else jnp.logical_and(ok, cond)
        return ok

    def announce(barrier):
        for d in dirs:
            @pl.when(has(*d))
            def _(d=d):
                pl.semaphore_signal(barrier, inc=1, device_id=dev(*d), device_id_type=MESH)
        one = jnp.int32(1)
        zero = jnp.int32(0)
        nv = one + jnp.where(h > 0, one, zero) + jnp.where(h < nh - 1, one, zero)
        nz = one + jnp.where(w > 0, one, zero) + jnp.where(w < nw - 1, one, zero)
        return nv * nz - 1

    def landing(k, dh, dw):
        rows, cl, cr = arrays[k][3:]
        side = cr if dw < 0 else cl
        if dw == 0:
            return rows, 1 if dh < 0 else 0
        if dh == 0:
            return side, slice(1, th + 1)
        return side, th + 1 if dh < 0 else 0

    def copy(k, i, dh, dw):
        u, first, last = arrays[k][:3]
        r = 0 if dh < 0 else th - 1
        edge = first if dw < 0 else last
        src = u.at[r] if dw == 0 else edge if dh == 0 else edge.at[r]
        ref, at = landing(k, dh, dw)
        return pltpu.make_async_remote_copy(src_ref=src, dst_ref=ref.at[at], send_sem=send.at[k * 8 + i], recv_sem=recv.at[k * 8 + i],
                                            device_id=dev(dh, dw), device_id_type=MESH)

    def start():
        for k, i, dh, dw in sends:
            @pl.when(has(dh, dw))
            def _(k=k, i=i, dh=dh, dw=dw):
                copy(k, i, dh, dw).start()

    def finish():
        for k, i, dh, dw in sends:
            @pl.when(jnp.logical_not(has(-dh, -dw)))
            def _(k=k, dh=dh, dw=dw):
                ref, at = landing(k, dh, dw)
                ref[at] = jnp.zeros(ref.at[at].shape, ref.dtype)

            @pl.when(has(dh, dw))
            def _(k=k, i=i, dh=dh, dw=dw):
                copy(k, i, dh, dw).wait_send()

            @pl.when(has(-dh, -dw))
            def _(k=k, i=i, dh=dh, dw=dw):
                copy(k, i, dh, dw).wait_recv()

    return announce, start, finish


def _halo_kernel(nh, nw, n_arr, *refs):
    ins = refs[:3 * n_arr]
    outs = refs[3 * n_arr:6 * n_arr]
    announce, start, finish = _exchange(nh, nw, [ins[3 * k:3 * k + 3] + outs[3 * k:3 * k + 3] for k in range(n_arr)], *refs[6 * n_arr:])
    barrier = pltpu.get_barrier_semaphore()
    pl.semaphore_wait(barrier, announce(barrier))
    start()
    finish()


def _halo(nh, nw, cid, *us):
    th, tw, c = us[0].shape
    n = len(us) // 3
    out = []
    for _ in range(n):
        out += [jax.ShapeDtypeStruct((2, tw, c), BF16), jax.ShapeDtypeStruct((th + 2, 1, c), F32), jax.ShapeDtypeStruct((th + 2, 1, c), F32)]
    res = pl.pallas_call(
        functools.partial(_halo_kernel, nh, nw, n), out_shape=out, in_specs=[ANY] * (3 * n), out_specs=[VM] * (3 * n),
        scratch_shapes=[pltpu.SemaphoreType.DMA((8 * n,)), pltpu.SemaphoreType.DMA((8 * n,))],
        compiler_params=pltpu.CompilerParams(collective_id=cid, has_side_effects=True, vmem_limit_bytes=VMEM_LIMIT),
        name=f"halo{cid}",
    )(*us)
    return [tuple(res[3 * k:3 * k + 3]) for k in range(n)]


def _allsum_kernel(nh, nw, cnt, mode, part_ref, par_ref, out_ref, mine, buf, same, lsem, send, recv):
    n = nh * nw
    w = lax.axis_index("w")
    h = lax.axis_index("x") * 2 + lax.axis_index("c")
    me = w * nh + h

    def dev(j):
        hh = j % nh
        return (j // nh, hh // 2, hh % 2)

    local = pltpu.make_async_copy(part_ref, mine, lsem)
    local.start()
    c = mine.shape[-1]
    gi = jnp.floor((lax.broadcasted_iota(jnp.int32, (c, c), 0).astype(F32) + 0.5) * (GROUPS / c))
    gj = jnp.floor((lax.broadcasted_iota(jnp.int32, (c, c), 1).astype(F32) + 0.5) * (GROUPS / c))
    same[...] = jnp.where(gi == gj, 1.0, 0.0).astype(BF16)

    def group_means(v):
        hi = v.astype(BF16)
        rest = v - hi.astype(F32)
        mid = rest.astype(BF16)
        lo = (rest - mid.astype(F32)).astype(BF16)
        return sum(jnp.dot(x, same[...], preferred_element_type=F32) for x in (lo, mid, hi)) / cnt

    barrier = pltpu.get_barrier_semaphore()
    for k in range(1, n):
        pl.semaphore_signal(barrier, inc=1, device_id=dev(lax.rem(me + k, n)), device_id_type=MESH)
    local.wait()
    pl.semaphore_wait(barrier, n - 1)
    copies = []
    for k in range(1, n):
        cp = pltpu.make_async_remote_copy(src_ref=mine, dst_ref=buf.at[k - 1], send_sem=send.at[k - 1], recv_sem=recv.at[k - 1],
                                          device_id=dev(lax.rem(me + k, n)), device_id_type=MESH)
        cp.start()
        copies.append(cp)
    for cp in copies:
        cp.wait()
    total = None
    vals = [mine[...]] + [buf[k] for k in range(n - 1)]
    for j in range(n):
        t = jnp.zeros_like(vals[0])
        off = lax.rem(me - j + n, n)
        for k in range(n):
            t = t + jnp.where(off == k, vals[k], 0.0)
        total = t if total is None else total + t
    row = lax.broadcasted_iota(jnp.int32, (8, c), 0)
    if mode == 0:
        m = group_means(total)
        mean, sq = m[0:1], m[1:2]
        rstd = lax.rsqrt(sq - mean * mean + EPS)
        out_ref[...] = jnp.where(row == 0, mean, jnp.where(row == 1, rstd, par_ref[...]))
    else:
        u = group_means(total * par_ref[2:3])
        out_ref[...] = jnp.where(row == 0, total[0:1], jnp.where(row == 1, total[1:2], jnp.where(row == 2, u[0:1], u[1:2])))


def _allsum(nh, nw, cnt, mode, cid, part, par):
    c = part.shape[-1]
    n = nh * nw
    return pl.pallas_call(
        functools.partial(_allsum_kernel, nh, nw, cnt, mode), out_shape=jax.ShapeDtypeStruct((8, c), F32),
        in_specs=[ANY, VM], out_specs=VM,
        scratch_shapes=[pltpu.VMEM((8, c), F32), pltpu.VMEM((n - 1, 8, c), F32), pltpu.VMEM((c, c), BF16), pltpu.SemaphoreType.DMA,
                        pltpu.SemaphoreType.DMA((n - 1,)), pltpu.SemaphoreType.DMA((n - 1,))],
        compiler_params=pltpu.CompilerParams(collective_id=cid, has_side_effects=True, vmem_limit_bytes=VMEM_LIMIT),
        name=f"allsum{cid}",
    )(part, par)


def _load_patches(u_ref, rows_ref, p, sems):
    th, c = u_ref.shape[0], u_ref.shape[2]
    cps = [pltpu.make_async_copy(u_ref, p.at[1:th + 1, :, c:2 * c], sems.at[0]),
           pltpu.make_async_copy(rows_ref.at[0], p.at[0, :, c:2 * c], sems.at[1]),
           pltpu.make_async_copy(rows_ref.at[1], p.at[th + 1, :, c:2 * c], sems.at[2])]
    for cp in cps:
        cp.start()
    return cps


def _shift_patches(p, cl_ref, cr_ref, r0=0):
    n, tw, c3 = p.shape
    c = c3 // 3
    ck = 128

    def row(r, _):
        idx = lax.broadcasted_iota(jnp.int32, (tw, ck), 0)
        for k in range(c // ck):
            f = p[r, :, c + k * ck:c + (k + 1) * ck].astype(F32)
            lo = cl_ref[r0 + r, :, k * ck:(k + 1) * ck]
            hi = cr_ref[r0 + r, :, k * ck:(k + 1) * ck]
            p[r, :, k * ck:(k + 1) * ck] = jnp.where(idx == 0, lo, pltpu.roll(f, 1, 0)).astype(BF16)
            p[r, :, 2 * c + k * ck:2 * c + (k + 1) * ck] = jnp.where(idx == tw - 1, hi, pltpu.roll(f, tw - 1, 0)).astype(BF16)
        return 0

    lax.fori_loop(0, n, row, 0)


def _transposed(v):
    return v.reshape(v.shape[0] * v.shape[1], v.shape[2]).T


def _conv_kernel(rb, epilogue, u_ref, rows_ref, cl_ref, cr_ref, w_ref, v_ref, vt_ref, *refs):
    outs = refs[:-4]
    p, wb, psem, wsem = refs[-4:]
    c = u_ref.shape[2]
    i = pl.program_id(0)

    @pl.when(i == 0)
    def _():
        cps = _load_patches(u_ref, rows_ref, p, psem)
        wc = pltpu.make_async_copy(w_ref, wb, wsem)
        wc.start()
        for cp in cps:
            cp.wait()
        _shift_patches(p, cl_ref, cr_ref)
        wc.wait()

    vt_ref[...] = _transposed(v_ref[...])
    tw = p.shape[1]
    acc = None
    for a in range(3):
        lhs = p[pl.ds(i * rb + a, rb)].reshape(rb * tw, 3 * c)
        d = jnp.dot(lhs, wb[a], preferred_element_type=F32)
        acc = d if acc is None else acc + d
    epilogue(i, acc, (), outs)


def _conv(name, epilogue, u, halo, w, v, outs, out_specs, rb=2):
    th, tw, c = u.shape
    full = pl.BlockSpec((th + 2, 1, c), lambda i: (0, 0, 0), pipeline_mode=pl.Buffered(1))
    wshape = (3, 3 * c, c)
    return pl.pallas_call(
        functools.partial(_conv_kernel, rb, epilogue),
        grid=(th // rb,), out_shape=[jax.ShapeDtypeStruct((c, th * tw), BF16)] + outs, in_specs=[ANY, ANY, full, full, ANY, out_specs[0]],
        out_specs=[pl.BlockSpec((c, rb * tw), lambda i: (0, i))] + out_specs,
        scratch_shapes=[pltpu.VMEM((th + 2, tw, 3 * c), BF16), pltpu.VMEM(wshape, BF16), pltpu.SemaphoreType.DMA((3,)), pltpu.SemaphoreType.DMA],
        compiler_params=pltpu.CompilerParams(dimension_semantics=("arbitrary",), vmem_limit_bytes=VMEM_LIMIT),
        name=name,
    )(u, *halo, w.reshape(wshape), v)


def _add_sums(i, s0, s1, s_ref):
    row = lax.broadcasted_iota(jnp.int32, s_ref.shape, 0)
    s = jnp.where(row == 0, s0, jnp.where(row == 1, s1, 0.0))

    @pl.when(i == 0)
    def _():
        s_ref[...] = s

    @pl.when(i > 0)
    def _():
        s_ref[...] += s


def _ep_conv1(i, acc, extra, outs):
    a_ref, s_ref = outs
    a16 = acc.astype(BF16)
    a_ref[...] = a16.reshape(a_ref.shape)
    a = a16.astype(F32)
    s0 = a.sum(0, keepdims=True)
    s1 = (a * a).sum(0, keepdims=True)
    _add_sums(i, s0, s1, s_ref)


def _ep_residual(i, acc, extra, outs):
    o_ref = outs[0]
    r = extra[0][...].astype(F32).reshape(acc.shape)
    o_ref[...] = (acc + r).astype(BF16).reshape(o_ref.shape)


def _ep_dz(i, acc, extra, outs):
    a_ref, st_ref = extra
    dn_ref, s_ref = outs
    mean, rstd, gamma, beta = _params(st_ref)
    xhat = (a_ref[...].astype(F32).reshape(acc.shape) - mean) * rstd
    dn = acc * _gelu_grad(xhat * gamma + beta)
    dn_ref[...] = dn.reshape(dn_ref.shape)
    s0 = (dn * xhat).sum(0, keepdims=True)
    s1 = dn.sum(0, keepdims=True)
    _add_sums(i, s0, s1, s_ref)


def _params(st_ref):
    st = st_ref[...]
    return [st[k:k + 1] for k in range(4)]


def _edges(v, first_ref, last_ref):
    first_ref[...] = v[:, 0:1, :]
    last_ref[...] = v[:, v.shape[1] - 1:, :]


def _z_kernel(a_ref, st_ref, z_ref, first_ref, last_ref):
    mean, rstd, gamma, beta = _params(st_ref)
    xhat = (a_ref[...].astype(F32) - mean) * rstd
    z = _gelu(xhat * gamma + beta).astype(BF16)
    z_ref[...] = z
    _edges(z.astype(F32), first_ref, last_ref)


def _copy_kernel(*refs):
    n = len(refs) // 2
    for src, dst in zip(refs[:n], refs[n:]):
        dst[...] = src[...]


def _da_kernel(dn_ref, a_ref, st_ref, t_ref, y0_ref, w0_ref, o_ref, ot_ref, first_ref, last_ref, y_ref, w_ref):
    _copy_kernel(y0_ref, w0_ref, y_ref, w_ref)
    mean, rstd, gamma, _ = _params(st_ref)
    _, _, u0, u1 = _params(t_ref)
    xhat = (a_ref[...].astype(F32) - mean) * rstd
    da = (rstd * (dn_ref[...] * gamma - u1 - xhat * u0)).astype(BF16)
    o_ref[...] = da
    ot_ref[...] = _transposed(da)
    _edges(da.astype(F32), first_ref, last_ref)


def _fused_kernel(nh, nw, own_u, ticks, nu, ep_u, ep_v, n_xu, n_xv, n_ov, u_ref, v_ref, vt_ref, first_ref, last_ref, rows_ref, cl_ref, cr_ref, w_ref, *refs):
    xu, refs = refs[:n_xu], refs[n_xu:]
    xv, refs = refs[:n_xv], refs[n_xv:]
    ou, refs = (refs[:1], refs[1:]) if nu else ((), refs)
    ov, refs = refs[:n_ov], refs[n_ov:]
    dw_ref, p, vt, wb, dsend, hown, recv0, recv1, recv2, erows, ecl, ecr, psem, wsem, vsem, send, recv, lsem, esend, erecv = refs
    i = pl.program_id(0)
    th, tw, c = u_ref.shape
    nt = w_ref.shape[0]
    half, q, e, sub = c // 2, c // 4, c // 8, c // 16
    wi, xi, ci = lax.axis_index("w"), lax.axis_index("x"), lax.axis_index("c")
    mate, xn, yn = (wi, xi, 1 - ci), (wi, 1 - xi, ci), (1 - wi, xi, ci)
    pa, pb = xi * e, q + wi * e
    fa, fb = pa + wi * sub, pb + xi * sub

    def rows(start, n):
        return pl.ds(pl.multiple_of(start, 8), n)

    def rc(stage, t, src, dst, dev):
        return pltpu.make_async_remote_copy(src_ref=src, dst_ref=dst, send_sem=send.at[stage, t], recv_sem=recv.at[stage, t],
                                            device_id=dev, device_id_type=MESH)

    def tap(t):
        return lax.rem(2 * lax.rem(t, 3) + 1, 3), lax.rem(2 * lax.div(t, 3) + 1, 3)

    def base(t):
        a, b = tap(t)
        return (a * 3 + b) * c + ci * half

    def s0(t):
        return [rc(0, t, dsend.at[lax.rem(t, 2)], recv0.at[lax.rem(t, 2)], mate)]

    def s1(t):
        return [rc(1, t, hown.at[t, rows((1 - xi) * e, e)], recv1.at[t, 0], xn),
                rc(2, t, hown.at[t, rows(q + (1 - wi) * e, e)], recv1.at[t, 1], yn)]

    def s2(t):
        return [rc(3, t, hown.at[t, rows(pa + (1 - wi) * sub, sub)], recv2.at[t, 0], yn),
                rc(4, t, hown.at[t, rows(pb + (1 - xi) * sub, sub)], recv2.at[t, 1], xn)]

    def s3(t):
        return [rc(5, t, hown.at[t, rows(fa, sub)], dw_ref.at[rows(base(t) + fa, sub)], yn),
                rc(6, t, hown.at[t, rows(fb, sub)], dw_ref.at[rows(base(t) + fb, sub)], xn)]

    def keep(t):
        return [pltpu.make_async_copy(hown.at[t, rows(fa, sub)], dw_ref.at[rows(base(t) + fa, sub)], lsem.at[0, t]),
                pltpu.make_async_copy(hown.at[t, rows(fb, sub)], dw_ref.at[rows(base(t) + fb, sub)], lsem.at[1, t])]

    def s4(t):
        return [rc(7, t, dw_ref.at[rows(base(t) + pa, e)], dw_ref.at[rows(base(t) + pa, e)], xn),
                rc(8, t, dw_ref.at[rows(base(t) + pb, e)], dw_ref.at[rows(base(t) + pb, e)], yn)]

    def s5(t):
        return [rc(9, t, dw_ref.at[rows(base(t), half)], dw_ref.at[rows(base(t), half)], mate)]

    def start(cps):
        for cp in cps:
            cp.start()

    def when_chunk(t, f):
        @pl.when(jnp.logical_and(t >= 0, t < nt))
        def _():
            f(t)

    def tick(j):
        def t2(t):
            for cp in s1(t):
                cp.wait_recv()
            hown[t, rows(pa, e), :] += recv1[t, 0]
            hown[t, rows(pb, e), :] += recv1[t, 1]

        def t3(t):
            for cp in s2(t):
                cp.wait_recv()
            hown[t, rows(fa, sub), :] += recv2[t, 0]
            hown[t, rows(fb, sub), :] += recv2[t, 1]

        def t4(t):
            for cp in s3(t):
                cp.wait_recv()
            for cp in keep(t):
                cp.wait()
            start(s4(t))

        def t5(t):
            for cp in s4(t):
                cp.wait_recv()
            start(s5(t))

        def t6(t):
            for cp in s5(t):
                cp.wait_recv()
            for cp in s1(t) + s2(t) + s3(t) + s4(t) + s5(t):
                cp.wait_send()

        lag = 2
        when_chunk(j, lambda t: start(s1(t)))
        when_chunk(j - lag, t2)
        when_chunk(j - 2 * lag, t3)
        when_chunk(j - 3 * lag, t4)
        when_chunk(j - 4 * lag, t5)
        when_chunk(j - lag, lambda t: start(s2(t)))
        when_chunk(j - 2 * lag, lambda t: start(s3(t) + keep(t)))
        when_chunk(j - 5 * lag, t6)

    wcp = pltpu.make_async_copy(w_ref, wb, wsem)
    exchanged = u_ref if own_u else v_ref
    announce, ex_start, ex_finish = _exchange(nh, nw, [(exchanged, first_ref, last_ref, erows, ecl, ecr)], esend, erecv)

    def given_rows():
        return [pltpu.make_async_copy(rows_ref.at[k], p.at[k * (th + 1), :, c:2 * c], psem.at[k]) for k in range(2)]

    def middle(src):
        return pltpu.make_async_copy(src, p.at[1:th + 1, :, c:2 * c], psem.at[2])

    def rows_in(own):
        if own:
            ex_finish()
            for k in range(2):
                p[k * (th + 1), :, c:2 * c] = erows[k]
        else:
            for cp in given_rows():
                cp.wait()

    def shift(own):
        _shift_patches(p, *((ecl, ecr) if own else (cl_ref, cr_ref)))

    @pl.when(i == 0)
    def _():
        vc = pltpu.make_async_copy(vt_ref, vt, vsem)
        mc = middle(u_ref)
        start([vc, mc] + ([] if own_u else given_rows()))
        barrier = pltpu.get_barrier_semaphore()
        n = announce(barrier)
        pl.semaphore_signal(barrier, inc=1, device_id=xn, device_id_type=MESH)
        pl.semaphore_wait(barrier, n + 1)
        ex_start()
        wcp.start()
        vc.wait()
        mc.wait()

    @pl.when(i == 1)
    def _():
        rows_in(own_u)

    @pl.when(i == 3)
    def _():
        shift(own_u)

    @pl.when(jnp.logical_and(i >= 2, i < nt + 2))
    def _():
        t = i - 2
        for cp in s0(t):
            cp.wait()
        hown[t] += recv0[lax.rem(t, 2)]

    @pl.when(jnp.logical_and(i >= 1, i < nt + 1))
    def _():
        start(s0(i - 1))

    @pl.when(i == nt)
    def _():
        wcp.wait()

    @pl.when(i == nt + nu)
    def _():
        mc = middle(v_ref)
        start([mc] + (given_rows() if own_u else []))
        mc.wait()
        rows_in(not own_u)
        shift(not own_u)

    j = jnp.int32(-1)
    now = jnp.int32(0)
    for s in ticks:
        j = j + jnp.where(i >= s, 1, 0)
        now = now + jnp.where(i == s, 1, 0)

    @pl.when(now > 0)
    def _():
        tick(j)

    @pl.when(i < nt)
    def _():
        a, b = tap(i)
        rhs = p[pl.ds(a, th), :, pl.ds(pl.multiple_of(b * c, 128), c)].reshape(th * tw, c)
        d = jnp.dot(vt[...], rhs, preferred_element_type=F32).T
        hown[i] = jnp.where(ci == 0, d[:half], d[half:])
        dsend[lax.rem(i, 2)] = jnp.where(ci == 0, d[half:], d[:half])

    def conv(ib, transposed):
        acc = None
        for a in range(3):
            lhs = p[pl.ds(ib * 2 + a, 2)].reshape(2 * tw, 3 * c)
            if transposed:
                k = nt - 1 - 3 * a
                rhs = jnp.concatenate([wb[k], wb[k - 1], wb[k - 2]], axis=1)
                d = lax.dot_general(lhs, rhs, (((1,), (1,)), ((), ())), preferred_element_type=F32)
            else:
                d = jnp.dot(lhs, wb[3 * a:3 * a + 3].reshape(3 * c, c), preferred_element_type=F32)
            acc = d if acc is None else acc + d
        return acc

    if nu:
        @pl.when(jnp.logical_and(i >= nt, i < nt + nu))
        def _():
            ep_u(i - nt, conv(i - nt, False), xu, ou)

    @pl.when(jnp.logical_and(i >= nt + nu, i < nt + nu + th // 2))
    def _():
        ib = i - nt - nu
        ep_v(ib, conv(ib, True), xv, ov)


def _fused(nh, nw, name, cid, own_u, steps, ticks, u, v, vt, edges, halo, w, nu, ep_u, xu, ep_v, xv, outs_v):
    th, tw, c = u.shape
    nt, half = 9, c // 2
    last = th // 2 - 1
    full = pl.BlockSpec((th + 2, 1, c), lambda i: (0, 0, 0), pipeline_mode=pl.Buffered(1))
    small = pl.BlockSpec((8, c), lambda i: (0, 0))
    ub = pl.BlockSpec((2, tw, c), lambda i: (jnp.minimum(jnp.maximum(i - nt, 0), nu - 1), 0, 0))
    vb = pl.BlockSpec((2, tw, c), lambda i: (jnp.minimum(jnp.maximum(i - nt - nu, 0), last), 0, 0))
    dma = pltpu.SemaphoreType.DMA
    side = pltpu.VMEM((th + 2, 1, c), F32)
    out_u = [jax.ShapeDtypeStruct((2 * nu, tw, c), BF16)] if nu else []
    call = pl.pallas_call(
        functools.partial(_fused_kernel, nh, nw, own_u, ticks, nu, ep_u, ep_v, len(xu), len(xv), len(outs_v)), grid=(steps,),
        out_shape=out_u + [o for o, _ in outs_v] + [jax.ShapeDtypeStruct((nt * c, c), F32)],
        in_specs=[ANY] * 6 + [full, full, ANY] + [ub for _ in xu] + [vb if b else small for _, b in xv],
        out_specs=[ub for _ in out_u] + [vb if b else small for _, b in outs_v] + [ANY],
        scratch_shapes=[pltpu.VMEM((th + 2, tw, 3 * c), BF16), pltpu.VMEM((c, th * tw), BF16), pltpu.VMEM((nt, c, c), BF16),
                        pltpu.VMEM((2, half, c), F32), pltpu.VMEM((nt, half, c), F32), pltpu.VMEM((2, half, c), F32),
                        pltpu.VMEM((nt, 2, c // 8, c), F32), pltpu.VMEM((nt, 2, c // 16, c), F32),
                        pltpu.VMEM((2, tw, c), BF16), side, side,
                        dma((3,)), dma, dma, dma((10, nt)), dma((10, nt)), dma((2, nt)), dma((8,)), dma((8,))],
        compiler_params=pltpu.CompilerParams(dimension_semantics=("arbitrary",), vmem_limit_bytes=VMEM_LIMIT, collective_id=cid, has_side_effects=True),
        name=name,
    )
    return call(u, v, vt, *edges, *halo, w.reshape(nt, c, c), *[x for x, _ in xu], *[x for x, _ in xv])


def solution(mesh):
    nh, nw = mesh.shape["h"], mesh.shape["w"]
    mesh3 = Mesh(mesh.devices.reshape(nw, nh // 2, 2), ("w", "x", "c"))
    tile = P(None, ("x", "c"), "w", None)

    def body(x, w1, gamma, beta, w2, g):
        _, th, tw, c = x.shape
        x, g = x[0], g[0]
        cnt = float(th * nh * tw * nw * (c // GROUPS))
        rb = 2
        blk = pl.BlockSpec((rb, tw, c), lambda i: (i, 0, 0))
        small = pl.BlockSpec((8, c), lambda i: (0, 0))
        img16 = jax.ShapeDtypeStruct((th, tw, c), BF16)
        img32 = jax.ShapeDtypeStruct((th, tw, c), F32)
        sums = jax.ShapeDtypeStruct((8, c), F32)
        par = jnp.concatenate([jnp.zeros((2, c), F32), gamma[None], beta[None], jnp.zeros((4, c), F32)])

        edge = jax.ShapeDtypeStruct((th, 1, c), F32)
        eblk = pl.BlockSpec((rb, 1, c), lambda i: (i, 0, 0))

        def with_edges(u):
            return u, u[:, 0:1, :].astype(F32), u[:, tw - 1:, :].astype(F32)

        xh, gh = _halo(nh, nw, 0, *with_edges(x), *with_edges(g))
        gt, a, s = _conv("conv1", _ep_conv1, x, xh, w1, g, [img16, sums], [blk, small])
        st = _allsum(nh, nw, cnt, 0, 1, s, par)
        z, *ze = pl.pallas_call(_z_kernel, grid=(th // rb,), out_shape=[img16, edge, edge], in_specs=[blk, small], out_specs=[blk, eblk, eblk], name="act")(a, st)
        y, dn, t, dw2 = _fused(nh, nw, "mid", 5, True, 25, (*range(2, 9), *range(10, 15, 2), *range(15, 24)), z, g, gt, ze, gh, w2, th // 2, _ep_residual,
                               [(x, True)], _ep_dz, [(a, True), (st, False)], [(img32, True), (sums, False)])
        t = _allsum(nh, nw, cnt, 1, 3, t, st)
        wblk = pl.BlockSpec((dw2.shape[0] * rb // th, c), lambda i: (i, 0))
        wout = jax.ShapeDtypeStruct(dw2.shape, F32)
        da, dat, da0, da1, y, dw2 = pl.pallas_call(
            _da_kernel, grid=(th // rb,), out_shape=[img16, jax.ShapeDtypeStruct((c, th * tw), BF16), edge, edge, img16, wout], in_specs=[blk, blk, small, small, blk, wblk],
            out_specs=[blk, pl.BlockSpec((c, rb * tw), lambda i: (0, i)), eblk, eblk, blk, wblk], name="da")(dn, a, st, t, y, dw2)
        dx, dw1 = _fused(nh, nw, "tail", 6, False, 25, (*range(2, 9), *range(10, 15, 2), *range(16, 25)), x, da, dat, (da0, da1), xh, w1, 0, None, [],
                         _ep_residual, [(g, True)], [(img16, True)])
        dx, dw1 = pl.pallas_call(_copy_kernel, grid=(th // rb,), out_shape=[img16, wout], in_specs=[blk, wblk], out_specs=[blk, wblk], name="finish")(dx, dw1)
        return y[None], dx[None], dw1.reshape(w1.shape), dw2.reshape(w2.shape), t[0], t[1]

    return jax.shard_map(body, mesh=mesh3, in_specs=(tile, P(), P(), P(), P(), tile), out_specs=(tile, tile, P(), P(), P(), P()), check_vma=False)
```

```python
import functools

import jax
import jax.numpy as jnp
from jax import lax
from jax.experimental import pallas as pl
from jax.experimental.pallas import tpu as pltpu
from jax.sharding import Mesh
from jax.sharding import PartitionSpec as P

GROUPS = 32
EPS = 1e-5
F32 = jnp.float32
BF16 = jnp.bfloat16
MESH = pl.DeviceIdType.MESH
VMEM_LIMIT = 61 * 1024 * 1024
ANY = pl.BlockSpec(memory_space=pl.ANY)
VM = pl.BlockSpec(memory_space=pltpu.VMEM)
GELU_C = 0.7978845608028654
GELU_A = 0.044715


def _whole(*shape, **kw):
    return pl.BlockSpec(shape, lambda i: (0,) * len(shape), **kw)


def _gelu_parts(n):
    n2 = n * n
    t = jnp.tanh(GELU_C * (n + GELU_A * n * n2))
    return n2, t


def _gelu(n):
    _, t = _gelu_parts(n)
    return 0.5 * n * (1.0 + t)


def _gelu_grad(n):
    n2, t = _gelu_parts(n)
    return 0.5 * (1.0 + t) + 0.5 * n * (1.0 - t * t) * (GELU_C * (1.0 + 3.0 * GELU_A * n2))


def _exchange(nh, nw, arrays, send, recv):
    th, tw, c = arrays[0][0].shape
    w = lax.axis_index("w")
    h = lax.axis_index("x") * 2 + lax.axis_index("c")
    dirs = [(dh, dw) for dh in (-1, 0, 1) for dw in (-1, 0, 1) if (dh, dw) != (0, 0)]
    sends = [(k, i, dh, dw) for k in range(len(arrays)) for i, (dh, dw) in enumerate(dirs)]

    def dev(dh, dw):
        hh = h + dh
        return (w + dw, hh // 2, hh % 2)

    def has(dh, dw):
        ok = None
        for cond in ([h > 0] if dh < 0 else [h < nh - 1] if dh > 0 else []) + ([w > 0] if dw < 0 else [w < nw - 1] if dw > 0 else []):
            ok = cond if ok is None else jnp.logical_and(ok, cond)
        return ok

    def announce(barrier):
        for d in dirs:
            @pl.when(has(*d))
            def _(d=d):
                pl.semaphore_signal(barrier, inc=1, device_id=dev(*d), device_id_type=MESH)
        one = jnp.int32(1)
        zero = jnp.int32(0)
        nv = one + jnp.where(h > 0, one, zero) + jnp.where(h < nh - 1, one, zero)
        nz = one + jnp.where(w > 0, one, zero) + jnp.where(w < nw - 1, one, zero)
        return nv * nz - 1

    def landing(k, dh, dw):
        rows, cl, cr = arrays[k][3:]
        side = cr if dw < 0 else cl
        if dw == 0:
            return rows, 1 if dh < 0 else 0
        if dh == 0:
            return side, slice(1, th + 1)
        return side, th + 1 if dh < 0 else 0

    def copy(k, i, dh, dw):
        u, first, last = arrays[k][:3]
        r = 0 if dh < 0 else th - 1
        edge = first if dw < 0 else last
        src = u.at[r] if dw == 0 else edge if dh == 0 else edge.at[r]
        ref, at = landing(k, dh, dw)
        return pltpu.make_async_remote_copy(src_ref=src, dst_ref=ref.at[at], send_sem=send.at[k * 8 + i], recv_sem=recv.at[k * 8 + i],
                                            device_id=dev(dh, dw), device_id_type=MESH)

    def start():
        for k, i, dh, dw in sends:
            @pl.when(has(dh, dw))
            def _(k=k, i=i, dh=dh, dw=dw):
                copy(k, i, dh, dw).start()

    def finish():
        for k, i, dh, dw in sends:
            @pl.when(jnp.logical_not(has(-dh, -dw)))
            def _(k=k, dh=dh, dw=dw):
                ref, at = landing(k, dh, dw)
                ref[at] = jnp.zeros(ref.at[at].shape, ref.dtype)

            @pl.when(has(dh, dw))
            def _(k=k, i=i, dh=dh, dw=dw):
                copy(k, i, dh, dw).wait_send()

            @pl.when(has(-dh, -dw))
            def _(k=k, i=i, dh=dh, dw=dw):
                copy(k, i, dh, dw).wait_recv()

    return announce, start, finish


def _halo_kernel(nh, nw, n_arr, *refs):
    ins = refs[:3 * n_arr]
    outs = refs[3 * n_arr:6 * n_arr]
    announce, start, finish = _exchange(nh, nw, [ins[3 * k:3 * k + 3] + outs[3 * k:3 * k + 3] for k in range(n_arr)], *refs[6 * n_arr:])
    barrier = pltpu.get_barrier_semaphore()
    pl.semaphore_wait(barrier, announce(barrier))
    start()
    finish()


def _halo(nh, nw, cid, *us):
    th, tw, c = us[0].shape
    n = len(us) // 3
    out = []
    for _ in range(n):
        out += [jax.ShapeDtypeStruct((2, tw, c), BF16), jax.ShapeDtypeStruct((th + 2, 1, c), F32), jax.ShapeDtypeStruct((th + 2, 1, c), F32)]
    res = pl.pallas_call(
        functools.partial(_halo_kernel, nh, nw, n), out_shape=out, in_specs=[ANY] * (3 * n), out_specs=[VM] * (3 * n),
        scratch_shapes=[pltpu.SemaphoreType.DMA((8 * n,)), pltpu.SemaphoreType.DMA((8 * n,))],
        compiler_params=pltpu.CompilerParams(collective_id=cid, has_side_effects=True, vmem_limit_bytes=VMEM_LIMIT),
        name=f"halo{cid}",
    )(*us)
    return [tuple(res[3 * k:3 * k + 3]) for k in range(n)]


def _allsum_kernel(nh, nw, cnt, mode, part_ref, par_ref, out_ref, mine, buf, same, lsem, send, recv):
    n = nh * nw
    w = lax.axis_index("w")
    h = lax.axis_index("x") * 2 + lax.axis_index("c")
    me = w * nh + h

    def dev(j):
        hh = j % nh
        return (j // nh, hh // 2, hh % 2)

    local = pltpu.make_async_copy(part_ref, mine, lsem)
    local.start()
    c = mine.shape[-1]
    gi = jnp.floor((lax.broadcasted_iota(jnp.int32, (c, c), 0).astype(F32) + 0.5) * (GROUPS / c))
    gj = jnp.floor((lax.broadcasted_iota(jnp.int32, (c, c), 1).astype(F32) + 0.5) * (GROUPS / c))
    same[...] = jnp.where(gi == gj, 1.0, 0.0).astype(BF16)

    def group_means(v):
        hi = v.astype(BF16)
        rest = v - hi.astype(F32)
        mid = rest.astype(BF16)
        lo = (rest - mid.astype(F32)).astype(BF16)
        return sum(jnp.dot(x, same[...], preferred_element_type=F32) for x in (lo, mid, hi)) / cnt

    barrier = pltpu.get_barrier_semaphore()
    for k in range(1, n):
        pl.semaphore_signal(barrier, inc=1, device_id=dev(lax.rem(me + k, n)), device_id_type=MESH)
    local.wait()
    pl.semaphore_wait(barrier, n - 1)
    copies = []
    for k in range(1, n):
        cp = pltpu.make_async_remote_copy(src_ref=mine, dst_ref=buf.at[k - 1], send_sem=send.at[k - 1], recv_sem=recv.at[k - 1],
                                          device_id=dev(lax.rem(me + k, n)), device_id_type=MESH)
        cp.start()
        copies.append(cp)
    for cp in copies:
        cp.wait()
    total = None
    vals = [mine[...]] + [buf[k] for k in range(n - 1)]
    for j in range(n):
        t = jnp.zeros_like(vals[0])
        off = lax.rem(me - j + n, n)
        for k in range(n):
            t = t + jnp.where(off == k, vals[k], 0.0)
        total = t if total is None else total + t
    row = lax.broadcasted_iota(jnp.int32, (8, c), 0)
    if mode == 0:
        m = group_means(total)
        mean, sq = m[0:1], m[1:2]
        rstd = lax.rsqrt(sq - mean * mean + EPS)
        out_ref[...] = jnp.where(row == 0, mean, jnp.where(row == 1, rstd, par_ref[...]))
    else:
        u = group_means(total * par_ref[2:3])
        out_ref[...] = jnp.where(row == 0, total[0:1], jnp.where(row == 1, total[1:2], jnp.where(row == 2, u[0:1], u[1:2])))


def _allsum(nh, nw, cnt, mode, cid, part, par):
    c = part.shape[-1]
    n = nh * nw
    return pl.pallas_call(
        functools.partial(_allsum_kernel, nh, nw, cnt, mode), out_shape=jax.ShapeDtypeStruct((8, c), F32),
        in_specs=[ANY, VM], out_specs=VM,
        scratch_shapes=[pltpu.VMEM((8, c), F32), pltpu.VMEM((n - 1, 8, c), F32), pltpu.VMEM((c, c), BF16), pltpu.SemaphoreType.DMA,
                        pltpu.SemaphoreType.DMA((n - 1,)), pltpu.SemaphoreType.DMA((n - 1,))],
        compiler_params=pltpu.CompilerParams(collective_id=cid, has_side_effects=True, vmem_limit_bytes=VMEM_LIMIT),
        name=f"allsum{cid}",
    )(part, par)


def _load_patches(u_ref, rows_ref, p, sems):
    th, c = u_ref.shape[0], u_ref.shape[2]
    cps = [pltpu.make_async_copy(u_ref, p.at[1:th + 1, :, c:2 * c], sems.at[0]),
           pltpu.make_async_copy(rows_ref.at[0], p.at[0, :, c:2 * c], sems.at[1]),
           pltpu.make_async_copy(rows_ref.at[1], p.at[th + 1, :, c:2 * c], sems.at[2])]
    for cp in cps:
        cp.start()
    return cps


def _shift_patches(p, cl_ref, cr_ref, first=0):
    n, tw, c3 = p.shape
    c = c3 // 3
    ck = 128

    def row(r, _):
        idx = lax.broadcasted_iota(jnp.int32, (tw, ck), 0)
        for k in range(c // ck):
            f = p[r, :, c + k * ck:c + (k + 1) * ck].astype(F32)
            lo = cl_ref[r, :, k * ck:(k + 1) * ck]
            hi = cr_ref[r, :, k * ck:(k + 1) * ck]
            p[r, :, k * ck:(k + 1) * ck] = jnp.where(idx == 0, lo, pltpu.roll(f, 1, 0)).astype(BF16)
            p[r, :, 2 * c + k * ck:2 * c + (k + 1) * ck] = jnp.where(idx == tw - 1, hi, pltpu.roll(f, tw - 1, 0)).astype(BF16)
        return 0

    lax.fori_loop(first, n, row, 0)


def _transposed(v):
    return v.reshape(v.shape[0] * v.shape[1], v.shape[2]).T


def _conv_kernel(rb, epilogue, u_ref, rows_ref, cl_ref, cr_ref, w_ref, v_ref, vt_ref, *refs):
    outs = refs[:-4]
    p, wb, psem, wsem = refs[-4:]
    c = u_ref.shape[2]
    i = pl.program_id(0)

    @pl.when(i == 0)
    def _():
        cps = _load_patches(u_ref, rows_ref, p, psem)
        wc = pltpu.make_async_copy(w_ref, wb, wsem)
        wc.start()
        for cp in cps:
            cp.wait()
        _shift_patches(p, cl_ref, cr_ref)
        wc.wait()

    vt_ref[...] = _transposed(v_ref[...])
    tw = p.shape[1]
    acc = None
    for a in range(3):
        lhs = p[pl.ds(i * rb + a, rb)].reshape(rb * tw, 3 * c)
        d = jnp.dot(lhs, wb[a], preferred_element_type=F32)
        acc = d if acc is None else acc + d
    epilogue(i, acc, (), outs)


def _conv(name, epilogue, u, halo, w, v, outs, out_specs, rb=2):
    th, tw, c = u.shape
    full = _whole(th + 2, 1, c, pipeline_mode=pl.Buffered(1))
    wshape = (3, 3 * c, c)
    return pl.pallas_call(
        functools.partial(_conv_kernel, rb, epilogue),
        grid=(th // rb,), out_shape=[jax.ShapeDtypeStruct((c, th * tw), BF16)] + outs, in_specs=[ANY, ANY, full, full, ANY, out_specs[0]],
        out_specs=[pl.BlockSpec((c, rb * tw), lambda i: (0, i))] + out_specs,
        scratch_shapes=[pltpu.VMEM((th + 2, tw, 3 * c), BF16), pltpu.VMEM(wshape, BF16), pltpu.SemaphoreType.DMA((3,)), pltpu.SemaphoreType.DMA],
        compiler_params=pltpu.CompilerParams(dimension_semantics=("arbitrary",), vmem_limit_bytes=VMEM_LIMIT),
        name=name,
    )(u, *halo, w.reshape(wshape), v)


def _add_sums(i, s0, s1, s_ref):
    row = lax.broadcasted_iota(jnp.int32, s_ref.shape, 0)
    s = jnp.where(row == 0, s0, jnp.where(row == 1, s1, 0.0))

    @pl.when(i == 0)
    def _():
        s_ref[...] = s

    @pl.when(i > 0)
    def _():
        s_ref[...] += s


def _ep_conv1(i, acc, extra, outs):
    a_ref, s_ref = outs
    a16 = acc.astype(BF16)
    a_ref[...] = a16.reshape(a_ref.shape)
    a = a16.astype(F32)
    s0 = a.sum(0, keepdims=True)
    s1 = (a * a).sum(0, keepdims=True)
    _add_sums(i, s0, s1, s_ref)


def _ep_residual(i, acc, extra, outs):
    o_ref = outs[0]
    r = extra[0][...].astype(F32).reshape(acc.shape)
    o_ref[...] = (acc + r).astype(BF16).reshape(o_ref.shape)


def _ep_dz(i, acc, extra, outs):
    a_ref, st_ref = extra
    dn_ref, s_ref = outs
    mean, rstd, gamma, beta = _params(st_ref)
    xhat = (a_ref[...].astype(F32).reshape(acc.shape) - mean) * rstd
    dn = acc * _gelu_grad(xhat * gamma + beta)
    dn_ref[...] = dn.reshape(dn_ref.shape)
    s0 = (dn * xhat).sum(0, keepdims=True)
    s1 = dn.sum(0, keepdims=True)
    _add_sums(i, s0, s1, s_ref)


def _params(st_ref):
    st = st_ref[...]
    return [st[k:k + 1] for k in range(4)]


def _edges(v, first_ref, last_ref):
    first_ref[...] = v[:, 0:1, :]
    last_ref[...] = v[:, v.shape[1] - 1:, :]


def _z_kernel(a_ref, st_ref, z_ref, first_ref, last_ref):
    mean, rstd, gamma, beta = _params(st_ref)
    xhat = (a_ref[...].astype(F32) - mean) * rstd
    z = _gelu(xhat * gamma + beta).astype(BF16)
    z_ref[...] = z
    _edges(z.astype(F32), first_ref, last_ref)


def _finish_kernel(ny, y0_ref, y1_ref, dx0_ref, w0_ref, y_ref, dx_ref, w_ref):
    dx_ref[...] = dx0_ref[...]
    w_ref[...] = w0_ref[...]
    first = pl.program_id(0) < ny

    @pl.when(first)
    def _():
        y_ref[...] = y0_ref[...]

    @pl.when(jnp.logical_not(first))
    def _():
        y_ref[...] = y1_ref[...]


def _da_kernel(dn_ref, a_ref, st_ref, t_ref, w0_ref, o_ref, ot_ref, first_ref, last_ref, w_ref):
    w_ref[...] = w0_ref[...]
    mean, rstd, gamma, _ = _params(st_ref)
    _, _, u0, u1 = _params(t_ref)
    xhat = (a_ref[...].astype(F32) - mean) * rstd
    da = (rstd * (dn_ref[...] * gamma - u1 - xhat * u0)).astype(BF16)
    o_ref[...] = da
    ot_ref[...] = _transposed(da)
    _edges(da.astype(F32), first_ref, last_ref)


def _fused_kernel(nh, nw, own_u, ticks, nu, nz, ep_u, ep_v, n_xu, n_xv, n_ov, u_ref, v_ref, vt_ref, first_ref, last_ref, rows_ref, cl_ref, cr_ref, w_ref, *refs):
    xu, refs = refs[:n_xu], refs[n_xu:]
    xv, refs = refs[:n_xv], refs[n_xv:]
    if nz:
        (z_ref, zrows, zcl, zcr, w2_ref), xz, refs = refs[:5], refs[5:6], refs[6:]
    ou, refs = (refs[:1], refs[1:]) if nu else ((), refs)
    ov, refs = refs[:n_ov], refs[n_ov:]
    if nz:
        oz, refs = refs[:1], refs[1:]
    if own_u:
        handed, refs = refs[:3], refs[3:]
    dw_ref, p, vt, wb, dsend, hown, recv0, recv1, recv2, erows, ecl, ecr, psem, wsem, vsem, send, recv, lsem, esend, erecv = refs
    i = pl.program_id(0)
    th, tw, c = u_ref.shape
    nt = w_ref.shape[0]
    half, q, e, sub = c // 2, c // 4, c // 8, c // 16
    wi, xi, ci = lax.axis_index("w"), lax.axis_index("x"), lax.axis_index("c")
    mate, xn, yn = (wi, xi, 1 - ci), (wi, 1 - xi, ci), (1 - wi, xi, ci)
    pa, pb = xi * e, q + wi * e
    fa, fb = pa + wi * sub, pb + xi * sub

    def rows(start, n):
        return pl.ds(pl.multiple_of(start, 8), n)

    def rc(stage, t, src, dst, dev):
        return pltpu.make_async_remote_copy(src_ref=src, dst_ref=dst, send_sem=send.at[stage, t], recv_sem=recv.at[stage, t],
                                            device_id=dev, device_id_type=MESH)

    def tap(t):
        return lax.rem(2 * lax.rem(t, 3) + 1, 3), lax.rem(2 * lax.div(t, 3) + 1, 3)

    def base(t):
        a, b = tap(t)
        return (a * 3 + b) * c + ci * half

    def s0(t):
        return [rc(0, t, dsend.at[lax.rem(t, 2)], recv0.at[lax.rem(t, 2)], mate)]

    def s1(t):
        return [rc(1, t, hown.at[t, rows((1 - xi) * e, e)], recv1.at[t, 0], xn),
                rc(2, t, hown.at[t, rows(q + (1 - wi) * e, e)], recv1.at[t, 1], yn)]

    def s2(t):
        return [rc(3, t, hown.at[t, rows(pa + (1 - wi) * sub, sub)], recv2.at[t, 0], yn),
                rc(4, t, hown.at[t, rows(pb + (1 - xi) * sub, sub)], recv2.at[t, 1], xn)]

    def s3(t):
        return [rc(5, t, hown.at[t, rows(fa, sub)], dw_ref.at[rows(base(t) + fa, sub)], yn),
                rc(6, t, hown.at[t, rows(fb, sub)], dw_ref.at[rows(base(t) + fb, sub)], xn)]

    def keep(t):
        return [pltpu.make_async_copy(hown.at[t, rows(fa, sub)], dw_ref.at[rows(base(t) + fa, sub)], lsem.at[0, t]),
                pltpu.make_async_copy(hown.at[t, rows(fb, sub)], dw_ref.at[rows(base(t) + fb, sub)], lsem.at[1, t])]

    def s4(t):
        return [rc(7, t, dw_ref.at[rows(base(t) + pa, e)], dw_ref.at[rows(base(t) + pa, e)], xn),
                rc(8, t, dw_ref.at[rows(base(t) + pb, e)], dw_ref.at[rows(base(t) + pb, e)], yn)]

    def s5(t):
        return [rc(9, t, dw_ref.at[rows(base(t), half)], dw_ref.at[rows(base(t), half)], mate)]

    def start(cps):
        for cp in cps:
            cp.start()

    def when_chunk(t, f):
        @pl.when(jnp.logical_and(t >= 0, t < nt))
        def _():
            f(t)

    def tick(j):
        def t2(t):
            for cp in s1(t):
                cp.wait_recv()
            hown[t, rows(pa, e), :] += recv1[t, 0]
            hown[t, rows(pb, e), :] += recv1[t, 1]

        def t3(t):
            for cp in s2(t):
                cp.wait_recv()
            hown[t, rows(fa, sub), :] += recv2[t, 0]
            hown[t, rows(fb, sub), :] += recv2[t, 1]

        def t4(t):
            for cp in s3(t):
                cp.wait_recv()
            for cp in keep(t):
                cp.wait()
            start(s4(t))

        def t5(t):
            for cp in s4(t):
                cp.wait_recv()
            start(s5(t))

        def t6(t):
            for cp in s5(t):
                cp.wait_recv()
            for cp in s1(t) + s2(t) + s3(t) + s4(t) + s5(t):
                cp.wait_send()

        lag = 2
        when_chunk(j, lambda t: start(s1(t)))
        when_chunk(j - lag, t2)
        when_chunk(j - 2 * lag, t3)
        when_chunk(j - 3 * lag, t4)
        when_chunk(j - 4 * lag, t5)
        when_chunk(j - lag, lambda t: start(s2(t)))
        when_chunk(j - 2 * lag, lambda t: start(s3(t) + keep(t)))
        when_chunk(j - 5 * lag, t6)

    wcp = pltpu.make_async_copy(w_ref, wb, wsem)
    exchanged = u_ref if own_u else v_ref
    announce, ex_start, ex_finish = _exchange(nh, nw, [(exchanged, first_ref, last_ref, erows, ecl, ecr)], esend, erecv)

    def given_rows(ref=rows_ref):
        return [pltpu.make_async_copy(ref.at[k], p.at[k * (th + 1), :, c:2 * c], psem.at[k]) for k in range(2)]

    def middle(src):
        return pltpu.make_async_copy(src, p.at[1:th + 1, :, c:2 * c], psem.at[2])

    def rows_in(own):
        if own:
            ex_finish()
            for k in range(2):
                p[k * (th + 1), :, c:2 * c] = erows[k]
        else:
            for cp in given_rows():
                cp.wait()

    def shift(own):
        _shift_patches(p, *((ecl, ecr) if own else (cl_ref, cr_ref)))

    @pl.when(i == 0)
    def _():
        vc = pltpu.make_async_copy(vt_ref, vt, vsem)
        mc = middle(u_ref)
        start([vc, mc] + ([] if own_u else given_rows()))
        barrier = pltpu.get_barrier_semaphore()
        n = announce(barrier)
        pl.semaphore_signal(barrier, inc=1, device_id=xn, device_id_type=MESH)
        pl.semaphore_wait(barrier, n + 1)
        ex_start()
        wcp.start()
        vc.wait()
        mc.wait()

    @pl.when(i == 1)
    def _():
        rows_in(own_u)
        if own_u:
            for dst, src in zip(handed, (erows, ecl, ecr)):
                dst[...] = src[...]

    @pl.when(i == 3)
    def _():
        shift(own_u)

    @pl.when(jnp.logical_and(i >= 2, i < nt + 2))
    def _():
        t = i - 2
        for cp in s0(t):
            cp.wait()
        hown[t] += recv0[lax.rem(t, 2)]

    @pl.when(jnp.logical_and(i >= 1, i < nt + 1))
    def _():
        start(s0(i - 1))

    @pl.when(i == nt)
    def _():
        wcp.wait()

    @pl.when(i == nt + nu)
    def _():
        mc = middle(v_ref)
        start([mc] + (given_rows() if own_u else []))
        mc.wait()
        rows_in(not own_u)
        shift(not own_u)

    if nz:
        @pl.when(i == nt + nu + th // 2)
        def _():
            cps = [middle(z_ref), pltpu.make_async_copy(w2_ref, wb, wsem)] + given_rows(zrows)
            start(cps)
            for cp in cps:
                cp.wait()
            _shift_patches(p, zcl, zcr, th - 2 * nz)

    j = jnp.int32(-1)
    now = jnp.int32(0)
    for s in ticks:
        j = j + jnp.where(i >= s, 1, 0)
        now = now + jnp.where(i == s, 1, 0)

    @pl.when(now > 0)
    def _():
        tick(j)

    @pl.when(i < nt)
    def _():
        a, b = tap(i)
        rhs = p[pl.ds(a, th), :, pl.ds(pl.multiple_of(b * c, 128), c)].reshape(th * tw, c)
        d = jnp.dot(vt[...], rhs, preferred_element_type=F32).T
        hown[i] = jnp.where(ci == 0, d[:half], d[half:])
        dsend[lax.rem(i, 2)] = jnp.where(ci == 0, d[half:], d[:half])

    def conv(ib, transposed):
        acc = None
        for a in range(3):
            lhs = p[pl.ds(ib * 2 + a, 2)].reshape(2 * tw, 3 * c)
            if transposed:
                k = nt - 1 - 3 * a
                rhs = jnp.concatenate([wb[k], wb[k - 1], wb[k - 2]], axis=1)
                d = lax.dot_general(lhs, rhs, (((1,), (1,)), ((), ())), preferred_element_type=F32)
            else:
                d = jnp.dot(lhs, wb[3 * a:3 * a + 3].reshape(3 * c, c), preferred_element_type=F32)
            acc = d if acc is None else acc + d
        return acc

    if nu:
        @pl.when(jnp.logical_and(i >= nt, i < nt + nu))
        def _():
            ep_u(i - nt, conv(i - nt, False), xu, ou)

    @pl.when(jnp.logical_and(i >= nt + nu, i < nt + nu + th // 2))
    def _():
        ib = i - nt - nu
        ep_v(ib, conv(ib, True), xv, ov)

    if nz:
        @pl.when(jnp.logical_and(i >= nt + nu + th // 2, i < nt + nu + th // 2 + nz))
        def _():
            ib = i - nt - nu - nz
            ep_u(ib, conv(ib, False), xz, oz)


def _fused(nh, nw, name, cid, own_u, steps, ticks, u, v, vt, edges, halo, w, nu, ep_u, xu, ep_v, xv, outs_v, z_args=(), nz=0):
    th, tw, c = u.shape
    nt, half = 9, c // 2
    last = th // 2 - 1
    full = _whole(th + 2, 1, c, pipeline_mode=pl.Buffered(1))
    small = _whole(8, c)
    ub = pl.BlockSpec((2, tw, c), lambda i: (jnp.minimum(jnp.maximum(i - nt, 0), nu - 1), 0, 0))
    vb = pl.BlockSpec((2, tw, c), lambda i: (jnp.minimum(jnp.maximum(i - nt - nu, 0), last), 0, 0))
    dma = pltpu.SemaphoreType.DMA
    side = pltpu.VMEM((th + 2, 1, c), F32)
    out_u = [jax.ShapeDtypeStruct((2 * nu, tw, c), BF16)] if nu else []
    zb, yb = [pl.BlockSpec((2, tw, c), lambda i, k=k: (jnp.minimum(jnp.maximum(i - nt - nu - last - 1, 0), nz - 1) + k, 0, 0)) for k in (last + 1 - nz, 0)]
    out_z = [jax.ShapeDtypeStruct((2 * nz, tw, c), BF16)] if nz else []
    rblk = _whole(2, tw, c)
    sblk = _whole(th + 2, 1, c)
    given = jax.ShapeDtypeStruct((th + 2, 1, c), F32)
    out_h = [jax.ShapeDtypeStruct((2, tw, c), BF16), given, given] if own_u else []
    call = pl.pallas_call(
        functools.partial(_fused_kernel, nh, nw, own_u, ticks, nu, nz, ep_u, ep_v, len(xu), len(xv), len(outs_v)), grid=(steps,),
        out_shape=out_u + [o for o, _ in outs_v] + out_z + out_h + [jax.ShapeDtypeStruct((nt * c, c), F32)],
        in_specs=[ANY] * 6 + [full, full, ANY] + [ub for _ in xu] + [vb if b else small for _, b in xv] + ([ANY, ANY, full, full, ANY, zb] if nz else []),
        out_specs=[ub for _ in out_u] + [vb if b else small for _, b in outs_v] + [yb for _ in out_z] + ([rblk, sblk, sblk] if own_u else []) + [ANY],
        scratch_shapes=[pltpu.VMEM((th + 2, tw, 3 * c), BF16), pltpu.VMEM((c, th * tw), BF16), pltpu.VMEM((nt, c, c), BF16),
                        pltpu.VMEM((2, half, c), F32), pltpu.VMEM((nt, half, c), F32), pltpu.VMEM((2, half, c), F32),
                        pltpu.VMEM((nt, 2, c // 8, c), F32), pltpu.VMEM((nt, 2, c // 16, c), F32),
                        pltpu.VMEM((2, tw, c), BF16), side, side,
                        dma((3,)), dma, dma, dma((10, nt)), dma((10, nt)), dma((2, nt)), dma((8,)), dma((8,))],
        compiler_params=pltpu.CompilerParams(dimension_semantics=("arbitrary",), vmem_limit_bytes=VMEM_LIMIT, collective_id=cid, has_side_effects=True),
        name=name,
    )
    return call(u, v, vt, *edges, *halo, w.reshape(nt, c, c), *[x for x, _ in xu], *[x for x, _ in xv], *z_args)


def solution(mesh):
    nh, nw = mesh.shape["h"], mesh.shape["w"]
    mesh3 = Mesh(mesh.devices.reshape(nw, nh // 2, 2), ("w", "x", "c"))
    tile = P(None, ("x", "c"), "w", None)

    def body(x, w1, gamma, beta, w2, g):
        _, th, tw, c = x.shape
        x, g = x[0], g[0]
        cnt = float(th * nh * tw * nw * (c // GROUPS))
        rb = 2
        blk = pl.BlockSpec((rb, tw, c), lambda i: (i, 0, 0))
        small = _whole(8, c)
        img16 = jax.ShapeDtypeStruct((th, tw, c), BF16)
        img32 = jax.ShapeDtypeStruct((th, tw, c), F32)
        sums = jax.ShapeDtypeStruct((8, c), F32)
        par = jnp.concatenate([jnp.zeros((2, c), F32), gamma[None], beta[None], jnp.zeros((4, c), F32)])

        edge = jax.ShapeDtypeStruct((th, 1, c), F32)
        eblk = pl.BlockSpec((rb, 1, c), lambda i: (i, 0, 0))

        def with_edges(u):
            return u, u[:, 0:1, :].astype(F32), u[:, tw - 1:, :].astype(F32)

        xh, gh = _halo(nh, nw, 0, *with_edges(x), *with_edges(g))
        gt, a, s = _conv("conv1", _ep_conv1, x, xh, w1, g, [img16, sums], [blk, small])
        st = _allsum(nh, nw, cnt, 0, 1, s, par)
        z, *ze = pl.pallas_call(_z_kernel, grid=(th // rb,), out_shape=[img16, edge, edge], in_specs=[blk, small], out_specs=[blk, eblk, eblk], name="act")(a, st)
        ny, nz = 3, th // rb - 3
        y0, dn, t, *zh, dw2 = _fused(nh, nw, "mid", 5, True, 24, (*range(2, 9), *range(10, 15, 2), *range(15, 24)), z, g, gt, ze, gh, w2, ny, _ep_residual,
                                     [(x, True)], _ep_dz, [(a, True), (st, False)], [(img32, True), (sums, False)])
        t = _allsum(nh, nw, cnt, 1, 3, t, st)
        wblk = pl.BlockSpec((dw2.shape[0] * rb // th, c), lambda i: (i, 0))
        wout = jax.ShapeDtypeStruct(dw2.shape, F32)
        da, dat, da0, da1, dw2 = pl.pallas_call(
            _da_kernel, grid=(th // rb,), out_shape=[img16, jax.ShapeDtypeStruct((c, th * tw), BF16), edge, edge, wout], in_specs=[blk, blk, small, small, wblk],
            out_specs=[blk, pl.BlockSpec((c, rb * tw), lambda i: (0, i)), eblk, eblk, wblk], name="da")(dn, a, st, t, dw2)
        dx, y1, dw1 = _fused(nh, nw, "tail", 6, False, 25, (*range(2, 9), *range(10, 15, 2), *range(16, 25)), x, da, dat, (da0, da1), xh, w1, 0, _ep_residual, [],
                             _ep_residual, [(g, True)], [(img16, True)], (z, *zh, w2.reshape(9, c, c), x), nz)
        lo, hi = pl.BlockSpec((rb, tw, c), lambda i: (jnp.minimum(i, ny - 1), 0, 0)), pl.BlockSpec((rb, tw, c), lambda i: (jnp.maximum(i - ny, 0), 0, 0))
        y, dx, dw1 = pl.pallas_call(functools.partial(_finish_kernel, ny), grid=(th // rb,), out_shape=[img16, img16, wout],
                                    in_specs=[lo, hi, blk, wblk], out_specs=[blk, blk, wblk], name="finish")(y0, y1, dx, dw1)
        return y[None], dx[None], dw1.reshape(w1.shape), dw2.reshape(w2.shape), t[0], t[1]

    return jax.shard_map(body, mesh=mesh3, in_specs=(tile, P(), P(), P(), P(), tile), out_specs=(tile, tile, P(), P(), P(), P()), check_vma=False)
```

```python
import functools

import jax
import jax.numpy as jnp
from jax import lax
from jax.experimental import pallas as pl
from jax.experimental.pallas import tpu as pltpu
from jax.sharding import Mesh
from jax.sharding import PartitionSpec as P

GROUPS = 32
EPS = 1e-5
F32 = jnp.float32
BF16 = jnp.bfloat16
MESH = pl.DeviceIdType.MESH
VMEM_LIMIT = 67043328
ANY = pl.BlockSpec(memory_space=pl.ANY)
VM = pl.BlockSpec(memory_space=pltpu.VMEM)
GELU_C = 0.7978845608028654
GELU_A = 0.044715


def _whole(*shape, **kw):
    return pl.BlockSpec(shape, lambda i: (0,) * len(shape), **kw)


def _gelu_parts(n):
    n2 = n * n
    t = jnp.tanh(GELU_C * (n + GELU_A * n * n2))
    return n2, t


def _gelu(n):
    _, t = _gelu_parts(n)
    return 0.5 * n * (1.0 + t)


def _gelu_grad(n):
    n2, t = _gelu_parts(n)
    return 0.5 * (1.0 + t) + 0.5 * n * (1.0 - t * t) * (GELU_C * (1.0 + 3.0 * GELU_A * n2))


def _exchange(nh, nw, arrays, send, recv):
    th, tw, c = arrays[0][0].shape
    w = lax.axis_index("w")
    h = lax.axis_index("x") * 2 + lax.axis_index("c")
    dirs = [(dh, dw) for dh in (-1, 0, 1) for dw in (-1, 0, 1) if (dh, dw) != (0, 0)]
    sends = [(k, i, dh, dw) for k in range(len(arrays)) for i, (dh, dw) in enumerate(dirs)]

    def dev(dh, dw):
        hh = h + dh
        return (w + dw, hh // 2, hh % 2)

    def has(dh, dw):
        ok = None
        for cond in ([h > 0] if dh < 0 else [h < nh - 1] if dh > 0 else []) + ([w > 0] if dw < 0 else [w < nw - 1] if dw > 0 else []):
            ok = cond if ok is None else jnp.logical_and(ok, cond)
        return ok

    def announce(barrier):
        for d in dirs:
            @pl.when(has(*d))
            def _(d=d):
                pl.semaphore_signal(barrier, inc=1, device_id=dev(*d), device_id_type=MESH)
        one = jnp.int32(1)
        zero = jnp.int32(0)
        nv = one + jnp.where(h > 0, one, zero) + jnp.where(h < nh - 1, one, zero)
        nz = one + jnp.where(w > 0, one, zero) + jnp.where(w < nw - 1, one, zero)
        return nv * nz - 1

    def landing(k, dh, dw):
        rows, cl, cr = arrays[k][3:]
        side = cr if dw < 0 else cl
        if dw == 0:
            return rows, 1 if dh < 0 else 0
        if dh == 0:
            return side, slice(1, th + 1)
        return side, th + 1 if dh < 0 else 0

    def copy(k, i, dh, dw):
        u, first, last = arrays[k][:3]
        r = 0 if dh < 0 else th - 1
        edge = first if dw < 0 else last
        src = u.at[r] if dw == 0 else edge if dh == 0 else edge.at[r]
        ref, at = landing(k, dh, dw)
        return pltpu.make_async_remote_copy(src_ref=src, dst_ref=ref.at[at], send_sem=send.at[k * 8 + i], recv_sem=recv.at[k * 8 + i],
                                            device_id=dev(dh, dw), device_id_type=MESH)

    def start():
        for k, i, dh, dw in sends:
            @pl.when(has(dh, dw))
            def _(k=k, i=i, dh=dh, dw=dw):
                copy(k, i, dh, dw).start()

    def finish():
        for k, i, dh, dw in sends:
            @pl.when(jnp.logical_not(has(-dh, -dw)))
            def _(k=k, dh=dh, dw=dw):
                ref, at = landing(k, dh, dw)
                ref[at] = jnp.zeros(ref.at[at].shape, ref.dtype)

            @pl.when(has(dh, dw))
            def _(k=k, i=i, dh=dh, dw=dw):
                copy(k, i, dh, dw).wait_send()

            @pl.when(has(-dh, -dw))
            def _(k=k, i=i, dh=dh, dw=dw):
                copy(k, i, dh, dw).wait_recv()

    return announce, start, finish


def _halo_kernel(nh, nw, n_arr, *refs):
    ins = refs[:3 * n_arr]
    outs = refs[3 * n_arr:6 * n_arr]
    announce, start, finish = _exchange(nh, nw, [ins[3 * k:3 * k + 3] + outs[3 * k:3 * k + 3] for k in range(n_arr)], *refs[6 * n_arr:])
    barrier = pltpu.get_barrier_semaphore()
    pl.semaphore_wait(barrier, announce(barrier))
    start()
    finish()


def _halo(nh, nw, cid, *us):
    th, tw, c = us[0].shape
    n = len(us) // 3
    out = []
    for _ in range(n):
        out += [jax.ShapeDtypeStruct((2, tw, c), BF16), jax.ShapeDtypeStruct((th + 2, 1, c), F32), jax.ShapeDtypeStruct((th + 2, 1, c), F32)]
    res = pl.pallas_call(
        functools.partial(_halo_kernel, nh, nw, n), out_shape=out, in_specs=[ANY] * (3 * n), out_specs=[VM] * (3 * n),
        scratch_shapes=[pltpu.SemaphoreType.DMA((8 * n,)), pltpu.SemaphoreType.DMA((8 * n,))],
        compiler_params=pltpu.CompilerParams(collective_id=cid, has_side_effects=True, vmem_limit_bytes=VMEM_LIMIT),
        name=f"halo{cid}",
    )(*us)
    return [tuple(res[3 * k:3 * k + 3]) for k in range(n)]


def _peers(nh, nw):
    n = nh * nw
    me = lax.axis_index("w") * nh + lax.axis_index("x") * 2 + lax.axis_index("c")

    def dev(j):
        hh = lax.rem(j, nh)
        return (lax.div(j, nh), lax.div(hh, 2), lax.rem(hh, 2))

    return me, [dev(lax.rem(me + k, n)) for k in range(1, n)]


def _meet(peers):
    barrier = pltpu.get_barrier_semaphore()
    for d in peers:
        pl.semaphore_signal(barrier, inc=1, device_id=d, device_id_type=MESH)
    pl.semaphore_wait(barrier, len(peers))


def _sum_devices(me, peers, mine, buf, send, recv):
    copies = [pltpu.make_async_remote_copy(src_ref=mine, dst_ref=buf.at[k], send_sem=send.at[k], recv_sem=recv.at[k],
                                           device_id=d, device_id_type=MESH) for k, d in enumerate(peers)]
    for cp in copies:
        cp.start()
    for cp in copies:
        cp.wait()
    n = len(peers) + 1
    vals = [mine[...]] + [buf[k] for k in range(n - 1)]
    total = 0.0
    for j in range(n):
        off = lax.rem(me - j + n, n)
        total = total + sum(jnp.where(off == k, v, 0.0) for k, v in enumerate(vals))
    return total


def _fill_same(same):
    c = same.shape[0]
    gi, gj = [jnp.floor((lax.broadcasted_iota(jnp.int32, (c, c), d).astype(F32) + 0.5) * (GROUPS / c)) for d in range(2)]
    same[...] = jnp.where(gi == gj, 1.0, 0.0).astype(BF16)


def _group_means(v, same, cnt):
    hi = v.astype(BF16)
    rest = v - hi.astype(F32)
    mid = rest.astype(BF16)
    lo = (rest - mid.astype(F32)).astype(BF16)
    return sum(jnp.dot(x, same[...], preferred_element_type=F32) for x in (lo, mid, hi)) / cnt


def _allsum_kernel(nh, nw, cnt, part_ref, par_ref, out_ref, mine, buf, same, lsem, send, recv):
    me, peers = _peers(nh, nw)
    local = pltpu.make_async_copy(part_ref, mine, lsem)
    local.start()
    _fill_same(same)
    local.wait()
    _meet(peers)
    m = _group_means(_sum_devices(me, peers, mine, buf, send, recv), same, cnt)
    mean = m[0:1]
    row = lax.broadcasted_iota(jnp.int32, m.shape, 0)
    out_ref[...] = jnp.where(row == 0, mean, jnp.where(row == 1, lax.rsqrt(m[1:2] - mean * mean + EPS), par_ref[...]))


def _allsum(nh, nw, cnt, cid, part, par):
    c = part.shape[-1]
    n = nh * nw
    return pl.pallas_call(
        functools.partial(_allsum_kernel, nh, nw, cnt), out_shape=jax.ShapeDtypeStruct((8, c), F32),
        in_specs=[ANY, VM], out_specs=VM,
        scratch_shapes=[pltpu.VMEM((8, c), F32), pltpu.VMEM((n - 1, 8, c), F32), pltpu.VMEM((c, c), BF16), pltpu.SemaphoreType.DMA,
                        pltpu.SemaphoreType.DMA((n - 1,)), pltpu.SemaphoreType.DMA((n - 1,))],
        compiler_params=pltpu.CompilerParams(collective_id=cid, has_side_effects=True, vmem_limit_bytes=VMEM_LIMIT),
        name=f"allsum{cid}",
    )(part, par)


def _load_patches(u_ref, rows_ref, p, sems):
    th, c = u_ref.shape[0], u_ref.shape[2]
    cps = [pltpu.make_async_copy(u_ref, p.at[1:th + 1, :, c:2 * c], sems.at[0]),
           pltpu.make_async_copy(rows_ref.at[0], p.at[0, :, c:2 * c], sems.at[1]),
           pltpu.make_async_copy(rows_ref.at[1], p.at[th + 1, :, c:2 * c], sems.at[2])]
    for cp in cps:
        cp.start()
    return cps


def _shift_patches(p, cl_ref, cr_ref, first=0):
    n, tw, c3 = p.shape
    c = c3 // 3
    ck = 128

    def row(r, _):
        idx = lax.broadcasted_iota(jnp.int32, (tw, ck), 0)
        for k in range(c // ck):
            f = p[r, :, c + k * ck:c + (k + 1) * ck].astype(F32)
            lo = cl_ref[r, :, k * ck:(k + 1) * ck]
            hi = cr_ref[r, :, k * ck:(k + 1) * ck]
            p[r, :, k * ck:(k + 1) * ck] = jnp.where(idx == 0, lo, pltpu.roll(f, 1, 0)).astype(BF16)
            p[r, :, 2 * c + k * ck:2 * c + (k + 1) * ck] = jnp.where(idx == tw - 1, hi, pltpu.roll(f, tw - 1, 0)).astype(BF16)
        return 0

    lax.fori_loop(first, n, row, 0)


def _transposed(v):
    return v.reshape(v.shape[0] * v.shape[1], v.shape[2]).T


def _conv_kernel(rb, epilogue, u_ref, rows_ref, cl_ref, cr_ref, w_ref, v_ref, vt_ref, *refs):
    outs = refs[:-4]
    p, wb, psem, wsem = refs[-4:]
    c = u_ref.shape[2]
    i = pl.program_id(0)

    @pl.when(i == 0)
    def _():
        cps = _load_patches(u_ref, rows_ref, p, psem)
        wc = pltpu.make_async_copy(w_ref, wb, wsem)
        wc.start()
        for cp in cps:
            cp.wait()
        _shift_patches(p, cl_ref, cr_ref)
        wc.wait()

    vt_ref[...] = _transposed(v_ref[...])
    tw = p.shape[1]
    acc = None
    for a in range(3):
        lhs = p[pl.ds(i * rb + a, rb)].reshape(rb * tw, 3 * c)
        d = jnp.dot(lhs, wb[a], preferred_element_type=F32)
        acc = d if acc is None else acc + d
    epilogue(i, acc, (), outs)


def _conv(name, epilogue, u, halo, w, v, outs, out_specs, rb=2):
    th, tw, c = u.shape
    full = _whole(th + 2, 1, c, pipeline_mode=pl.Buffered(1))
    wshape = (3, 3 * c, c)
    return pl.pallas_call(
        functools.partial(_conv_kernel, rb, epilogue),
        grid=(th // rb,), out_shape=[jax.ShapeDtypeStruct((c, th * tw), BF16)] + outs, in_specs=[ANY, ANY, full, full, ANY, out_specs[0]],
        out_specs=[pl.BlockSpec((c, rb * tw), lambda i: (0, i))] + out_specs,
        scratch_shapes=[pltpu.VMEM((th + 2, tw, 3 * c), BF16), pltpu.VMEM(wshape, BF16), pltpu.SemaphoreType.DMA((3,)), pltpu.SemaphoreType.DMA],
        compiler_params=pltpu.CompilerParams(dimension_semantics=("arbitrary",), vmem_limit_bytes=VMEM_LIMIT),
        name=name,
    )(u, *halo, w.reshape(wshape), v)


def _add_sums(i, s0, s1, s_ref):
    row = lax.broadcasted_iota(jnp.int32, s_ref.shape, 0)
    s = jnp.where(row == 0, s0, jnp.where(row == 1, s1, 0.0))

    @pl.when(i == 0)
    def _():
        s_ref[...] = s

    @pl.when(i > 0)
    def _():
        s_ref[...] += s


def _ep_residual(acc, r_ref, o_ref):
    o_ref[...] = (acc + r_ref[...].astype(F32).reshape(acc.shape)).astype(BF16).reshape(o_ref.shape)


def _ep_conv1(i, acc, extra, outs):
    a_ref, s_ref = outs
    a16 = acc.astype(BF16)
    a_ref[...] = a16.reshape(a_ref.shape)
    a = a16.astype(F32)
    s0 = a.sum(0, keepdims=True)
    s1 = (a * a).sum(0, keepdims=True)
    _add_sums(i, s0, s1, s_ref)


def _params(st_ref):
    st = st_ref[...]
    return [st[k:k + 1] for k in range(4)]


def _edges(v, first_ref, last_ref):
    first_ref[...] = v[:, 0:1, :]
    last_ref[...] = v[:, v.shape[1] - 1:, :]


def _z_kernel(a_ref, st_ref, z_ref, first_ref, last_ref):
    mean, rstd, gamma, beta = _params(st_ref)
    xhat = (a_ref[...].astype(F32) - mean) * rstd
    z = _gelu(xhat * gamma + beta).astype(BF16)
    z_ref[...] = z
    _edges(z.astype(F32), first_ref, last_ref)


def _plan(nt, nb):
    starts = [0, nt, nt + nb, nt + 2 * nb, 2 * nt + 2 * nb, 2 * nt + 3 * nb, 2 * nt + 4 * nb]
    late = [*range(2, 9), *range(10, 15, 2), *range(16, 25)]
    return starts, [*range(2, 10), 11, 13, 16, 17, 20, 24, 26] + [starts[3] + s for s in late], 15


def _main_kernel(nh, nw, cnt, z_ref, z0_ref, z1_ref, g_ref, gt_ref, grows, gcl, gcr, x_ref, xrows, xcl, xcr, w1_ref, w2_ref, st_ref, xb_ref, gb_ref, ab_ref,
                 y_ref, dx_ref, t_ref, dn_ref, da_ref, dw_ref,
                 p, vt, wb, dsend, hown, recv0, recv1, recv2, zrows, zcl, zcr, arows, acl, acr, e0, e1, dnb, dab, sacc, sbuf, same,
                 psem, wsem, vsem, send, recv, lsem, zsend, zrecv, asend, arecv, ssend, srecv, dsem):
    i = pl.program_id(0)
    th, tw, c = x_ref.shape
    nt, nb = w1_ref.shape[0], th // 2
    (_, s_z, s_a, s_w, s_x, s_y, _), ticks, second = _plan(nt, nb)
    half, q, e, sub = c // 2, c // 4, c // 8, c // 16
    wi, xi, ci = lax.axis_index("w"), lax.axis_index("x"), lax.axis_index("c")
    mate, xn, yn = (wi, xi, 1 - ci), (wi, 1 - xi, ci), (1 - wi, xi, ci)
    pa, pb = xi * e, q + wi * e
    fa, fb = pa + wi * sub, pb + xi * sub
    me, peers = _peers(nh, nw)

    def slot(t):
        return jnp.where(t < nt, t, t - second)

    def sem_of(t):
        return jnp.where(t < nt, t, t - second + nt)

    def rows(start, n):
        return pl.ds(pl.multiple_of(start, 8), n)

    def rc(stage, t, src, dst, dev):
        return pltpu.make_async_remote_copy(src_ref=src, dst_ref=dst, send_sem=send.at[stage, sem_of(t)], recv_sem=recv.at[stage, sem_of(t)],
                                            device_id=dev, device_id_type=MESH)

    def tap(k):
        return lax.rem(2 * lax.rem(k, 3) + 1, 3), lax.rem(2 * lax.div(k, 3) + 1, 3)

    def base(t):
        a, b = tap(slot(t))
        return (jnp.where(t < nt, 0, nt) + a * 3 + b) * c + ci * half

    def s0(t):
        return [rc(0, t, dsend.at[lax.rem(slot(t), 2)], recv0.at[lax.rem(slot(t), 2)], mate)]

    def s1(t):
        return [rc(1, t, hown.at[slot(t), rows((1 - xi) * e, e)], recv1.at[slot(t), 0], xn),
                rc(2, t, hown.at[slot(t), rows(q + (1 - wi) * e, e)], recv1.at[slot(t), 1], yn)]

    def s2(t):
        return [rc(3, t, hown.at[slot(t), rows(pa + (1 - wi) * sub, sub)], recv2.at[slot(t), 0], yn),
                rc(4, t, hown.at[slot(t), rows(pb + (1 - xi) * sub, sub)], recv2.at[slot(t), 1], xn)]

    def s3(t):
        return [rc(5, t, hown.at[slot(t), rows(fa, sub)], dw_ref.at[rows(base(t) + fa, sub)], yn),
                rc(6, t, hown.at[slot(t), rows(fb, sub)], dw_ref.at[rows(base(t) + fb, sub)], xn)]

    def keep(t):
        return [pltpu.make_async_copy(hown.at[slot(t), rows(fa, sub)], dw_ref.at[rows(base(t) + fa, sub)], lsem.at[0, sem_of(t)]),
                pltpu.make_async_copy(hown.at[slot(t), rows(fb, sub)], dw_ref.at[rows(base(t) + fb, sub)], lsem.at[1, sem_of(t)])]

    def s4(t):
        return [rc(7, t, dw_ref.at[rows(base(t) + pa, e)], dw_ref.at[rows(base(t) + pa, e)], xn),
                rc(8, t, dw_ref.at[rows(base(t) + pb, e)], dw_ref.at[rows(base(t) + pb, e)], yn)]

    def s5(t):
        return [rc(9, t, dw_ref.at[rows(base(t), half)], dw_ref.at[rows(base(t), half)], mate)]

    def start(cps):
        for cp in cps:
            cp.start()

    def when_chunk(t, f):
        one = jnp.logical_and(t >= 0, t < nt)
        two = jnp.logical_and(t >= second, t < second + nt)

        @pl.when(jnp.logical_or(one, two))
        def _():
            f(t)

    def tick(j):
        def t2(t):
            for cp in s1(t):
                cp.wait_recv()
            hown[slot(t), rows(pa, e), :] += recv1[slot(t), 0]
            hown[slot(t), rows(pb, e), :] += recv1[slot(t), 1]

        def t3(t):
            for cp in s2(t):
                cp.wait_recv()
            hown[slot(t), rows(fa, sub), :] += recv2[slot(t), 0]
            hown[slot(t), rows(fb, sub), :] += recv2[slot(t), 1]

        def t4(t):
            for cp in s3(t):
                cp.wait_recv()
            for cp in keep(t):
                cp.wait()
            for cp in s1(t) + s2(t) + s3(t):
                cp.wait_send()
            start(s4(t))

        def t5(t):
            for cp in s4(t):
                cp.wait_recv()
            start(s5(t))

        def t6(t):
            for cp in s5(t):
                cp.wait_recv()
            for cp in s4(t) + s5(t):
                cp.wait_send()

        lag = 2
        when_chunk(j, lambda t: start(s1(t)))
        when_chunk(j - lag, t2)
        when_chunk(j - 2 * lag, t3)
        when_chunk(j - 3 * lag, t4)
        when_chunk(j - 4 * lag, t5)
        when_chunk(j - lag, lambda t: start(s2(t)))
        when_chunk(j - 2 * lag, lambda t: start(s3(t) + keep(t)))
        when_chunk(j - 5 * lag, t6)

    _, z_start, z_finish = _exchange(nh, nw, [(z_ref, z0_ref, z1_ref, zrows, zcl, zcr)], zsend, zrecv)
    _, a_start, a_finish = _exchange(nh, nw, [(da_ref, e0, e1, arows, acl, acr)], asend, arecv)

    def wcp(ref):
        return pltpu.make_async_copy(ref, wb, wsem)

    def middle(src):
        return pltpu.make_async_copy(src, p.at[1:th + 1, :, c:2 * c], psem.at[2])

    def given(ref):
        return [pltpu.make_async_copy(ref.at[k], p.at[k * (th + 1), :, c:2 * c], psem.at[k]) for k in range(2)]

    def put_rows(ref):
        for k in range(2):
            p[k * (th + 1), :, c:2 * c] = ref[k]

    def run(cps):
        start(cps)
        for cp in cps:
            cp.wait()

    def at(step):
        return pl.when(i == step)

    def within(a, b):
        return pl.when(jnp.logical_and(i >= a, i < b))

    @at(0)
    def _():
        cps = [pltpu.make_async_copy(gt_ref, vt, vsem), middle(z_ref)]
        start(cps)
        _meet(peers)
        z_start()
        wcp(w2_ref).start()
        _fill_same(same)
        sacc[...] = jnp.zeros_like(sacc)
        for cp in cps:
            cp.wait()

    @at(1)
    def _():
        z_finish()
        put_rows(zrows)

    @at(3)
    def _():
        _shift_patches(p, zcl, zcr)

    @at(s_z)
    def _():
        run([middle(g_ref)] + given(grows))
        _shift_patches(p, gcl, gcr)
        wcp(w2_ref).wait()

    @at(s_w + 3)
    def _():
        _shift_patches(p, xcl, xcr)

    def dn_out(k):
        return pltpu.make_async_copy(dnb.at[lax.rem(k, 2)], dn_ref.at[pl.ds(2 * k, 2)], dsem.at[0, lax.rem(k, 2)])

    def dn_in(k):
        return pltpu.make_async_copy(dn_ref.at[pl.ds(2 * k, 2)], dnb.at[lax.rem(k, 2)], dsem.at[1, lax.rem(k, 2)])

    def da_out(k):
        return pltpu.make_async_copy(dab.at[lax.rem(k, 2)], da_ref.at[pl.ds(2 * k, 2)], dsem.at[2, lax.rem(k, 2)])

    @at(s_a)
    def _():
        for k in range(2):
            dn_out(nb - 2 + k).wait()
        start([dn_in(0), middle(x_ref), wcp(w1_ref)] + given(xrows))
        total = _sum_devices(me, peers, sacc, sbuf, ssend, srecv)
        u = _group_means(total * _params(st_ref)[2], same, cnt)
        row = lax.broadcasted_iota(jnp.int32, total.shape, 0)
        t_ref[...] = jnp.where(row < 2, total, jnp.where(row == 2, u[0:1], u[1:2]))

    @at(s_w)
    def _():
        for k in range(2):
            da_out(nb - 2 + k).wait()
        a_start()
        for cp in [middle(x_ref)] + given(xrows):
            cp.wait()

    @at(s_x)
    def _():
        start([middle(da_ref)])
        a_finish()
        middle(da_ref).wait()
        put_rows(arows)
        _shift_patches(p, acl, acr)
        wcp(w1_ref).wait()

    @at(s_y)
    def _():
        cps = [middle(z_ref), wcp(w2_ref)]
        start(cps)
        put_rows(zrows)
        for cp in cps:
            cp.wait()
        _shift_patches(p, zcl, zcr)

    later = i >= s_w
    step = jnp.where(later, i - s_w, i)
    chunk0 = jnp.where(later, second, 0)

    @pl.when(jnp.logical_and(step >= 2, step < nt + 2))
    def _():
        k = step - 2
        for cp in s0(chunk0 + k):
            cp.wait()
        hown[k] += recv0[lax.rem(k, 2)]

    @pl.when(jnp.logical_and(step >= 1, step < nt + 1))
    def _():
        start(s0(chunk0 + step - 1))

    j = jnp.int32(-1)
    now = jnp.int32(0)
    for s in ticks:
        j = j + jnp.where(i >= s, 1, 0)
        now = now + jnp.where(i == s, 1, 0)

    @pl.when(now > 0)
    def _():
        tick(j)

    @pl.when(step < nt)
    def _():
        a, b = tap(step)
        rhs = p[pl.ds(a, th), :, pl.ds(pl.multiple_of(b * c, 128), c)].reshape(th * tw, c)
        d = jnp.dot(vt[...], rhs, preferred_element_type=F32).T
        hown[step] = jnp.where(ci == 0, d[:half], d[half:])
        dsend[lax.rem(step, 2)] = jnp.where(ci == 0, d[half:], d[:half])

    def conv(ib, transposed):
        acc = None
        for a in range(3):
            lhs = p[pl.ds(ib * 2 + a, 2)].reshape(2 * tw, 3 * c)
            if transposed:
                k = nt - 1 - 3 * a
                rhs = jnp.concatenate([wb[k], wb[k - 1], wb[k - 2]], axis=1)
                d = lax.dot_general(lhs, rhs, (((1,), (1,)), ((), ())), preferred_element_type=F32)
            else:
                d = jnp.dot(lhs, wb[3 * a:3 * a + 3].reshape(3 * c, c), preferred_element_type=F32)
            acc = d if acc is None else acc + d
        return acc

    @within(s_z, s_a)
    def _():
        k = i - s_z

        @pl.when(k > 1)
        def _():
            dn_out(k - 2).wait()

        acc = conv(k, True)
        mean, rstd, gamma, beta = _params(st_ref)
        xhat = (ab_ref[...].astype(F32).reshape(acc.shape) - mean) * rstd
        dn = acc * _gelu_grad(xhat * gamma + beta)
        dnb[lax.rem(k, 2)] = dn.reshape(2, tw, c)
        dn_out(k).start()
        row = lax.broadcasted_iota(jnp.int32, sacc.shape, 0)
        sacc[...] += jnp.where(row == 0, (dn * xhat).sum(0, keepdims=True), jnp.where(row == 1, dn.sum(0, keepdims=True), 0.0))

    @within(s_a, s_w)
    def _():
        k = i - s_a

        @pl.when(k + 1 < nb)
        def _():
            dn_in(k + 1).start()

        @pl.when(k > 1)
        def _():
            da_out(k - 2).wait()

        dn_in(k).wait()
        mean, rstd, gamma, _ = _params(st_ref)
        _, _, u0, u1 = _params(t_ref)
        xhat = (ab_ref[...].astype(F32) - mean) * rstd
        da = (rstd * (dnb[lax.rem(k, 2)] * gamma - u1 - xhat * u0)).astype(BF16)
        dab[lax.rem(k, 2)] = da
        _edges(da.astype(F32), e0.at[pl.ds(2 * k, 2)], e1.at[pl.ds(2 * k, 2)])
        vt[:, pl.ds(pl.multiple_of(2 * k * tw, 2 * tw), 2 * tw)] = _transposed(da)
        da_out(k).start()

    @within(s_x, s_y)
    def _():
        _ep_residual(conv(i - s_x, True), gb_ref, dx_ref)

    @pl.when(i >= s_y)
    def _():
        _ep_residual(conv(i - s_y, False), xb_ref, y_ref)


def _main(nh, nw, cnt, z, z0, z1, g, gt, gh, x, xh, w1, w2, st, a):
    th, tw, c = x.shape
    nt, nb, half = 9, th // 2, c // 2
    (_, s_z, _, _, s_x, s_y, end), _, _ = _plan(nt, nb)
    full = _whole(th + 2, 1, c, pipeline_mode=pl.Buffered(1))
    one = _whole(8, c)

    def blocks(first, passes=1):
        return pl.BlockSpec((2, tw, c), lambda i: (lax.rem(jnp.minimum(jnp.maximum(i - first, 0), passes * nb - 1), nb), 0, 0))

    dma = pltpu.SemaphoreType.DMA
    img16, img32 = jax.ShapeDtypeStruct((th, tw, c), BF16), jax.ShapeDtypeStruct((th, tw, c), F32)
    side, edge, hrow = pltpu.VMEM((th + 2, 1, c), F32), pltpu.VMEM((th, 1, c), F32), pltpu.VMEM((2, tw, c), BF16)
    n = nh * nw - 1
    return pl.pallas_call(
        functools.partial(_main_kernel, nh, nw, cnt), grid=(end,),
        out_shape=[img16, img16, jax.ShapeDtypeStruct((8, c), F32), img32, img16, jax.ShapeDtypeStruct((2 * nt * c, c), F32)],
        in_specs=[ANY] * 6 + [full, full, ANY, ANY, full, full, ANY, ANY, one, blocks(s_y), blocks(s_x), blocks(s_z, 2)],
        out_specs=[blocks(s_y), blocks(s_x), one, ANY, ANY, ANY],
        scratch_shapes=[pltpu.VMEM((th + 2, tw, 3 * c), BF16), pltpu.VMEM((c, th * tw), BF16), pltpu.VMEM((nt, c, c), BF16),
                        pltpu.VMEM((2, half, c), F32), pltpu.VMEM((nt, half, c), F32), pltpu.VMEM((2, half, c), F32),
                        pltpu.VMEM((nt, 2, c // 8, c), F32), pltpu.VMEM((nt, 2, c // 16, c), F32),
                        hrow, side, side, hrow, side, side, edge, edge, pltpu.VMEM((2, 2, tw, c), F32), pltpu.VMEM((2, 2, tw, c), BF16),
                        pltpu.VMEM((8, c), F32), pltpu.VMEM((n, 8, c), F32), pltpu.VMEM((c, c), BF16),
                        dma((3,)), dma, dma, dma((10, 2 * nt)), dma((10, 2 * nt)), dma((2, 2 * nt)), dma((8,)), dma((8,)), dma((8,)), dma((8,)), dma((n,)), dma((n,)), dma((3, 2))],
        compiler_params=pltpu.CompilerParams(dimension_semantics=("arbitrary",), vmem_limit_bytes=VMEM_LIMIT, collective_id=5, has_side_effects=True),
        name="main",
    )(z, z0, z1, g, gt, *gh, x, *xh, w1.reshape(nt, c, c), w2.reshape(nt, c, c), st, x, g, a)


def _finish_kernel(*refs):
    n = len(refs) // 2
    for src, dst in zip(refs[:n], refs[n:]):
        dst[...] = src[...]


def solution(mesh):
    nh, nw = mesh.shape["h"], mesh.shape["w"]
    mesh3 = Mesh(mesh.devices.reshape(nw, nh // 2, 2), ("w", "x", "c"))
    tile = P(None, ("x", "c"), "w", None)

    def body(x, w1, gamma, beta, w2, g):
        _, th, tw, c = x.shape
        x, g = x[0], g[0]
        cnt = float(th * nh * tw * nw * (c // GROUPS))
        rb = 2
        blk = pl.BlockSpec((rb, tw, c), lambda i: (i, 0, 0))
        small = _whole(8, c)
        img16 = jax.ShapeDtypeStruct((th, tw, c), BF16)
        img32 = jax.ShapeDtypeStruct((th, tw, c), F32)
        sums = jax.ShapeDtypeStruct((8, c), F32)
        par = jnp.concatenate([jnp.zeros((2, c), F32), gamma[None], beta[None], jnp.zeros((4, c), F32)])

        edge = jax.ShapeDtypeStruct((th, 1, c), F32)
        eblk = pl.BlockSpec((rb, 1, c), lambda i: (i, 0, 0))

        def with_edges(u):
            return u, u[:, 0:1, :].astype(F32), u[:, tw - 1:, :].astype(F32)

        xh, gh = _halo(nh, nw, 0, *with_edges(x), *with_edges(g))
        gt, a, s = _conv("conv1", _ep_conv1, x, xh, w1, g, [img16, sums], [blk, small])
        st = _allsum(nh, nw, cnt, 1, s, par)
        z, *ze = pl.pallas_call(_z_kernel, grid=(th // rb,), out_shape=[img16, edge, edge], in_specs=[blk, small], out_specs=[blk, eblk, eblk], name="act")(a, st)
        y, dx, t, _, _, d = _main(nh, nw, cnt, z, *ze, g, gt, gh, x, xh, w1, w2, st, a)
        rows = d.shape[0] // th
        halves = [pl.BlockSpec((rows, c), lambda i, k=k: (i + k, 0)) for k in (th // 2, 0)]
        own = pl.BlockSpec((rows, c), lambda i: (i, 0))
        wout = jax.ShapeDtypeStruct((d.shape[0] // 2, c), F32)
        y, dx, dw1, dw2 = pl.pallas_call(_finish_kernel, grid=(th // rb,), out_shape=[img16, img16, wout, wout], in_specs=[blk, blk] + halves,
                                         out_specs=[blk, blk, own, own], name="finish")(y, dx, d, d)
        return y[None], dx[None], dw1.reshape(w1.shape), dw2.reshape(w2.shape), t[0], t[1]

    return jax.shard_map(body, mesh=mesh3, in_specs=(tile, P(), P(), P(), P(), tile), out_specs=(tile, tile, P(), P(), P(), P()), check_vma=False)
```

```python
import functools

import jax
import jax.numpy as jnp
from jax import lax
from jax.experimental import pallas as pl
from jax.experimental.pallas import tpu as pltpu
from jax.sharding import Mesh
from jax.sharding import PartitionSpec as P

GROUPS = 32
EPS = 1e-5
F32 = jnp.float32
BF16 = jnp.bfloat16
MESH = pl.DeviceIdType.MESH
VMEM_LIMIT = 67043328
ANY = pl.BlockSpec(memory_space=pl.ANY)
VM = pl.BlockSpec(memory_space=pltpu.VMEM)
GELU_C = 0.7978845608028654
GELU_A = 0.044715


def _whole(*shape, **kw):
    return pl.BlockSpec(shape, lambda i: (0,) * len(shape), **kw)


def _gelu_parts(n):
    n2 = n * n
    t = jnp.tanh(GELU_C * (n + GELU_A * n * n2))
    return n2, t


def _gelu(n):
    _, t = _gelu_parts(n)
    return 0.5 * n * (1.0 + t)


def _gelu_grad(n):
    n2, t = _gelu_parts(n)
    return 0.5 * (1.0 + t) + 0.5 * n * (1.0 - t * t) * (GELU_C * (1.0 + 3.0 * GELU_A * n2))


def _exchange(nh, nw, arrays, send, recv):
    th, tw, c = arrays[0][0].shape
    w = lax.axis_index("w")
    h = lax.axis_index("x") * 2 + lax.axis_index("c")
    dirs = [(dh, dw) for dh in (-1, 0, 1) for dw in (-1, 0, 1) if (dh, dw) != (0, 0)]
    sends = [(k, i, dh, dw) for k in range(len(arrays)) for i, (dh, dw) in enumerate(dirs)]

    def dev(dh, dw):
        hh = h + dh
        return (w + dw, hh // 2, hh % 2)

    def has(dh, dw):
        ok = None
        for cond in ([h > 0] if dh < 0 else [h < nh - 1] if dh > 0 else []) + ([w > 0] if dw < 0 else [w < nw - 1] if dw > 0 else []):
            ok = cond if ok is None else jnp.logical_and(ok, cond)
        return ok

    def landing(k, dh, dw):
        rows, cl, cr = arrays[k][3:]
        side = cr if dw < 0 else cl
        if dw == 0:
            return rows, 1 if dh < 0 else 0
        if dh == 0:
            return side, slice(1, th + 1)
        return side, th + 1 if dh < 0 else 0

    def copy(k, i, dh, dw):
        u, first, last = arrays[k][:3]
        r = 0 if dh < 0 else th - 1
        edge = first if dw < 0 else last
        src = u.at[r] if dw == 0 else edge if dh == 0 else edge.at[r]
        ref, at = landing(k, dh, dw)
        return pltpu.make_async_remote_copy(src_ref=src, dst_ref=ref.at[at], send_sem=send.at[k * 8 + i], recv_sem=recv.at[k * 8 + i],
                                            device_id=dev(dh, dw), device_id_type=MESH)

    def start():
        for k, i, dh, dw in sends:
            @pl.when(has(dh, dw))
            def _(k=k, i=i, dh=dh, dw=dw):
                copy(k, i, dh, dw).start()

    def finish():
        for k, i, dh, dw in sends:
            @pl.when(jnp.logical_not(has(-dh, -dw)))
            def _(k=k, dh=dh, dw=dw):
                ref, at = landing(k, dh, dw)
                ref[at] = jnp.zeros(ref.at[at].shape, ref.dtype)

            @pl.when(has(dh, dw))
            def _(k=k, i=i, dh=dh, dw=dw):
                copy(k, i, dh, dw).wait_send()

            @pl.when(has(-dh, -dw))
            def _(k=k, i=i, dh=dh, dw=dw):
                copy(k, i, dh, dw).wait_recv()

    return start, finish


def _peers(nh, nw):
    n = nh * nw
    me = lax.axis_index("w") * nh + lax.axis_index("x") * 2 + lax.axis_index("c")

    def dev(j):
        hh = lax.rem(j, nh)
        return (lax.div(j, nh), lax.div(hh, 2), lax.rem(hh, 2))

    return me, [dev(lax.rem(me + k, n)) for k in range(1, n)]


def _meet(peers):
    barrier = pltpu.get_barrier_semaphore()
    for d in peers:
        pl.semaphore_signal(barrier, inc=1, device_id=d, device_id_type=MESH)
    pl.semaphore_wait(barrier, len(peers))


def _sum_devices(me, peers, mine, buf, send, recv):
    copies = [pltpu.make_async_remote_copy(src_ref=mine, dst_ref=buf.at[k], send_sem=send.at[k], recv_sem=recv.at[k],
                                           device_id=d, device_id_type=MESH) for k, d in enumerate(peers)]
    for cp in copies:
        cp.start()
    for cp in copies:
        cp.wait()
    n = len(peers) + 1
    vals = [mine[...]] + [buf[k] for k in range(n - 1)]
    total = 0.0
    for j in range(n):
        off = lax.rem(me - j + n, n)
        total = total + sum(jnp.where(off == k, v, 0.0) for k, v in enumerate(vals))
    return total


def _fill_same(same):
    c = same.shape[0]
    gi, gj = [jnp.floor((lax.broadcasted_iota(jnp.int32, (c, c), d).astype(F32) + 0.5) * (GROUPS / c)) for d in range(2)]
    same[...] = jnp.where(gi == gj, 1.0, 0.0).astype(BF16)


def _group_means(v, same, cnt):
    hi = v.astype(BF16)
    rest = v - hi.astype(F32)
    mid = rest.astype(BF16)
    lo = (rest - mid.astype(F32)).astype(BF16)
    return sum(jnp.dot(x, same[...], preferred_element_type=F32) for x in (lo, mid, hi)) / cnt


def _shift_patches(p, cl_ref, cr_ref, r0=0):
    n, tw, c3 = p.shape
    c = c3 // 3
    ck = 128

    def row(r, _):
        idx = lax.broadcasted_iota(jnp.int32, (tw, ck), 0)
        for k in range(c // ck):
            f = p[r, :, c + k * ck:c + (k + 1) * ck].astype(F32)
            lo = cl_ref[r0 + r, :, k * ck:(k + 1) * ck]
            hi = cr_ref[r0 + r, :, k * ck:(k + 1) * ck]
            p[r, :, k * ck:(k + 1) * ck] = jnp.where(idx == 0, lo, pltpu.roll(f, 1, 0)).astype(BF16)
            p[r, :, 2 * c + k * ck:2 * c + (k + 1) * ck] = jnp.where(idx == tw - 1, hi, pltpu.roll(f, tw - 1, 0)).astype(BF16)
        return 0

    lax.fori_loop(0, n, row, 0)


def _transposed(v):
    return v.reshape(v.shape[0] * v.shape[1], v.shape[2]).T


def _put_rows(p, ref):
    th, c = p.shape[0] - 2, ref.shape[2]
    for k in range(2):
        p[k * (th + 1), :, c:2 * c] = ref[k]


def _conv_kernel(nh, nw, cnt, x_ref, x0_ref, x1_ref, g_ref, g0_ref, g1_ref, w_ref, par_ref, gb_ref, gt_ref, a_ref, st_ref, *refs):
    handed, (p, wb, *halo), (sacc, sbuf, same, psem, wsem, hsend, hrecv, ssend, srecv) = refs[:6], refs[6:14], refs[14:]
    i = pl.program_id(0)
    th, tw, c = x_ref.shape
    me, peers = _peers(nh, nw)
    last = th // 2

    @pl.when(i == 0)
    def _():
        xc = pltpu.make_async_copy(x_ref, p.at[1:th + 1, :, c:2 * c], psem)
        wc = pltpu.make_async_copy(w_ref, wb, wsem)
        xc.start()
        wc.start()
        start, finish = _exchange(nh, nw, [(x_ref, x0_ref, x1_ref, *halo[:3]), (g_ref, g0_ref, g1_ref, *halo[3:])], hsend, hrecv)
        _meet(peers)
        start()
        _fill_same(same)
        sacc[...] = jnp.zeros_like(sacc)
        finish()
        for dst, src in zip(handed, halo):
            dst[...] = src[...]
        xc.wait()
        _put_rows(p, halo[0])
        _shift_patches(p, halo[1], halo[2])
        wc.wait()

    @pl.when(i < last)
    def _():
        gt_ref[...] = _transposed(gb_ref[...])
        acc = None
        for a in range(3):
            d = jnp.dot(p[pl.ds(i * 2 + a, 2)].reshape(2 * tw, 3 * c), wb[a], preferred_element_type=F32)
            acc = d if acc is None else acc + d
        a16 = acc.astype(BF16)
        a_ref[...] = a16.reshape(a_ref.shape)
        v = a16.astype(F32)
        row = lax.broadcasted_iota(jnp.int32, sacc.shape, 0)
        sacc[...] += jnp.where(row == 0, v.sum(0, keepdims=True), jnp.where(row == 1, (v * v).sum(0, keepdims=True), 0.0))

    @pl.when(i == last)
    def _():
        m = _group_means(_sum_devices(me, peers, sacc, sbuf, ssend, srecv), same, cnt)
        mean = m[0:1]
        row = lax.broadcasted_iota(jnp.int32, m.shape, 0)
        st_ref[...] = jnp.where(row == 0, mean, jnp.where(row == 1, lax.rsqrt(m[1:2] - mean * mean + EPS), par_ref[...]))


def _conv(nh, nw, cnt, x, xe, g, ge, w, par):
    th, tw, c = x.shape
    n, last = nh * nw - 1, th // 2 - 1
    wshape = (3, 3 * c, c)
    one = _whole(8, c)
    dma = pltpu.SemaphoreType.DMA
    halo = [(2, tw, c), (th + 2, 1, c), (th + 2, 1, c)] * 2
    types = [BF16, F32, F32] * 2
    blk = pl.BlockSpec((2, tw, c), lambda i: (jnp.minimum(i, last), 0, 0))
    return pl.pallas_call(
        functools.partial(_conv_kernel, nh, nw, cnt), grid=(th // 2 + 1,),
        out_shape=[jax.ShapeDtypeStruct((c, th * tw), BF16), jax.ShapeDtypeStruct((th, tw, c), BF16), jax.ShapeDtypeStruct((8, c), F32)]
        + [jax.ShapeDtypeStruct(h, t) for h, t in zip(halo, types)],
        in_specs=[ANY] * 7 + [one, blk], out_specs=[pl.BlockSpec((c, 2 * tw), lambda i: (0, jnp.minimum(i, last))), blk, one] + [_whole(*h) for h in halo],
        scratch_shapes=[pltpu.VMEM((th + 2, tw, 3 * c), BF16), pltpu.VMEM(wshape, BF16)] + [pltpu.VMEM(h, t) for h, t in zip(halo, types)]
        + [pltpu.VMEM((8, c), F32), pltpu.VMEM((n, 8, c), F32), pltpu.VMEM((c, c), BF16), dma, dma, dma((16,)), dma((16,)), dma((n,)), dma((n,))],
        compiler_params=pltpu.CompilerParams(dimension_semantics=("arbitrary",), vmem_limit_bytes=VMEM_LIMIT, collective_id=1, has_side_effects=True),
        name="conv1",
    )(x, *xe, g, *ge, w.reshape(wshape), par, g)


def _ep_residual(acc, r_ref, o_ref):
    o_ref[...] = (acc + r_ref[...].astype(F32).reshape(acc.shape)).astype(BF16).reshape(o_ref.shape)


def _params(st_ref):
    st = st_ref[...]
    return [st[k:k + 1] for k in range(4)]


def _edges(v, first_ref, last_ref):
    first_ref[...] = v[:, 0:1, :]
    last_ref[...] = v[:, v.shape[1] - 1:, :]


def _z_kernel(a_ref, st_ref, z_ref, first_ref, last_ref):
    mean, rstd, gamma, beta = _params(st_ref)
    xhat = (a_ref[...].astype(F32) - mean) * rstd
    z = _gelu(xhat * gamma + beta).astype(BF16)
    z_ref[...] = z
    _edges(z.astype(F32), first_ref, last_ref)


def _plan(nt, nb):
    starts = [0]
    for n in (nt, nb, nb, nt, nb, nb):
        starts.append(starts[-1] + n)
    late = [*range(2, 9), *range(10, 15, 2), *range(16, 25)]
    return starts, [*range(2, 10), 11, 13, 16, 17, 20, 24, 26] + [starts[3] + s for s in late], 15


def _main_kernel(nh, nw, cnt, z_ref, z0_ref, z1_ref, g_ref, gt_ref, grows, gcl, gcr, x_ref, xrows, xcl, xcr, w1_ref, w2_ref, st_ref, xb_ref, gb_ref, ab_ref,
                 y_ref, dx_ref, t_ref, dn_ref, da_ref, dw_ref, hrows, hcl, hcr,
                 p, vt, wb, dsend, hown, recv0, recv1, recv2, zrows, zcl, zcr, arows, acl, acr, e0, e1, dnb, dab, sacc, sbuf, same,
                 psem, wsem, vsem, send, recv, lsem, zsend, zrecv, asend, arecv, ssend, srecv, dsem):
    i = pl.program_id(0)
    th, tw, c = x_ref.shape
    nt, nb = w1_ref.shape[0], th // 2
    (_, s_z, s_a, s_w, s_x, s_y, _), ticks, second = _plan(nt, nb)
    half, q, e, sub = c // 2, c // 4, c // 8, c // 16
    wi, xi, ci = lax.axis_index("w"), lax.axis_index("x"), lax.axis_index("c")
    mate, xn, yn = (wi, xi, 1 - ci), (wi, 1 - xi, ci), (1 - wi, xi, ci)
    pa, pb = xi * e, q + wi * e
    fa, fb = pa + wi * sub, pb + xi * sub
    me, peers = _peers(nh, nw)

    def slot(t):
        return jnp.where(t < nt, t, t - second)

    def sem_of(t):
        return jnp.where(t < nt, t, t - second + nt)

    def rows(start, n):
        return pl.ds(pl.multiple_of(start, 8), n)

    def rc(stage, t, src, dst, dev):
        return pltpu.make_async_remote_copy(src_ref=src, dst_ref=dst, send_sem=send.at[stage, sem_of(t)], recv_sem=recv.at[stage, sem_of(t)],
                                            device_id=dev, device_id_type=MESH)

    def tap(k):
        return lax.rem(2 * lax.rem(k, 3) + 1, 3), lax.rem(2 * lax.div(k, 3) + 1, 3)

    def base(t):
        a, b = tap(slot(t))
        return (jnp.where(t < nt, 0, nt) + a * 3 + b) * c + ci * half

    def s0(t):
        return [rc(0, t, dsend.at[lax.rem(slot(t), 2)], recv0.at[lax.rem(slot(t), 2)], mate)]

    def s1(t):
        return [rc(1, t, hown.at[slot(t), rows((1 - xi) * e, e)], recv1.at[slot(t), 0], xn),
                rc(2, t, hown.at[slot(t), rows(q + (1 - wi) * e, e)], recv1.at[slot(t), 1], yn)]

    def s2(t):
        return [rc(3, t, hown.at[slot(t), rows(pa + (1 - wi) * sub, sub)], recv2.at[slot(t), 0], yn),
                rc(4, t, hown.at[slot(t), rows(pb + (1 - xi) * sub, sub)], recv2.at[slot(t), 1], xn)]

    def s3(t):
        return [rc(5, t, hown.at[slot(t), rows(fa, sub)], dw_ref.at[rows(base(t) + fa, sub)], yn),
                rc(6, t, hown.at[slot(t), rows(fb, sub)], dw_ref.at[rows(base(t) + fb, sub)], xn)]

    def keep(t):
        return [pltpu.make_async_copy(hown.at[slot(t), rows(fa, sub)], dw_ref.at[rows(base(t) + fa, sub)], lsem.at[0, sem_of(t)]),
                pltpu.make_async_copy(hown.at[slot(t), rows(fb, sub)], dw_ref.at[rows(base(t) + fb, sub)], lsem.at[1, sem_of(t)])]

    def s4(t):
        return [rc(7, t, dw_ref.at[rows(base(t) + pa, e)], dw_ref.at[rows(base(t) + pa, e)], xn),
                rc(8, t, dw_ref.at[rows(base(t) + pb, e)], dw_ref.at[rows(base(t) + pb, e)], yn)]

    def s5(t):
        return [rc(9, t, dw_ref.at[rows(base(t), half)], dw_ref.at[rows(base(t), half)], mate)]

    def start(cps):
        for cp in cps:
            cp.start()

    def when_chunk(t, f):
        one = jnp.logical_and(t >= 0, t < nt)
        two = jnp.logical_and(t >= second, t < second + nt)

        @pl.when(jnp.logical_or(one, two))
        def _():
            f(t)

    def tick(j):
        def t2(t):
            for cp in s1(t):
                cp.wait_recv()
            hown[slot(t), rows(pa, e), :] += recv1[slot(t), 0]
            hown[slot(t), rows(pb, e), :] += recv1[slot(t), 1]

        def t3(t):
            for cp in s2(t):
                cp.wait_recv()
            hown[slot(t), rows(fa, sub), :] += recv2[slot(t), 0]
            hown[slot(t), rows(fb, sub), :] += recv2[slot(t), 1]

        def t4(t):
            for cp in s3(t):
                cp.wait_recv()
            for cp in keep(t):
                cp.wait()
            for cp in s1(t) + s2(t) + s3(t):
                cp.wait_send()
            start(s4(t))

        def t5(t):
            for cp in s4(t):
                cp.wait_recv()
            start(s5(t))

        def t6(t):
            for cp in s5(t):
                cp.wait_recv()
            for cp in s4(t) + s5(t):
                cp.wait_send()

        lag = 2
        when_chunk(j, lambda t: start(s1(t)))
        when_chunk(j - lag, t2)
        when_chunk(j - 2 * lag, t3)
        when_chunk(j - 3 * lag, t4)
        when_chunk(j - 4 * lag, t5)
        when_chunk(j - lag, lambda t: start(s2(t)))
        when_chunk(j - 2 * lag, lambda t: start(s3(t) + keep(t)))
        when_chunk(j - 5 * lag, t6)

    z_start, z_finish = _exchange(nh, nw, [(z_ref, z0_ref, z1_ref, zrows, zcl, zcr)], zsend, zrecv)
    a_start, a_finish = _exchange(nh, nw, [(da_ref, e0, e1, arows, acl, acr)], asend, arecv)

    def wcp(ref):
        return pltpu.make_async_copy(ref, wb, wsem)

    def middle(src):
        return pltpu.make_async_copy(src, p.at[1:th + 1, :, c:2 * c], psem.at[2])

    def given(ref):
        return [pltpu.make_async_copy(ref.at[k], p.at[k * (th + 1), :, c:2 * c], psem.at[k]) for k in range(2)]

    def run(cps):
        start(cps)
        for cp in cps:
            cp.wait()

    def at(step):
        return pl.when(i == step)

    def within(a, b):
        return pl.when(jnp.logical_and(i >= a, i < b))

    @at(0)
    def _():
        cps = [pltpu.make_async_copy(gt_ref, vt, vsem), middle(z_ref)]
        start(cps)
        _meet(peers)
        z_start()
        wcp(w2_ref).start()
        _fill_same(same)
        sacc[...] = jnp.zeros_like(sacc)
        for cp in cps:
            cp.wait()

    @at(1)
    def _():
        z_finish()
        _put_rows(p, zrows)

    @at(3)
    def _():
        run([pltpu.make_async_copy(src, dst, psem.at[k]) for k, (src, dst) in enumerate(zip((zrows, zcl, zcr), (hrows, hcl, hcr)))])
        _shift_patches(p, zcl, zcr)

    @at(s_z)
    def _():
        run([middle(g_ref)] + given(grows))
        _shift_patches(p, gcl, gcr)
        wcp(w2_ref).wait()

    @at(s_w + 3)
    def _():
        _shift_patches(p, xcl, xcr)

    def dn_out(k):
        return pltpu.make_async_copy(dnb.at[lax.rem(k, 2)], dn_ref.at[pl.ds(2 * k, 2)], dsem.at[0, lax.rem(k, 2)])

    def dn_in(k):
        return pltpu.make_async_copy(dn_ref.at[pl.ds(2 * k, 2)], dnb.at[lax.rem(k, 2)], dsem.at[1, lax.rem(k, 2)])

    def da_out(k):
        return pltpu.make_async_copy(dab.at[lax.rem(k, 2)], da_ref.at[pl.ds(2 * k, 2)], dsem.at[2, lax.rem(k, 2)])

    @at(s_a)
    def _():
        for k in range(2):
            dn_out(nb - 2 + k).wait()
        start([dn_in(0), middle(x_ref), wcp(w1_ref)] + given(xrows))
        total = _sum_devices(me, peers, sacc, sbuf, ssend, srecv)
        u = _group_means(total * _params(st_ref)[2], same, cnt)
        row = lax.broadcasted_iota(jnp.int32, total.shape, 0)
        t_ref[...] = jnp.where(row < 2, total, jnp.where(row == 2, u[0:1], u[1:2]))

    @at(s_w)
    def _():
        for k in range(2):
            da_out(nb - 2 + k).wait()
        a_start()
        for cp in [middle(x_ref)] + given(xrows):
            cp.wait()

    @at(s_x)
    def _():
        start([middle(da_ref)])
        a_finish()
        middle(da_ref).wait()
        _put_rows(p, arows)
        _shift_patches(p, acl, acr)
        wcp(w1_ref).wait()

    @at(s_y)
    def _():
        cps = [middle(z_ref), wcp(w2_ref)]
        start(cps)
        _put_rows(p, zrows)
        for cp in cps:
            cp.wait()
        _shift_patches(p, zcl, zcr)

    later = i >= s_w
    step = jnp.where(later, i - s_w, i)
    chunk0 = jnp.where(later, second, 0)

    @pl.when(jnp.logical_and(step >= 2, step < nt + 2))
    def _():
        k = step - 2
        for cp in s0(chunk0 + k):
            cp.wait()
        hown[k] += recv0[lax.rem(k, 2)]

    @pl.when(jnp.logical_and(step >= 1, step < nt + 1))
    def _():
        start(s0(chunk0 + step - 1))

    j = jnp.int32(-1)
    now = jnp.int32(0)
    for s in ticks:
        j = j + jnp.where(i >= s, 1, 0)
        now = now + jnp.where(i == s, 1, 0)

    @pl.when(now > 0)
    def _():
        tick(j)

    @pl.when(step < nt)
    def _():
        a, b = tap(step)
        rhs = p[pl.ds(a, th), :, pl.ds(pl.multiple_of(b * c, 128), c)].reshape(th * tw, c)
        d = jnp.dot(vt[...], rhs, preferred_element_type=F32).T
        hown[step] = jnp.where(ci == 0, d[:half], d[half:])
        dsend[lax.rem(step, 2)] = jnp.where(ci == 0, d[half:], d[:half])

    def conv(ib, transposed):
        acc = None
        for a in range(3):
            lhs = p[pl.ds(ib * 2 + a, 2)].reshape(2 * tw, 3 * c)
            if transposed:
                k = nt - 1 - 3 * a
                rhs = jnp.concatenate([wb[k], wb[k - 1], wb[k - 2]], axis=1)
                d = lax.dot_general(lhs, rhs, (((1,), (1,)), ((), ())), preferred_element_type=F32)
            else:
                d = jnp.dot(lhs, wb[3 * a:3 * a + 3].reshape(3 * c, c), preferred_element_type=F32)
            acc = d if acc is None else acc + d
        return acc

    @within(s_z, s_a)
    def _():
        k = i - s_z

        @pl.when(k > 1)
        def _():
            dn_out(k - 2).wait()

        acc = conv(k, True)
        mean, rstd, gamma, beta = _params(st_ref)
        xhat = (ab_ref[...].astype(F32).reshape(acc.shape) - mean) * rstd
        dn = acc * _gelu_grad(xhat * gamma + beta)
        dnb[lax.rem(k, 2)] = dn.reshape(2, tw, c)
        dn_out(k).start()
        row = lax.broadcasted_iota(jnp.int32, sacc.shape, 0)
        sacc[...] += jnp.where(row == 0, (dn * xhat).sum(0, keepdims=True), jnp.where(row == 1, dn.sum(0, keepdims=True), 0.0))

    @within(s_a, s_w)
    def _():
        k = i - s_a

        @pl.when(k + 1 < nb)
        def _():
            dn_in(k + 1).start()

        @pl.when(k > 1)
        def _():
            da_out(k - 2).wait()

        dn_in(k).wait()
        mean, rstd, gamma, _ = _params(st_ref)
        _, _, u0, u1 = _params(t_ref)
        xhat = (ab_ref[...].astype(F32) - mean) * rstd
        da = (rstd * (dnb[lax.rem(k, 2)] * gamma - u1 - xhat * u0)).astype(BF16)
        dab[lax.rem(k, 2)] = da
        _edges(da.astype(F32), e0.at[pl.ds(2 * k, 2)], e1.at[pl.ds(2 * k, 2)])
        vt[:, pl.ds(pl.multiple_of(2 * k * tw, 2 * tw), 2 * tw)] = _transposed(da)
        da_out(k).start()

    @within(s_x, s_y)
    def _():
        _ep_residual(conv(i - s_x, True), gb_ref, dx_ref)

    @within(s_y, s_y + nb // 2)
    def _():
        _ep_residual(conv(i - s_y, False), xb_ref, y_ref)


def _main(nh, nw, cnt, z, z0, z1, g, gt, gh, x, xh, w1, w2, st, a):
    th, tw, c = x.shape
    nt, nb, half = 9, th // 2, c // 2
    (_, s_z, _, _, s_x, s_y, end), _, _ = _plan(nt, nb)
    full = _whole(th + 2, 1, c, pipeline_mode=pl.Buffered(1))
    one = _whole(8, c)

    def blocks(first, count=nb):
        return pl.BlockSpec((2, tw, c), lambda i: (lax.rem(jnp.minimum(jnp.maximum(i - first, 0), count - 1), nb), 0, 0))

    dma = pltpu.SemaphoreType.DMA
    img16, img32 = jax.ShapeDtypeStruct((th, tw, c), BF16), jax.ShapeDtypeStruct((th, tw, c), F32)
    side, edge, hrow = pltpu.VMEM((th + 2, 1, c), F32), pltpu.VMEM((th, 1, c), F32), pltpu.VMEM((2, tw, c), BF16)
    n = nh * nw - 1
    return pl.pallas_call(
        functools.partial(_main_kernel, nh, nw, cnt), grid=(end,),
        out_shape=[jax.ShapeDtypeStruct((nb, tw, c), BF16), img16, jax.ShapeDtypeStruct((8, c), F32), img32, img16, jax.ShapeDtypeStruct((2 * nt * c, c), F32)]
        + [jax.ShapeDtypeStruct(h.shape, h.dtype) for h in gh],
        in_specs=[ANY] * 6 + [full, full, ANY, ANY, full, full, ANY, ANY, one, blocks(s_y, nb // 2), blocks(s_x), blocks(s_z, 2 * nb)],
        out_specs=[blocks(s_y, nb // 2), blocks(s_x), one] + [ANY] * 6,
        scratch_shapes=[pltpu.VMEM((th + 2, tw, 3 * c), BF16), pltpu.VMEM((c, th * tw), BF16), pltpu.VMEM((nt, c, c), BF16),
                        pltpu.VMEM((2, half, c), F32), pltpu.VMEM((nt, half, c), F32), pltpu.VMEM((2, half, c), F32),
                        pltpu.VMEM((nt, 2, c // 8, c), F32), pltpu.VMEM((nt, 2, c // 16, c), F32),
                        hrow, side, side, hrow, side, side, edge, edge, pltpu.VMEM((2, 2, tw, c), F32), pltpu.VMEM((2, 2, tw, c), BF16),
                        pltpu.VMEM((8, c), F32), pltpu.VMEM((n, 8, c), F32), pltpu.VMEM((c, c), BF16),
                        dma((3,)), dma, dma, dma((10, 2 * nt)), dma((10, 2 * nt)), dma((2, 2 * nt)), dma((8,)), dma((8,)), dma((8,)), dma((8,)), dma((n,)), dma((n,)), dma((3, 2))],
        compiler_params=pltpu.CompilerParams(dimension_semantics=("arbitrary",), vmem_limit_bytes=VMEM_LIMIT, collective_id=5, has_side_effects=True),
        name="main",
    )(z, z0, z1, g, gt, *gh, x, *xh, w1.reshape(nt, c, c), w2.reshape(nt, c, c), st, x, g, a)


def _finish_kernel(z_ref, rows_ref, cl_ref, cr_ref, w_ref, xb_ref, y0_ref, dx0_ref, d1_ref, d2_ref, y_ref, dx_ref, dw1_ref, dw2_ref,
                   p, wb, yb, psem, wsem, ysem, csem):
    i = pl.program_id(0)
    steps = pl.num_programs(0)
    th, tw, c = z_ref.shape
    r0 = th // 2
    n = th - r0 + 1

    def yout(k):
        return pltpu.make_async_copy(yb.at[lax.rem(k, 2)], y_ref.at[r0 + k], ysem.at[lax.rem(k, 2)])

    ycopy = pltpu.make_async_copy(y0_ref.at[0], y_ref.at[i], csem)
    ycopy.start()

    @pl.when(i == 0)
    def _():
        cps = [pltpu.make_async_copy(z_ref.at[r0 - 1:], p.at[:n, :, c:2 * c], psem.at[0]),
               pltpu.make_async_copy(rows_ref.at[1], p.at[n, :, c:2 * c], psem.at[1])]
        wc = pltpu.make_async_copy(w_ref, wb, wsem)
        for cp in cps + [wc]:
            cp.start()
        for cp in cps:
            cp.wait()
        _shift_patches(p, cl_ref, cr_ref, r0)
        wc.wait()

    @pl.when(i > 1)
    def _():
        yout(i - 2).wait()

    for src, dst in ((dx0_ref, dx_ref), (d1_ref, dw1_ref), (d2_ref, dw2_ref)):
        dst[...] = src[...]
    acc = None
    for a in range(3):
        d = jnp.dot(p[i + a], wb[a], preferred_element_type=F32)
        acc = d if acc is None else acc + d
    yb[lax.rem(i, 2)] = (acc + xb_ref[0].astype(F32)).astype(BF16)
    yout(i).start()
    ycopy.wait()

    @pl.when(i == steps - 1)
    def _():
        yout(i - 1).wait()
        yout(i).wait()


def _finish(z, zh, w, x, y0, dx0, d):
    th, tw, c = x.shape
    steps = th // 2
    rows = d.shape[0] // th
    wshape = (3, 3 * c, c)
    dma = pltpu.SemaphoreType.DMA
    full = _whole(th + 2, 1, c)

    def part(k):
        return pl.BlockSpec((rows, c), lambda i: (i + k, 0))

    def img(n, k=0):
        return pl.BlockSpec((n, tw, c), lambda i: (i + k, 0, 0))

    wout = jax.ShapeDtypeStruct((d.shape[0] // 2, c), F32)
    iout = jax.ShapeDtypeStruct((th, tw, c), BF16)
    return pl.pallas_call(
        _finish_kernel, grid=(steps,), out_shape=[iout, iout, wout, wout],
        in_specs=[ANY, ANY, full, full, ANY, img(1, steps), img(1), img(2), part(steps), part(0)], out_specs=[ANY, img(2), part(0), part(0)],
        scratch_shapes=[pltpu.VMEM((steps + 2, tw, 3 * c), BF16), pltpu.VMEM(wshape, BF16), pltpu.VMEM((2, tw, c), BF16), dma((2,)), dma, dma((2,)), dma],
        compiler_params=pltpu.CompilerParams(dimension_semantics=("arbitrary",), vmem_limit_bytes=VMEM_LIMIT), name="finish",
    )(z, *zh, w.reshape(wshape), x, y0, dx0, d, d)


def solution(mesh):
    nh, nw = mesh.shape["h"], mesh.shape["w"]
    mesh3 = Mesh(mesh.devices.reshape(nw, nh // 2, 2), ("w", "x", "c"))
    tile = P(None, ("x", "c"), "w", None)

    def body(x, w1, gamma, beta, w2, g):
        _, th, tw, c = x.shape
        x, g = x[0], g[0]
        cnt = float(th * nh * tw * nw * (c // GROUPS))
        rb = 2
        blk = pl.BlockSpec((rb, tw, c), lambda i: (i, 0, 0))
        small = _whole(8, c)
        img16 = jax.ShapeDtypeStruct((th, tw, c), BF16)
        par = jnp.concatenate([jnp.zeros((2, c), F32), gamma[None], beta[None], jnp.zeros((4, c), F32)])

        edge = jax.ShapeDtypeStruct((th, 1, c), F32)
        eblk = pl.BlockSpec((rb, 1, c), lambda i: (i, 0, 0))

        def edges(u):
            return u[:, 0:1, :].astype(F32), u[:, tw - 1:, :].astype(F32)

        gt, a, st, *halos = _conv(nh, nw, cnt, x, edges(x), g, edges(g), w1, par)
        xh, gh = halos[:3], halos[3:]
        z, *ze = pl.pallas_call(_z_kernel, grid=(th // rb,), out_shape=[img16, edge, edge], in_specs=[blk, small], out_specs=[blk, eblk, eblk], name="act")(a, st)
        y, dx, t, _, _, d, *zh = _main(nh, nw, cnt, z, *ze, g, gt, gh, x, xh, w1, w2, st, a)
        y, dx, dw1, dw2 = _finish(z, zh, w2, x, y, dx, d)
        return y[None], dx[None], dw1.reshape(w1.shape), dw2.reshape(w2.shape), t[0], t[1]

    return jax.shard_map(body, mesh=mesh3, in_specs=(tile, P(), P(), P(), P(), tile), out_specs=(tile, tile, P(), P(), P(), P()), check_vma=False)
```

```python
import functools

import jax
import jax.numpy as jnp
from jax import lax
from jax.experimental import pallas as pl
from jax.experimental.pallas import tpu as pltpu
from jax.sharding import Mesh
from jax.sharding import PartitionSpec as P

GROUPS = 32
EPS = 1e-5
F32 = jnp.float32
BF16 = jnp.bfloat16
MESH = pl.DeviceIdType.MESH
VMEM_LIMIT = 67043328
ANY = pl.BlockSpec(memory_space=pl.ANY)
VM = pl.BlockSpec(memory_space=pltpu.VMEM)
LAST = 4
GELU_C = 0.7978845608028654
GELU_A = 0.044715


def _whole(*shape, **kw):
    return pl.BlockSpec(shape, lambda i: (0,) * len(shape), **kw)


def _gelu_parts(n):
    n2 = n * n
    t = jnp.tanh(GELU_C * (n + GELU_A * n * n2))
    return n2, t


def _gelu(n):
    _, t = _gelu_parts(n)
    return 0.5 * n * (1.0 + t)


def _gelu_grad(n):
    n2, t = _gelu_parts(n)
    return 0.5 * (1.0 + t) + 0.5 * n * (1.0 - t * t) * (GELU_C * (1.0 + 3.0 * GELU_A * n2))


def _exchange(nh, nw, u, first, last, rows, cl, cr, send, recv):
    th = u.shape[0]
    w = lax.axis_index("w")
    h = lax.axis_index("x") * 2 + lax.axis_index("c")
    dirs = [(dh, dw) for dh in (-1, 0, 1) for dw in (-1, 0, 1) if (dh, dw) != (0, 0)]

    def dev(dh, dw):
        hh = h + dh
        return (w + dw, hh // 2, hh % 2)

    def has(dh, dw):
        ok = None
        for cond in ([h > 0] if dh < 0 else [h < nh - 1] if dh > 0 else []) + ([w > 0] if dw < 0 else [w < nw - 1] if dw > 0 else []):
            ok = cond if ok is None else jnp.logical_and(ok, cond)
        return ok

    def landing(dh, dw):
        side = cr if dw < 0 else cl
        if dw == 0:
            return rows, 1 if dh < 0 else 0
        if dh == 0:
            return side, slice(1, th + 1)
        return side, th + 1 if dh < 0 else 0

    def copy(i, dh, dw):
        r = 0 if dh < 0 else th - 1
        edge = first if dw < 0 else last
        src = u.at[r] if dw == 0 else edge if dh == 0 else edge.at[r]
        ref, at = landing(dh, dw)
        return pltpu.make_async_remote_copy(src_ref=src, dst_ref=ref.at[at], send_sem=send.at[i], recv_sem=recv.at[i],
                                            device_id=dev(dh, dw), device_id_type=MESH)

    def start():
        for i, (dh, dw) in enumerate(dirs):
            @pl.when(has(dh, dw))
            def _(i=i, dh=dh, dw=dw):
                copy(i, dh, dw).start()

    def finish():
        for i, (dh, dw) in enumerate(dirs):
            @pl.when(jnp.logical_not(has(-dh, -dw)))
            def _(dh=dh, dw=dw):
                ref, at = landing(dh, dw)
                ref[at] = jnp.zeros(ref.at[at].shape, ref.dtype)

            @pl.when(has(dh, dw))
            def _(i=i, dh=dh, dw=dw):
                copy(i, dh, dw).wait_send()

            @pl.when(has(-dh, -dw))
            def _(i=i, dh=dh, dw=dw):
                copy(i, dh, dw).wait_recv()

    return start, finish


def _peers(nh, nw):
    n = nh * nw
    me = lax.axis_index("w") * nh + lax.axis_index("x") * 2 + lax.axis_index("c")

    def dev(j):
        hh = lax.rem(j, nh)
        return (lax.div(j, nh), lax.div(hh, 2), lax.rem(hh, 2))

    return me, [dev(lax.rem(me + k, n)) for k in range(1, n)]


def _meet(peers):
    barrier = pltpu.get_barrier_semaphore()
    for d in peers:
        pl.semaphore_signal(barrier, inc=1, device_id=d, device_id_type=MESH)
    pl.semaphore_wait(barrier, len(peers))


def _sum_devices(me, peers, mine, buf, send, recv):
    copies = [pltpu.make_async_remote_copy(src_ref=mine, dst_ref=buf.at[k], send_sem=send.at[k], recv_sem=recv.at[k],
                                           device_id=d, device_id_type=MESH) for k, d in enumerate(peers)]
    for cp in copies:
        cp.start()
    for cp in copies:
        cp.wait()
    n = len(peers) + 1
    vals = [mine[...]] + [buf[k] for k in range(n - 1)]
    total = 0.0
    for j in range(n):
        off = lax.rem(me - j + n, n)
        total = total + sum(jnp.where(off == k, v, 0.0) for k, v in enumerate(vals))
    return total


def _fill_same(same):
    c = same.shape[0]
    gi, gj = [jnp.floor((lax.broadcasted_iota(jnp.int32, (c, c), d).astype(F32) + 0.5) * (GROUPS / c)) for d in range(2)]
    same[...] = jnp.where(gi == gj, 1.0, 0.0).astype(BF16)


def _group_means(v, same, cnt):
    hi = v.astype(BF16)
    rest = v - hi.astype(F32)
    mid = rest.astype(BF16)
    lo = (rest - mid.astype(F32)).astype(BF16)
    return sum(jnp.dot(x, same[...], preferred_element_type=F32) for x in (lo, mid, hi)) / cnt


def _shift_patches(p, cl_ref, cr_ref, r0=0):
    n, tw, c3 = p.shape
    c = c3 // 3
    ck = 128

    def row(r, _):
        idx = lax.broadcasted_iota(jnp.int32, (tw, ck), 0)
        for k in range(c // ck):
            f = p[r, :, c + k * ck:c + (k + 1) * ck].astype(F32)
            lo = cl_ref[r0 + r, :, k * ck:(k + 1) * ck]
            hi = cr_ref[r0 + r, :, k * ck:(k + 1) * ck]
            p[r, :, k * ck:(k + 1) * ck] = jnp.where(idx == 0, lo, pltpu.roll(f, 1, 0)).astype(BF16)
            p[r, :, 2 * c + k * ck:2 * c + (k + 1) * ck] = jnp.where(idx == tw - 1, hi, pltpu.roll(f, tw - 1, 0)).astype(BF16)
        return 0

    lax.fori_loop(0, n, row, 0)


def _transposed(v):
    return v.reshape(v.shape[0] * v.shape[1], v.shape[2]).T


def _put_rows(p, ref):
    th, c = p.shape[0] - 2, ref.shape[2]
    for k in range(2):
        p[k * (th + 1), :, c:2 * c] = ref[k]


def _conv_kernel(nh, nw, cnt, x_ref, x0_ref, x1_ref, g_ref, g0_ref, g1_ref, w_ref, par_ref, gb_ref, gt_ref, a_ref, st_ref, *refs):
    handed, (p, wb, *halo), (sacc, sbuf, same, psem, wsem, hsend, hrecv, ssend, srecv) = refs[:6], refs[6:14], refs[14:]
    i = pl.program_id(0)
    th, tw, c = x_ref.shape
    me, peers = _peers(nh, nw)
    last = th // 2
    x_start, x_finish = _exchange(nh, nw, x_ref, x0_ref, x1_ref, *halo[:3], hsend.at[0], hrecv.at[0])
    g_start, g_finish = _exchange(nh, nw, g_ref, g0_ref, g1_ref, *halo[3:], hsend.at[1], hrecv.at[1])

    @pl.when(i == 0)
    def _():
        xc = pltpu.make_async_copy(x_ref, p.at[1:th + 1, :, c:2 * c], psem)
        wc = pltpu.make_async_copy(w_ref, wb, wsem)
        xc.start()
        wc.start()
        _meet(peers)
        x_start()
        g_start()
        _fill_same(same)
        sacc[...] = jnp.zeros_like(sacc)
        x_finish()
        xc.wait()
        _put_rows(p, halo[0])
        _shift_patches(p, halo[1], halo[2])
        wc.wait()

    @pl.when(i < last)
    def _():
        gt_ref[...] = _transposed(gb_ref[...])
        acc = None
        for a in range(3):
            d = jnp.dot(p[pl.ds(i * 2 + a, 2)].reshape(2 * tw, 3 * c), wb[a], preferred_element_type=F32)
            acc = d if acc is None else acc + d
        a16 = acc.astype(BF16)
        a_ref[...] = a16.reshape(a_ref.shape)
        v = a16.astype(F32)
        row = lax.broadcasted_iota(jnp.int32, sacc.shape, 0)
        sacc[...] += jnp.where(row == 0, v.sum(0, keepdims=True), jnp.where(row == 1, (v * v).sum(0, keepdims=True), 0.0))

    @pl.when(i == last)
    def _():
        g_finish()
        for dst, src in zip(handed, halo):
            dst[...] = src[...]
        m = _group_means(_sum_devices(me, peers, sacc, sbuf, ssend, srecv), same, cnt)
        mean = m[0:1]
        row = lax.broadcasted_iota(jnp.int32, m.shape, 0)
        st_ref[...] = jnp.where(row == 0, mean, jnp.where(row == 1, lax.rsqrt(m[1:2] - mean * mean + EPS), par_ref[...]))


def _conv(nh, nw, cnt, x, xe, g, ge, w, par):
    th, tw, c = x.shape
    n, last = nh * nw - 1, th // 2 - 1
    wshape = (3, 3 * c, c)
    one = _whole(8, c)
    dma = pltpu.SemaphoreType.DMA
    halo = [(2, tw, c), (th + 2, 1, c), (th + 2, 1, c)] * 2
    types = [BF16, F32, F32] * 2
    blk = pl.BlockSpec((2, tw, c), lambda i: (jnp.minimum(i, last), 0, 0))
    return pl.pallas_call(
        functools.partial(_conv_kernel, nh, nw, cnt), grid=(th // 2 + 1,),
        out_shape=[jax.ShapeDtypeStruct((c, th * tw), BF16), jax.ShapeDtypeStruct((th, tw, c), BF16), jax.ShapeDtypeStruct((8, c), F32)]
        + [jax.ShapeDtypeStruct(h, t) for h, t in zip(halo, types)],
        in_specs=[ANY] * 7 + [one, blk], out_specs=[pl.BlockSpec((c, 2 * tw), lambda i: (0, jnp.minimum(i, last))), blk, one] + [_whole(*h) for h in halo],
        scratch_shapes=[pltpu.VMEM((th + 2, tw, 3 * c), BF16), pltpu.VMEM(wshape, BF16)] + [pltpu.VMEM(h, t) for h, t in zip(halo, types)]
        + [pltpu.VMEM((8, c), F32), pltpu.VMEM((n, 8, c), F32), pltpu.VMEM((c, c), BF16), dma, dma, dma((2, 8)), dma((2, 8)), dma((n,)), dma((n,))],
        compiler_params=pltpu.CompilerParams(dimension_semantics=("arbitrary",), vmem_limit_bytes=VMEM_LIMIT, collective_id=1, has_side_effects=True),
        name="conv1",
    )(x, *xe, g, *ge, w.reshape(wshape), par, g)


def _ep_residual(acc, r_ref, o_ref):
    o_ref[...] = (acc + r_ref[...].astype(F32).reshape(acc.shape)).astype(BF16).reshape(o_ref.shape)


def _params(st_ref):
    st = st_ref[...]
    return [st[k:k + 1] for k in range(4)]


def _edges(v, first_ref, last_ref):
    first_ref[...] = v[:, 0:1, :]
    last_ref[...] = v[:, v.shape[1] - 1:, :]


def _z_kernel(a_ref, st_ref, z_ref, first_ref, last_ref):
    mean, rstd, gamma, beta = _params(st_ref)
    xhat = (a_ref[...].astype(F32) - mean) * rstd
    z = _gelu(xhat * gamma + beta).astype(BF16)
    z_ref[...] = z
    _edges(z.astype(F32), first_ref, last_ref)


def _plan(nt, nb):
    starts = [0]
    for n in (nt, nb, nb, nt, nb, nb):
        starts.append(starts[-1] + n)
    late = [*range(2, 9), *range(10, 15, 2), *range(16, 25)]
    return starts, [*range(2, 11), *range(12, 17), 18, 20, 23, 25] + [starts[3] + s for s in late], 18


def _main_kernel(nh, nw, cnt, z_ref, z0_ref, z1_ref, g_ref, gt_ref, grows, gcl, gcr, x_ref, xrows, xcl, xcr, w1_ref, w2_ref, st_ref, xb_ref, gb_ref, ab_ref,
                 y_ref, dx_ref, t_ref, dn_ref, da_ref, dw_ref, hrows, hcl, hcr,
                 p, vt, wb, dsend, hown, recv0, recv1, recv2, zrows, zcl, zcr, arows, acl, acr, e0, e1, dnb, dab, sacc, sbuf, same,
                 psem, wsem, vsem, send, recv, lsem, zsend, zrecv, asend, arecv, ssend, srecv, dsem):
    i = pl.program_id(0)
    th, tw, c = x_ref.shape
    nt, nb = w1_ref.shape[0], th // 2
    (_, s_z, s_a, s_w, s_x, s_y, _), ticks, second = _plan(nt, nb)
    half, q, e, sub = c // 2, c // 4, c // 8, c // 16
    wi, xi, ci = lax.axis_index("w"), lax.axis_index("x"), lax.axis_index("c")
    mate, xn, yn = (wi, xi, 1 - ci), (wi, 1 - xi, ci), (1 - wi, xi, ci)
    pa, pb = xi * e, q + wi * e
    fa, fb = pa + wi * sub, pb + xi * sub
    me, peers = _peers(nh, nw)

    def slot(t):
        return jnp.where(t < nt, t, t - second)

    def sem_of(t):
        return jnp.where(t < nt, t, t - second + nt)

    def rows(start, n):
        return pl.ds(pl.multiple_of(start, 8), n)

    def rc(stage, t, src, dst, dev):
        return pltpu.make_async_remote_copy(src_ref=src, dst_ref=dst, send_sem=send.at[stage, sem_of(t)], recv_sem=recv.at[stage, sem_of(t)],
                                            device_id=dev, device_id_type=MESH)

    def tap(k):
        return lax.rem(2 * lax.rem(k, 3) + 1, 3), lax.rem(2 * lax.div(k, 3) + 1, 3)

    def base(t):
        a, b = tap(slot(t))
        return (jnp.where(t < nt, 0, nt) + a * 3 + b) * c + ci * half

    def s0(t):
        return [rc(0, t, dsend.at[lax.rem(slot(t), 2)], recv0.at[lax.rem(slot(t), 2)], mate)]

    def s1(t):
        return [rc(1, t, hown.at[slot(t), rows((1 - xi) * e, e)], recv1.at[slot(t), 0], xn),
                rc(2, t, hown.at[slot(t), rows(q + (1 - wi) * e, e)], recv1.at[slot(t), 1], yn)]

    def s2(t):
        return [rc(3, t, hown.at[slot(t), rows(pa + (1 - wi) * sub, sub)], recv2.at[slot(t), 0], yn),
                rc(4, t, hown.at[slot(t), rows(pb + (1 - xi) * sub, sub)], recv2.at[slot(t), 1], xn)]

    def s3(t):
        return [rc(5, t, hown.at[slot(t), rows(fa, sub)], dw_ref.at[rows(base(t) + fa, sub)], yn),
                rc(6, t, hown.at[slot(t), rows(fb, sub)], dw_ref.at[rows(base(t) + fb, sub)], xn)]

    def keep(t):
        return [pltpu.make_async_copy(hown.at[slot(t), rows(fa, sub)], dw_ref.at[rows(base(t) + fa, sub)], lsem.at[0, sem_of(t)]),
                pltpu.make_async_copy(hown.at[slot(t), rows(fb, sub)], dw_ref.at[rows(base(t) + fb, sub)], lsem.at[1, sem_of(t)])]

    def s4(t):
        return [rc(7, t, dw_ref.at[rows(base(t) + pa, e)], dw_ref.at[rows(base(t) + pa, e)], xn),
                rc(8, t, dw_ref.at[rows(base(t) + pb, e)], dw_ref.at[rows(base(t) + pb, e)], yn)]

    def s5(t):
        return [rc(9, t, dw_ref.at[rows(base(t), half)], dw_ref.at[rows(base(t), half)], mate)]

    def start(cps):
        for cp in cps:
            cp.start()

    def when_chunk(j, stages, f):
        for first, lag in ((0, 3), (second, 2)):
            t = j - stages * lag

            @pl.when(jnp.logical_and(t >= first, t < first + nt))
            def _(t=t):
                f(t)

    def tick(j):
        def t2(t):
            for cp in s1(t):
                cp.wait_recv()
            hown[slot(t), rows(pa, e), :] += recv1[slot(t), 0]
            hown[slot(t), rows(pb, e), :] += recv1[slot(t), 1]

        def t3(t):
            for cp in s2(t):
                cp.wait_recv()
            hown[slot(t), rows(fa, sub), :] += recv2[slot(t), 0]
            hown[slot(t), rows(fb, sub), :] += recv2[slot(t), 1]

        def t4(t):
            for cp in s3(t):
                cp.wait_recv()
            for cp in keep(t):
                cp.wait()
            for cp in s1(t) + s2(t) + s3(t):
                cp.wait_send()
            start(s4(t))

        def t5(t):
            for cp in s4(t):
                cp.wait_recv()
            start(s5(t))

        def t6(t):
            for cp in s5(t):
                cp.wait_recv()
            for cp in s4(t) + s5(t):
                cp.wait_send()

        when_chunk(j, 0, lambda t: start(s1(t)))
        for stages, f in enumerate((t2, t3, t4, t5)):
            when_chunk(j, stages + 1, f)
        when_chunk(j, 1, lambda t: start(s2(t)))
        when_chunk(j, 2, lambda t: start(s3(t) + keep(t)))
        when_chunk(j, 5, t6)

    z_start, z_finish = _exchange(nh, nw, z_ref, z0_ref, z1_ref, zrows, zcl, zcr, zsend, zrecv)
    a_start, a_finish = _exchange(nh, nw, da_ref, e0, e1, arows, acl, acr, asend, arecv)

    def wcp(ref):
        return pltpu.make_async_copy(ref, wb, wsem)

    def middle(src):
        return pltpu.make_async_copy(src, p.at[1:th + 1, :, c:2 * c], psem.at[2])

    def given(ref):
        return [pltpu.make_async_copy(ref.at[k], p.at[k * (th + 1), :, c:2 * c], psem.at[k]) for k in range(2)]

    def run(cps):
        start(cps)
        for cp in cps:
            cp.wait()

    def at(step):
        return pl.when(i == step)

    def within(a, b):
        return pl.when(jnp.logical_and(i >= a, i < b))

    @at(0)
    def _():
        cps = [pltpu.make_async_copy(gt_ref, vt, vsem), middle(z_ref)]
        start(cps)
        _meet(peers)
        z_start()
        wcp(w2_ref).start()
        _fill_same(same)
        sacc[...] = jnp.zeros_like(sacc)
        for cp in cps:
            cp.wait()

    @at(1)
    def _():
        z_finish()
        _put_rows(p, zrows)

    @at(3)
    def _():
        run([pltpu.make_async_copy(src, dst, psem.at[k]) for k, (src, dst) in enumerate(zip((zrows, zcl, zcr), (hrows, hcl, hcr)))])
        _shift_patches(p, zcl, zcr)

    @at(s_z)
    def _():
        run([middle(g_ref)] + given(grows))
        _shift_patches(p, gcl, gcr)
        wcp(w2_ref).wait()

    @at(s_w + 3)
    def _():
        _shift_patches(p, xcl, xcr)

    def dn_out(k):
        return pltpu.make_async_copy(dnb.at[lax.rem(k, 2)], dn_ref.at[pl.ds(2 * k, 2)], dsem.at[0, lax.rem(k, 2)])

    def dn_in(k):
        return pltpu.make_async_copy(dn_ref.at[pl.ds(2 * k, 2)], dnb.at[lax.rem(k, 2)], dsem.at[1, lax.rem(k, 2)])

    def da_out(k):
        return pltpu.make_async_copy(dab.at[lax.rem(k, 2)], da_ref.at[pl.ds(2 * k, 2)], dsem.at[2, lax.rem(k, 2)])

    @at(s_a)
    def _():
        for k in range(2):
            dn_out(nb - 2 + k).wait()
        start([dn_in(0), middle(x_ref), wcp(w1_ref)] + given(xrows))
        total = _sum_devices(me, peers, sacc, sbuf, ssend, srecv)
        u = _group_means(total * _params(st_ref)[2], same, cnt)
        row = lax.broadcasted_iota(jnp.int32, total.shape, 0)
        t_ref[...] = jnp.where(row < 2, total, jnp.where(row == 2, u[0:1], u[1:2]))

    @at(s_w)
    def _():
        for k in range(2):
            da_out(nb - 2 + k).wait()
        a_start()
        for cp in [middle(x_ref)] + given(xrows):
            cp.wait()

    @at(s_x)
    def _():
        start([middle(da_ref)])
        a_finish()
        middle(da_ref).wait()
        _put_rows(p, arows)
        _shift_patches(p, acl, acr)
        wcp(w1_ref).wait()

    @at(s_y)
    def _():
        cps = [middle(z_ref), wcp(w2_ref)]
        start(cps)
        _put_rows(p, zrows)
        for cp in cps:
            cp.wait()
        _shift_patches(p, zcl, zcr)

    later = i >= s_w
    step = jnp.where(later, i - s_w, i)
    chunk0 = jnp.where(later, second, 0)

    @pl.when(jnp.logical_and(step >= 2, step < nt + 2))
    def _():
        k = step - 2
        for cp in s0(chunk0 + k):
            cp.wait()
        hown[k] += recv0[lax.rem(k, 2)]

    @pl.when(jnp.logical_and(step >= 1, step < nt + 1))
    def _():
        start(s0(chunk0 + step - 1))

    j = jnp.int32(-1)
    now = jnp.int32(0)
    for s in ticks:
        j = j + jnp.where(i >= s, 1, 0)
        now = now + jnp.where(i == s, 1, 0)

    @pl.when(now > 0)
    def _():
        tick(j)

    @pl.when(step < nt)
    def _():
        a, b = tap(step)
        rhs = p[pl.ds(a, th), :, pl.ds(pl.multiple_of(b * c, 128), c)].reshape(th * tw, c)
        d = jnp.dot(vt[...], rhs, preferred_element_type=F32).T
        hown[step] = jnp.where(ci == 0, d[:half], d[half:])
        dsend[lax.rem(step, 2)] = jnp.where(ci == 0, d[half:], d[:half])

    def conv(ib, transposed):
        acc = None
        for a in range(3):
            lhs = p[pl.ds(ib * 2 + a, 2)].reshape(2 * tw, 3 * c)
            if transposed:
                k = nt - 1 - 3 * a
                rhs = jnp.concatenate([wb[k], wb[k - 1], wb[k - 2]], axis=1)
                d = lax.dot_general(lhs, rhs, (((1,), (1,)), ((), ())), preferred_element_type=F32)
            else:
                d = jnp.dot(lhs, wb[3 * a:3 * a + 3].reshape(3 * c, c), preferred_element_type=F32)
            acc = d if acc is None else acc + d
        return acc

    @within(s_z, s_a)
    def _():
        k = i - s_z

        @pl.when(k > 1)
        def _():
            dn_out(k - 2).wait()

        acc = conv(k, True)
        mean, rstd, gamma, beta = _params(st_ref)
        xhat = (ab_ref[...].astype(F32).reshape(acc.shape) - mean) * rstd
        dn = acc * _gelu_grad(xhat * gamma + beta)
        dnb[lax.rem(k, 2)] = dn.reshape(2, tw, c)
        dn_out(k).start()
        row = lax.broadcasted_iota(jnp.int32, sacc.shape, 0)
        sacc[...] += jnp.where(row == 0, (dn * xhat).sum(0, keepdims=True), jnp.where(row == 1, dn.sum(0, keepdims=True), 0.0))

    @within(s_a, s_w)
    def _():
        k = i - s_a

        @pl.when(k + 1 < nb)
        def _():
            dn_in(k + 1).start()

        @pl.when(k > 1)
        def _():
            da_out(k - 2).wait()

        dn_in(k).wait()
        mean, rstd, gamma, _ = _params(st_ref)
        _, _, u0, u1 = _params(t_ref)
        xhat = (ab_ref[...].astype(F32) - mean) * rstd
        da = (rstd * (dnb[lax.rem(k, 2)] * gamma - u1 - xhat * u0)).astype(BF16)
        dab[lax.rem(k, 2)] = da
        _edges(da.astype(F32), e0.at[pl.ds(2 * k, 2)], e1.at[pl.ds(2 * k, 2)])
        vt[:, pl.ds(pl.multiple_of(2 * k * tw, 2 * tw), 2 * tw)] = _transposed(da)
        da_out(k).start()

    @within(s_x, s_y)
    def _():
        _ep_residual(conv(i - s_x, True), gb_ref, dx_ref)

    @within(s_y, s_y + (th - LAST) // 2)
    def _():
        _ep_residual(conv(i - s_y, False), xb_ref, y_ref)


def _main(nh, nw, cnt, z, z0, z1, g, gt, gh, x, xh, w1, w2, st, a):
    th, tw, c = x.shape
    nt, nb, half = 9, th // 2, c // 2
    (_, s_z, _, _, s_x, s_y, end), _, _ = _plan(nt, nb)
    full = _whole(th + 2, 1, c, pipeline_mode=pl.Buffered(1))
    one = _whole(8, c)

    def blocks(first, count=nb):
        return pl.BlockSpec((2, tw, c), lambda i: (lax.rem(jnp.minimum(jnp.maximum(i - first, 0), count - 1), nb), 0, 0))

    dma = pltpu.SemaphoreType.DMA
    img16, img32 = jax.ShapeDtypeStruct((th, tw, c), BF16), jax.ShapeDtypeStruct((th, tw, c), F32)
    side, edge, hrow = pltpu.VMEM((th + 2, 1, c), F32), pltpu.VMEM((th, 1, c), F32), pltpu.VMEM((2, tw, c), BF16)
    n = nh * nw - 1
    return pl.pallas_call(
        functools.partial(_main_kernel, nh, nw, cnt), grid=(end,),
        out_shape=[jax.ShapeDtypeStruct((th - LAST, tw, c), BF16), img16, jax.ShapeDtypeStruct((8, c), F32), img32, img16, jax.ShapeDtypeStruct((2 * nt * c, c), F32)]
        + [jax.ShapeDtypeStruct(h.shape, h.dtype) for h in gh],
        in_specs=[ANY] * 6 + [full, full, ANY, ANY, full, full, ANY, ANY, one, blocks(s_y, (th - LAST) // 2), blocks(s_x), blocks(s_z, 2 * nb)],
        out_specs=[blocks(s_y, (th - LAST) // 2), blocks(s_x), one] + [ANY] * 6,
        scratch_shapes=[pltpu.VMEM((th + 2, tw, 3 * c), BF16), pltpu.VMEM((c, th * tw), BF16), pltpu.VMEM((nt, c, c), BF16),
                        pltpu.VMEM((2, half, c), F32), pltpu.VMEM((nt, half, c), F32), pltpu.VMEM((2, half, c), F32),
                        pltpu.VMEM((nt, 2, c // 8, c), F32), pltpu.VMEM((nt, 2, c // 16, c), F32),
                        hrow, side, side, hrow, side, side, edge, edge, pltpu.VMEM((2, 2, tw, c), F32), pltpu.VMEM((2, 2, tw, c), BF16),
                        pltpu.VMEM((8, c), F32), pltpu.VMEM((n, 8, c), F32), pltpu.VMEM((c, c), BF16),
                        dma((3,)), dma, dma, dma((10, 2 * nt)), dma((10, 2 * nt)), dma((2, 2 * nt)), dma((8,)), dma((8,)), dma((8,)), dma((8,)), dma((n,)), dma((n,)), dma((3, 2))],
        compiler_params=pltpu.CompilerParams(dimension_semantics=("arbitrary",), vmem_limit_bytes=VMEM_LIMIT, collective_id=5, has_side_effects=True),
        name="main",
    )(z, z0, z1, g, gt, *gh, x, *xh, w1.reshape(nt, c, c), w2.reshape(nt, c, c), st, x, g, a)


def _finish_kernel(z_ref, rows_ref, cl_ref, cr_ref, w_ref, xb_ref, y0_ref, dx0_ref, d1_ref, d2_ref, y_ref, dx_ref, dw1_ref, dw2_ref,
                   p, wb, yb, psem, wsem, ysem, csem):
    i = pl.program_id(0)
    steps = pl.num_programs(0)
    th, tw, c = z_ref.shape
    r0 = th - LAST
    wait = steps - LAST
    n = y0_ref.shape[0]
    cps = [pltpu.make_async_copy(z_ref.at[r0 - 1:], p.at[:LAST + 1, :, c:2 * c], psem.at[0]),
           pltpu.make_async_copy(rows_ref.at[1], p.at[LAST + 1, :, c:2 * c], psem.at[1]), pltpu.make_async_copy(w_ref, wb, wsem)]
    ycopy = pltpu.make_async_copy(y0_ref, y_ref.at[pl.ds(i * n, n)], csem)

    def yout(k):
        return pltpu.make_async_copy(yb.at[lax.rem(k, 2)], y_ref.at[r0 + k], ysem.at[lax.rem(k, 2)])

    @pl.when(i == 0)
    def _():
        for cp in cps:
            cp.start()

    @pl.when(i == wait)
    def _():
        for cp in cps:
            cp.wait()
        _shift_patches(p, cl_ref, cr_ref, r0)

    @pl.when(i < wait)
    def _():
        ycopy.start()

    for src, dst in ((dx0_ref, dx_ref), (d1_ref, dw1_ref), (d2_ref, dw2_ref)):
        dst[...] = src[...]

    @pl.when(i < wait)
    def _():
        ycopy.wait()

    @pl.when(i >= wait)
    def _():
        k = i - wait

        @pl.when(k > 1)
        def _():
            yout(k - 2).wait()

        acc = None
        for a in range(3):
            d = jnp.dot(p[k + a], wb[a], preferred_element_type=F32)
            acc = d if acc is None else acc + d
        yb[lax.rem(k, 2)] = (acc + xb_ref[0].astype(F32)).astype(BF16)
        yout(k).start()

    @pl.when(i == steps - 1)
    def _():
        yout(LAST - 2).wait()
        yout(LAST - 1).wait()


def _finish(z, zh, w, x, y0, dx0, d):
    th, tw, c = x.shape
    steps = th // 2
    rows = d.shape[0] // th
    wshape = (3, 3 * c, c)
    dma = pltpu.SemaphoreType.DMA
    full = _whole(th + 2, 1, c)

    def part(k):
        return pl.BlockSpec((rows, c), lambda i: (i + k, 0))

    def img(n, at=lambda i: i):
        return pl.BlockSpec((n, tw, c), lambda i: (at(i), 0, 0))

    wait = steps - LAST
    y0_spec, x_spec = img((th - LAST) // wait, lambda i: jnp.minimum(i, wait - 1)), img(1, lambda i: th - LAST + jnp.maximum(i - wait, 0))

    wout = jax.ShapeDtypeStruct((d.shape[0] // 2, c), F32)
    iout = jax.ShapeDtypeStruct((th, tw, c), BF16)
    return pl.pallas_call(
        _finish_kernel, grid=(steps,), out_shape=[iout, iout, wout, wout],
        in_specs=[ANY, ANY, full, full, ANY, x_spec, y0_spec, img(2), part(steps), part(0)], out_specs=[ANY, img(2), part(0), part(0)],
        scratch_shapes=[pltpu.VMEM((LAST + 2, tw, 3 * c), BF16), pltpu.VMEM(wshape, BF16), pltpu.VMEM((2, tw, c), BF16), dma((2,)), dma, dma((2,)), dma],
        compiler_params=pltpu.CompilerParams(dimension_semantics=("arbitrary",), vmem_limit_bytes=VMEM_LIMIT), name="finish",
    )(z, *zh, w.reshape(wshape), x, y0, dx0, d, d)


def solution(mesh):
    nh, nw = mesh.shape["h"], mesh.shape["w"]
    mesh3 = Mesh(mesh.devices.reshape(nw, nh // 2, 2), ("w", "x", "c"))
    tile = P(None, ("x", "c"), "w", None)

    def body(x, w1, gamma, beta, w2, g):
        _, th, tw, c = x.shape
        x, g = x[0], g[0]
        cnt = float(th * nh * tw * nw * (c // GROUPS))
        rb = 2
        blk = pl.BlockSpec((rb, tw, c), lambda i: (i, 0, 0))
        small = _whole(8, c)
        img16 = jax.ShapeDtypeStruct((th, tw, c), BF16)
        par = jnp.concatenate([jnp.zeros((2, c), F32), gamma[None], beta[None], jnp.zeros((4, c), F32)])

        edge = jax.ShapeDtypeStruct((th, 1, c), F32)
        eblk = pl.BlockSpec((rb, 1, c), lambda i: (i, 0, 0))

        def edges(u):
            return u[:, 0:1, :].astype(F32), u[:, tw - 1:, :].astype(F32)

        gt, a, st, *halos = _conv(nh, nw, cnt, x, edges(x), g, edges(g), w1, par)
        xh, gh = halos[:3], halos[3:]
        z, *ze = pl.pallas_call(_z_kernel, grid=(th // rb,), out_shape=[img16, edge, edge], in_specs=[blk, small], out_specs=[blk, eblk, eblk], name="act")(a, st)
        y, dx, t, _, _, d, *zh = _main(nh, nw, cnt, z, *ze, g, gt, gh, x, xh, w1, w2, st, a)
        y, dx, dw1, dw2 = _finish(z, zh, w2, x, y, dx, d)
        return y[None], dx[None], dw1.reshape(w1.shape), dw2.reshape(w2.shape), t[0], t[1]

    return jax.shard_map(body, mesh=mesh3, in_specs=(tile, P(), P(), P(), P(), tile), out_specs=(tile, tile, P(), P(), P(), P()), check_vma=False)
```

```python
import functools

import jax
import jax.numpy as jnp
from jax import lax
from jax.experimental import pallas as pl
from jax.experimental.pallas import tpu as pltpu
from jax.sharding import Mesh
from jax.sharding import PartitionSpec as P

GROUPS = 32
EPS = 1e-5
F32 = jnp.float32
BF16 = jnp.bfloat16
MESH = pl.DeviceIdType.MESH
VMEM_LIMIT = 67043328
ANY = pl.BlockSpec(memory_space=pl.ANY)
VM = pl.BlockSpec(memory_space=pltpu.VMEM)
LAST = 8
GELU_C = 0.7978845608028654
GELU_A = 0.044715


def _whole(*shape, **kw):
    return pl.BlockSpec(shape, lambda i: (0,) * len(shape), **kw)


def _gelu_parts(n):
    n2 = n * n
    t = jnp.tanh(GELU_C * (n + GELU_A * n * n2))
    return n2, t


def _gelu(n):
    _, t = _gelu_parts(n)
    return 0.5 * n * (1.0 + t)


def _gelu_grad(n):
    n2, t = _gelu_parts(n)
    return 0.5 * (1.0 + t) + 0.5 * n * (1.0 - t * t) * (GELU_C * (1.0 + 3.0 * GELU_A * n2))


def _exchange(nh, nw, u, first, last, rows, cl, cr, send, recv):
    th = u.shape[0]
    w = lax.axis_index("w")
    h = lax.axis_index("x") * 2 + lax.axis_index("c")
    dirs = [(dh, dw) for dh in (-1, 0, 1) for dw in (-1, 0, 1) if (dh, dw) != (0, 0)]

    def dev(dh, dw):
        hh = h + dh
        return (w + dw, hh // 2, hh % 2)

    def has(dh, dw):
        ok = None
        for cond in ([h > 0] if dh < 0 else [h < nh - 1] if dh > 0 else []) + ([w > 0] if dw < 0 else [w < nw - 1] if dw > 0 else []):
            ok = cond if ok is None else jnp.logical_and(ok, cond)
        return ok

    def landing(dh, dw):
        side = cr if dw < 0 else cl
        if dw == 0:
            return rows, 1 if dh < 0 else 0
        if dh == 0:
            return side, slice(1, th + 1)
        return side, th + 1 if dh < 0 else 0

    def copy(i, dh, dw):
        r = 0 if dh < 0 else th - 1
        edge = first if dw < 0 else last
        src = u.at[r] if dw == 0 else edge if dh == 0 else edge.at[r]
        ref, at = landing(dh, dw)
        return pltpu.make_async_remote_copy(src_ref=src, dst_ref=ref.at[at], send_sem=send.at[i], recv_sem=recv.at[i],
                                            device_id=dev(dh, dw), device_id_type=MESH)

    def start():
        for i, (dh, dw) in enumerate(dirs):
            @pl.when(has(dh, dw))
            def _(i=i, dh=dh, dw=dw):
                copy(i, dh, dw).start()

    def finish():
        for i, (dh, dw) in enumerate(dirs):
            @pl.when(jnp.logical_not(has(-dh, -dw)))
            def _(dh=dh, dw=dw):
                ref, at = landing(dh, dw)
                ref[at] = jnp.zeros(ref.at[at].shape, ref.dtype)

            @pl.when(has(dh, dw))
            def _(i=i, dh=dh, dw=dw):
                copy(i, dh, dw).wait_send()

            @pl.when(has(-dh, -dw))
            def _(i=i, dh=dh, dw=dw):
                copy(i, dh, dw).wait_recv()

    return start, finish


def _peers(nh, nw):
    n = nh * nw
    me = lax.axis_index("w") * nh + lax.axis_index("x") * 2 + lax.axis_index("c")

    def dev(j):
        hh = lax.rem(j, nh)
        return (lax.div(j, nh), lax.div(hh, 2), lax.rem(hh, 2))

    return me, [dev(lax.rem(me + k, n)) for k in range(1, n)]


def _meet(peers):
    barrier = pltpu.get_barrier_semaphore()
    for d in peers:
        pl.semaphore_signal(barrier, inc=1, device_id=d, device_id_type=MESH)
    pl.semaphore_wait(barrier, len(peers))


def _sum_devices(me, peers, mine, buf, send, recv):
    copies = [pltpu.make_async_remote_copy(src_ref=mine, dst_ref=buf.at[k], send_sem=send.at[k], recv_sem=recv.at[k],
                                           device_id=d, device_id_type=MESH) for k, d in enumerate(peers)]
    for cp in copies:
        cp.start()
    for cp in copies:
        cp.wait()
    n = len(peers) + 1
    vals = [mine[...]] + [buf[k] for k in range(n - 1)]
    total = 0.0
    for j in range(n):
        off = lax.rem(me - j + n, n)
        total = total + sum(jnp.where(off == k, v, 0.0) for k, v in enumerate(vals))
    return total


def _fill_same(same):
    c = same.shape[0]
    gi, gj = [jnp.floor((lax.broadcasted_iota(jnp.int32, (c, c), d).astype(F32) + 0.5) * (GROUPS / c)) for d in range(2)]
    same[...] = jnp.where(gi == gj, 1.0, 0.0).astype(BF16)


def _group_means(v, same, cnt):
    hi = v.astype(BF16)
    rest = v - hi.astype(F32)
    mid = rest.astype(BF16)
    lo = (rest - mid.astype(F32)).astype(BF16)
    return sum(jnp.dot(x, same[...], preferred_element_type=F32) for x in (lo, mid, hi)) / cnt


def _shift_patches(p, cl_ref, cr_ref, r0=0):
    n, tw, c3 = p.shape
    c = c3 // 3
    ck = 128

    def row(r, _):
        idx = lax.broadcasted_iota(jnp.int32, (tw, ck), 0)
        for k in range(c // ck):
            f = p[r, :, c + k * ck:c + (k + 1) * ck].astype(F32)
            lo = cl_ref[r0 + r, :, k * ck:(k + 1) * ck]
            hi = cr_ref[r0 + r, :, k * ck:(k + 1) * ck]
            p[r, :, k * ck:(k + 1) * ck] = jnp.where(idx == 0, lo, pltpu.roll(f, 1, 0)).astype(BF16)
            p[r, :, 2 * c + k * ck:2 * c + (k + 1) * ck] = jnp.where(idx == tw - 1, hi, pltpu.roll(f, tw - 1, 0)).astype(BF16)
        return 0

    lax.fori_loop(0, n, row, 0)


def _transposed(v):
    return v.reshape(v.shape[0] * v.shape[1], v.shape[2]).T


def _put_rows(p, ref):
    th, c = p.shape[0] - 2, ref.shape[2]
    for k in range(2):
        p[k * (th + 1), :, c:2 * c] = ref[k]


def _conv_kernel(nh, nw, cnt, x_ref, x0_ref, x1_ref, g_ref, g0_ref, g1_ref, w_ref, par_ref, gb_ref, gt_ref, a_ref, st_ref, *refs):
    handed, (p, wb, *halo), (sacc, sbuf, same, psem, wsem, hsend, hrecv, ssend, srecv) = refs[:6], refs[6:14], refs[14:]
    i = pl.program_id(0)
    th, tw, c = x_ref.shape
    me, peers = _peers(nh, nw)
    last = th // 2
    x_start, x_finish = _exchange(nh, nw, x_ref, x0_ref, x1_ref, *halo[:3], hsend.at[0], hrecv.at[0])
    g_start, g_finish = _exchange(nh, nw, g_ref, g0_ref, g1_ref, *halo[3:], hsend.at[1], hrecv.at[1])

    @pl.when(i == 0)
    def _():
        xc = pltpu.make_async_copy(x_ref, p.at[1:th + 1, :, c:2 * c], psem)
        wc = pltpu.make_async_copy(w_ref, wb, wsem)
        xc.start()
        wc.start()
        _meet(peers)
        x_start()
        g_start()
        _fill_same(same)
        sacc[...] = jnp.zeros_like(sacc)
        x_finish()
        xc.wait()
        _put_rows(p, halo[0])
        _shift_patches(p, halo[1], halo[2])
        wc.wait()

    @pl.when(i < last)
    def _():
        gt_ref[...] = _transposed(gb_ref[...])
        acc = None
        for a in range(3):
            d = jnp.dot(p[pl.ds(i * 2 + a, 2)].reshape(2 * tw, 3 * c), wb[a], preferred_element_type=F32)
            acc = d if acc is None else acc + d
        a16 = acc.astype(BF16)
        a_ref[...] = a16.reshape(a_ref.shape)
        v = a16.astype(F32)
        row = lax.broadcasted_iota(jnp.int32, sacc.shape, 0)
        sacc[...] += jnp.where(row == 0, v.sum(0, keepdims=True), jnp.where(row == 1, (v * v).sum(0, keepdims=True), 0.0))

    @pl.when(i == last)
    def _():
        g_finish()
        for dst, src in zip(handed, halo):
            dst[...] = src[...]
        m = _group_means(_sum_devices(me, peers, sacc, sbuf, ssend, srecv), same, cnt)
        mean = m[0:1]
        row = lax.broadcasted_iota(jnp.int32, m.shape, 0)
        st_ref[...] = jnp.where(row == 0, mean, jnp.where(row == 1, lax.rsqrt(m[1:2] - mean * mean + EPS), par_ref[...]))


def _conv(nh, nw, cnt, x, xe, g, ge, w, par):
    th, tw, c = x.shape
    n, last = nh * nw - 1, th // 2 - 1
    wshape = (3, 3 * c, c)
    one = _whole(8, c)
    dma = pltpu.SemaphoreType.DMA
    halo = [(2, tw, c), (th + 2, 1, c), (th + 2, 1, c)] * 2
    types = [BF16, F32, F32] * 2
    blk = pl.BlockSpec((2, tw, c), lambda i: (jnp.minimum(i, last), 0, 0))
    return pl.pallas_call(
        functools.partial(_conv_kernel, nh, nw, cnt), grid=(th // 2 + 1,),
        out_shape=[jax.ShapeDtypeStruct((c, th * tw), BF16), jax.ShapeDtypeStruct((th, tw, c), BF16), jax.ShapeDtypeStruct((8, c), F32)]
        + [jax.ShapeDtypeStruct(h, t) for h, t in zip(halo, types)],
        in_specs=[ANY] * 7 + [one, blk], out_specs=[pl.BlockSpec((c, 2 * tw), lambda i: (0, jnp.minimum(i, last))), blk, one] + [_whole(*h) for h in halo],
        scratch_shapes=[pltpu.VMEM((th + 2, tw, 3 * c), BF16), pltpu.VMEM(wshape, BF16)] + [pltpu.VMEM(h, t) for h, t in zip(halo, types)]
        + [pltpu.VMEM((8, c), F32), pltpu.VMEM((n, 8, c), F32), pltpu.VMEM((c, c), BF16), dma, dma, dma((2, 8)), dma((2, 8)), dma((n,)), dma((n,))],
        compiler_params=pltpu.CompilerParams(dimension_semantics=("arbitrary",), vmem_limit_bytes=VMEM_LIMIT, collective_id=1, has_side_effects=True),
        name="conv1",
    )(x, *xe, g, *ge, w.reshape(wshape), par, g)


def _ep_residual(acc, r_ref, o_ref):
    o_ref[...] = (acc + r_ref[...].astype(F32).reshape(acc.shape)).astype(BF16).reshape(o_ref.shape)


def _params(st_ref):
    st = st_ref[...]
    return [st[k:k + 1] for k in range(4)]


def _edges(v, first_ref, last_ref):
    first_ref[...] = v[:, 0:1, :]
    last_ref[...] = v[:, v.shape[1] - 1:, :]


def _z_kernel(a_ref, st_ref, z_ref, first_ref, last_ref):
    mean, rstd, gamma, beta = _params(st_ref)
    xhat = (a_ref[...].astype(F32) - mean) * rstd
    z = _gelu(xhat * gamma + beta).astype(BF16)
    z_ref[...] = z
    _edges(z.astype(F32), first_ref, last_ref)


def _plan(nt, nb):
    starts = [0]
    for n in (nt, nb, nb, nt, nb, nb):
        starts.append(starts[-1] + n)
    late = [*range(2, 9), *range(10, 15, 2), *range(16, 25)]
    return starts, [*range(2, 11), *range(12, 17), 18, 20, 23, 25] + [starts[3] + s for s in late], 18


def _main_kernel(nh, nw, cnt, z_ref, z0_ref, z1_ref, g_ref, gt_ref, grows, gcl, gcr, x_ref, xrows, xcl, xcr, w1_ref, w2_ref, st_ref, xb_ref, gb_ref, ab_ref,
                 y_ref, dx_ref, t_ref, dn_ref, da_ref, dw_ref, hrows, hcl, hcr,
                 p, vt, wb, dsend, hown, recv0, recv1, recv2, zrows, zcl, zcr, arows, acl, acr, e0, e1, dnb, dab, sacc, sbuf, same,
                 psem, wsem, vsem, send, recv, lsem, zsend, zrecv, asend, arecv, ssend, srecv, dsem):
    i = pl.program_id(0)
    th, tw, c = x_ref.shape
    nt, nb = w1_ref.shape[0], th // 2
    (_, s_z, s_a, s_w, s_x, s_y, _), ticks, second = _plan(nt, nb)
    half, q, e, sub = c // 2, c // 4, c // 8, c // 16
    wi, xi, ci = lax.axis_index("w"), lax.axis_index("x"), lax.axis_index("c")
    mate, xn, yn = (wi, xi, 1 - ci), (wi, 1 - xi, ci), (1 - wi, xi, ci)
    pa, pb = xi * e, q + wi * e
    fa, fb = pa + wi * sub, pb + xi * sub
    me, peers = _peers(nh, nw)

    def slot(t):
        return jnp.where(t < nt, t, t - second)

    def sem_of(t):
        return jnp.where(t < nt, t, t - second + nt)

    def rows(start, n):
        return pl.ds(pl.multiple_of(start, 8), n)

    def rc(stage, t, src, dst, dev):
        return pltpu.make_async_remote_copy(src_ref=src, dst_ref=dst, send_sem=send.at[stage, sem_of(t)], recv_sem=recv.at[stage, sem_of(t)],
                                            device_id=dev, device_id_type=MESH)

    def tap(k):
        return lax.rem(2 * lax.rem(k, 3) + 1, 3), lax.rem(2 * lax.div(k, 3) + 1, 3)

    def base(t):
        a, b = tap(slot(t))
        return (jnp.where(t < nt, 0, nt) + a * 3 + b) * c + ci * half

    def s0(t):
        return [rc(0, t, dsend.at[lax.rem(slot(t), 2)], recv0.at[lax.rem(slot(t), 2)], mate)]

    def s1(t):
        return [rc(1, t, hown.at[slot(t), rows((1 - xi) * e, e)], recv1.at[slot(t), 0], xn),
                rc(2, t, hown.at[slot(t), rows(q + (1 - wi) * e, e)], recv1.at[slot(t), 1], yn)]

    def s2(t):
        return [rc(3, t, hown.at[slot(t), rows(pa + (1 - wi) * sub, sub)], recv2.at[slot(t), 0], yn),
                rc(4, t, hown.at[slot(t), rows(pb + (1 - xi) * sub, sub)], recv2.at[slot(t), 1], xn)]

    def s3(t):
        return [rc(5, t, hown.at[slot(t), rows(fa, sub)], dw_ref.at[rows(base(t) + fa, sub)], yn),
                rc(6, t, hown.at[slot(t), rows(fb, sub)], dw_ref.at[rows(base(t) + fb, sub)], xn)]

    def keep(t):
        return [pltpu.make_async_copy(hown.at[slot(t), rows(fa, sub)], dw_ref.at[rows(base(t) + fa, sub)], lsem.at[0, sem_of(t)]),
                pltpu.make_async_copy(hown.at[slot(t), rows(fb, sub)], dw_ref.at[rows(base(t) + fb, sub)], lsem.at[1, sem_of(t)])]

    def s4(t):
        return [rc(7, t, dw_ref.at[rows(base(t) + pa, e)], dw_ref.at[rows(base(t) + pa, e)], xn),
                rc(8, t, dw_ref.at[rows(base(t) + pb, e)], dw_ref.at[rows(base(t) + pb, e)], yn)]

    def s5(t):
        return [rc(9, t, dw_ref.at[rows(base(t), half)], dw_ref.at[rows(base(t), half)], mate)]

    def start(cps):
        for cp in cps:
            cp.start()

    def when_chunk(j, stages, f):
        for first, lag in ((0, 3), (second, 2)):
            t = j - stages * lag

            @pl.when(jnp.logical_and(t >= first, t < first + nt))
            def _(t=t):
                f(t)

    def tick(j):
        def t2(t):
            for cp in s1(t):
                cp.wait_recv()
            hown[slot(t), rows(pa, e), :] += recv1[slot(t), 0]
            hown[slot(t), rows(pb, e), :] += recv1[slot(t), 1]

        def t3(t):
            for cp in s2(t):
                cp.wait_recv()
            hown[slot(t), rows(fa, sub), :] += recv2[slot(t), 0]
            hown[slot(t), rows(fb, sub), :] += recv2[slot(t), 1]

        def t4(t):
            for cp in s3(t):
                cp.wait_recv()
            for cp in keep(t):
                cp.wait()
            for cp in s1(t) + s2(t) + s3(t):
                cp.wait_send()
            start(s4(t))

        def t5(t):
            for cp in s4(t):
                cp.wait_recv()
            start(s5(t))

        def t6(t):
            for cp in s5(t):
                cp.wait_recv()
            for cp in s4(t) + s5(t):
                cp.wait_send()

        when_chunk(j, 0, lambda t: start(s1(t)))
        for stages, f in enumerate((t2, t3, t4, t5)):
            when_chunk(j, stages + 1, f)
        when_chunk(j, 1, lambda t: start(s2(t)))
        when_chunk(j, 2, lambda t: start(s3(t) + keep(t)))
        when_chunk(j, 5, t6)

    z_start, z_finish = _exchange(nh, nw, z_ref, z0_ref, z1_ref, zrows, zcl, zcr, zsend, zrecv)
    a_start, a_finish = _exchange(nh, nw, da_ref, e0, e1, arows, acl, acr, asend, arecv)

    def wcp(ref):
        return pltpu.make_async_copy(ref, wb, wsem)

    def middle(src):
        return pltpu.make_async_copy(src, p.at[1:th + 1, :, c:2 * c], psem.at[2])

    def given(ref):
        return [pltpu.make_async_copy(ref.at[k], p.at[k * (th + 1), :, c:2 * c], psem.at[k]) for k in range(2)]

    def run(cps):
        start(cps)
        for cp in cps:
            cp.wait()

    def at(step):
        return pl.when(i == step)

    def within(a, b):
        return pl.when(jnp.logical_and(i >= a, i < b))

    @at(0)
    def _():
        cps = [pltpu.make_async_copy(gt_ref, vt, vsem), middle(z_ref)]
        start(cps)
        _meet(peers)
        z_start()
        wcp(w2_ref).start()
        _fill_same(same)
        sacc[...] = jnp.zeros_like(sacc)
        for cp in cps:
            cp.wait()

    @at(1)
    def _():
        z_finish()
        _put_rows(p, zrows)

    @at(3)
    def _():
        run([pltpu.make_async_copy(src, dst, psem.at[k]) for k, (src, dst) in enumerate(zip((zrows, zcl, zcr), (hrows, hcl, hcr)))])
        _shift_patches(p, zcl, zcr)

    @at(s_z)
    def _():
        run([middle(g_ref)] + given(grows))
        _shift_patches(p, gcl, gcr)
        wcp(w2_ref).wait()

    @at(s_w + 3)
    def _():
        _shift_patches(p, xcl, xcr)

    def dn_out(k):
        return pltpu.make_async_copy(dnb.at[lax.rem(k, 2)], dn_ref.at[pl.ds(2 * k, 2)], dsem.at[0, lax.rem(k, 2)])

    def dn_in(k):
        return pltpu.make_async_copy(dn_ref.at[pl.ds(2 * k, 2)], dnb.at[lax.rem(k, 2)], dsem.at[1, lax.rem(k, 2)])

    def da_out(k):
        return pltpu.make_async_copy(dab.at[lax.rem(k, 2)], da_ref.at[pl.ds(2 * k, 2)], dsem.at[2, lax.rem(k, 2)])

    @at(s_a)
    def _():
        for k in range(2):
            dn_out(nb - 2 + k).wait()
        start([dn_in(0), dn_in(1), middle(x_ref), wcp(w1_ref)] + given(xrows))
        total = _sum_devices(me, peers, sacc, sbuf, ssend, srecv)
        u = _group_means(total * _params(st_ref)[2], same, cnt)
        row = lax.broadcasted_iota(jnp.int32, total.shape, 0)
        t_ref[...] = jnp.where(row < 2, total, jnp.where(row == 2, u[0:1], u[1:2]))

    @at(s_w)
    def _():
        for k in range(2):
            da_out(nb - 2 + k).wait()
        a_start()
        for cp in [middle(x_ref)] + given(xrows):
            cp.wait()

    @at(s_x)
    def _():
        start([middle(da_ref)])
        a_finish()
        middle(da_ref).wait()
        _put_rows(p, arows)
        _shift_patches(p, acl, acr)
        wcp(w1_ref).wait()

    @at(s_y)
    def _():
        cps = [middle(z_ref), wcp(w2_ref)]
        start(cps)
        _put_rows(p, zrows)
        for cp in cps:
            cp.wait()
        _shift_patches(p, zcl, zcr)

    later = i >= s_w
    step = jnp.where(later, i - s_w, i)
    chunk0 = jnp.where(later, second, 0)

    @pl.when(jnp.logical_and(step >= 2, step < nt + 2))
    def _():
        k = step - 2
        for cp in s0(chunk0 + k):
            cp.wait()
        hown[k] += recv0[lax.rem(k, 2)]

    @pl.when(jnp.logical_and(step >= 1, step < nt + 1))
    def _():
        start(s0(chunk0 + step - 1))

    j = jnp.int32(-1)
    now = jnp.int32(0)
    for s in ticks:
        j = j + jnp.where(i >= s, 1, 0)
        now = now + jnp.where(i == s, 1, 0)

    @pl.when(now > 0)
    def _():
        tick(j)

    @pl.when(step < nt)
    def _():
        a, b = tap(step)
        rhs = p[pl.ds(a, th), :, pl.ds(pl.multiple_of(b * c, 128), c)].reshape(th * tw, c)
        d = jnp.dot(vt[...], rhs, preferred_element_type=F32).T
        hown[step] = jnp.where(ci == 0, d[:half], d[half:])
        dsend[lax.rem(step, 2)] = jnp.where(ci == 0, d[half:], d[:half])

    def conv(ib, transposed):
        acc = None
        for a in range(3):
            lhs = p[pl.ds(ib * 2 + a, 2)].reshape(2 * tw, 3 * c)
            if transposed:
                k = nt - 1 - 3 * a
                rhs = jnp.concatenate([wb[k], wb[k - 1], wb[k - 2]], axis=1)
                d = lax.dot_general(lhs, rhs, (((1,), (1,)), ((), ())), preferred_element_type=F32)
            else:
                d = jnp.dot(lhs, wb[3 * a:3 * a + 3].reshape(3 * c, c), preferred_element_type=F32)
            acc = d if acc is None else acc + d
        return acc

    @within(s_z, s_a)
    def _():
        k = i - s_z

        @pl.when(k > 1)
        def _():
            dn_out(k - 2).wait()

        acc = conv(k, True)
        mean, rstd, gamma, beta = _params(st_ref)
        xhat = (ab_ref[...].astype(F32).reshape(acc.shape) - mean) * rstd
        dn = acc * _gelu_grad(xhat * gamma + beta)
        dnb[lax.rem(k, 2)] = dn.reshape(2, tw, c)
        dn_out(k).start()
        row = lax.broadcasted_iota(jnp.int32, sacc.shape, 0)
        sacc[...] += jnp.where(row == 0, (dn * xhat).sum(0, keepdims=True), jnp.where(row == 1, dn.sum(0, keepdims=True), 0.0))

    @within(s_a, s_w)
    def _():
        k = i - s_a

        @pl.when(k > 1)
        def _():
            da_out(k - 2).wait()

        dn_in(k).wait()
        mean, rstd, gamma, _ = _params(st_ref)
        _, _, u0, u1 = _params(t_ref)
        xhat = (ab_ref[...].astype(F32) - mean) * rstd
        da = (rstd * (dnb[lax.rem(k, 2)] * gamma - u1 - xhat * u0)).astype(BF16)
        dab[lax.rem(k, 2)] = da

        @pl.when(k + 2 < nb)
        def _():
            dn_in(k + 2).start()

        _edges(da.astype(F32), e0.at[pl.ds(2 * k, 2)], e1.at[pl.ds(2 * k, 2)])
        vt[:, pl.ds(pl.multiple_of(2 * k * tw, 2 * tw), 2 * tw)] = _transposed(da)
        da_out(k).start()

    @within(s_x, s_y)
    def _():
        _ep_residual(conv(i - s_x, True), gb_ref, dx_ref)

    @within(s_y, s_y + (th - LAST) // 2)
    def _():
        _ep_residual(conv(i - s_y, False), xb_ref, y_ref)


def _main(nh, nw, cnt, z, z0, z1, g, gt, gh, x, xh, w1, w2, st, a):
    th, tw, c = x.shape
    nt, nb, half = 9, th // 2, c // 2
    (_, s_z, _, _, s_x, s_y, end), _, _ = _plan(nt, nb)
    full = _whole(th + 2, 1, c, pipeline_mode=pl.Buffered(1))
    one = _whole(8, c)

    def blocks(first, count=nb):
        return pl.BlockSpec((2, tw, c), lambda i: (lax.rem(jnp.minimum(jnp.maximum(i - first, 0), count - 1), nb), 0, 0))

    dma = pltpu.SemaphoreType.DMA
    img16, img32 = jax.ShapeDtypeStruct((th, tw, c), BF16), jax.ShapeDtypeStruct((th, tw, c), F32)
    side, edge, hrow = pltpu.VMEM((th + 2, 1, c), F32), pltpu.VMEM((th, 1, c), F32), pltpu.VMEM((2, tw, c), BF16)
    n = nh * nw - 1
    return pl.pallas_call(
        functools.partial(_main_kernel, nh, nw, cnt), grid=(end,),
        out_shape=[jax.ShapeDtypeStruct((th - LAST, tw, c), BF16), img16, jax.ShapeDtypeStruct((8, c), F32), img32, img16, jax.ShapeDtypeStruct((2 * nt * c, c), F32)]
        + [jax.ShapeDtypeStruct(h.shape, h.dtype) for h in gh],
        in_specs=[ANY] * 6 + [full, full, ANY, ANY, full, full, ANY, ANY, one, blocks(s_y, (th - LAST) // 2), blocks(s_x), blocks(s_z, 2 * nb)],
        out_specs=[blocks(s_y, (th - LAST) // 2), blocks(s_x), one] + [ANY] * 6,
        scratch_shapes=[pltpu.VMEM((th + 2, tw, 3 * c), BF16), pltpu.VMEM((c, th * tw), BF16), pltpu.VMEM((nt, c, c), BF16),
                        pltpu.VMEM((2, half, c), F32), pltpu.VMEM((nt, half, c), F32), pltpu.VMEM((2, half, c), F32),
                        pltpu.VMEM((nt, 2, c // 8, c), F32), pltpu.VMEM((nt, 2, c // 16, c), F32),
                        hrow, side, side, hrow, side, side, edge, edge, pltpu.VMEM((2, 2, tw, c), F32), pltpu.VMEM((2, 2, tw, c), BF16),
                        pltpu.VMEM((8, c), F32), pltpu.VMEM((n, 8, c), F32), pltpu.VMEM((c, c), BF16),
                        dma((3,)), dma, dma, dma((10, 2 * nt)), dma((10, 2 * nt)), dma((2, 2 * nt)), dma((8,)), dma((8,)), dma((8,)), dma((8,)), dma((n,)), dma((n,)), dma((3, 2))],
        compiler_params=pltpu.CompilerParams(dimension_semantics=("arbitrary",), vmem_limit_bytes=VMEM_LIMIT, collective_id=5, has_side_effects=True),
        name="main",
    )(z, z0, z1, g, gt, *gh, x, *xh, w1.reshape(nt, c, c), w2.reshape(nt, c, c), st, x, g, a)


def _finish_kernel(z_ref, rows_ref, cl_ref, cr_ref, w_ref, xb_ref, y0_ref, dx0_ref, d1_ref, d2_ref, y_ref, dx_ref, dw1_ref, dw2_ref,
                   p, wb, yb, psem, wsem, ysem, csem):
    i = pl.program_id(0)
    steps = pl.num_programs(0)
    th, tw, c = z_ref.shape
    r0 = th - LAST
    n = LAST + 1

    def yout(k):
        return pltpu.make_async_copy(yb.at[lax.rem(k, 2)], y_ref.at[r0 + k], ysem.at[lax.rem(k, 2)])

    ycopy = pltpu.make_async_copy(y0_ref.at[0], y_ref.at[i], csem)
    ycopy.start()

    @pl.when(i == 0)
    def _():
        cps = [pltpu.make_async_copy(z_ref.at[r0 - 1:], p.at[:n, :, c:2 * c], psem.at[0]),
               pltpu.make_async_copy(rows_ref.at[1], p.at[n, :, c:2 * c], psem.at[1])]
        wc = pltpu.make_async_copy(w_ref, wb, wsem)
        for cp in cps + [wc]:
            cp.start()
        for cp in cps:
            cp.wait()
        _shift_patches(p, cl_ref, cr_ref, r0)
        wc.wait()

    @pl.when(i > 1)
    def _():
        yout(i - 2).wait()

    for src, dst in ((dx0_ref, dx_ref), (d1_ref, dw1_ref), (d2_ref, dw2_ref)):
        dst[...] = src[...]
    acc = None
    for a in range(3):
        d = jnp.dot(p[i + a], wb[a], preferred_element_type=F32)
        acc = d if acc is None else acc + d
    yb[lax.rem(i, 2)] = (acc + xb_ref[0].astype(F32)).astype(BF16)
    yout(i).start()
    ycopy.wait()

    @pl.when(i == steps - 1)
    def _():
        yout(i - 1).wait()
        yout(i).wait()


def _finish(z, zh, w, x, y0, dx0, d):
    th, tw, c = x.shape
    steps = LAST
    rows = d.shape[0] // 2 // steps
    wshape = (3, 3 * c, c)
    dma = pltpu.SemaphoreType.DMA
    full = _whole(th + 2, 1, c)

    def part(k):
        return pl.BlockSpec((rows, c), lambda i: (i + k, 0))

    def img(n, k=0):
        return pl.BlockSpec((n, tw, c), lambda i: (i + k, 0, 0))

    wout = jax.ShapeDtypeStruct((d.shape[0] // 2, c), F32)
    iout = jax.ShapeDtypeStruct((th, tw, c), BF16)
    return pl.pallas_call(
        _finish_kernel, grid=(steps,), out_shape=[iout, iout, wout, wout],
        in_specs=[ANY, ANY, full, full, ANY, img(1, steps), img(1), img(2), part(steps), part(0)], out_specs=[ANY, img(2), part(0), part(0)],
        scratch_shapes=[pltpu.VMEM((steps + 2, tw, 3 * c), BF16), pltpu.VMEM(wshape, BF16), pltpu.VMEM((2, tw, c), BF16), dma((2,)), dma, dma((2,)), dma],
        compiler_params=pltpu.CompilerParams(dimension_semantics=("arbitrary",), vmem_limit_bytes=VMEM_LIMIT), name="finish",
    )(z, *zh, w.reshape(wshape), x, y0, dx0, d, d)


def solution(mesh):
    nh, nw = mesh.shape["h"], mesh.shape["w"]
    mesh3 = Mesh(mesh.devices.reshape(nw, nh // 2, 2), ("w", "x", "c"))
    tile = P(None, ("x", "c"), "w", None)

    def body(x, w1, gamma, beta, w2, g):
        _, th, tw, c = x.shape
        x, g = x[0], g[0]
        cnt = float(th * nh * tw * nw * (c // GROUPS))
        rb = 2
        blk = pl.BlockSpec((rb, tw, c), lambda i: (i, 0, 0))
        small = _whole(8, c)
        img16 = jax.ShapeDtypeStruct((th, tw, c), BF16)
        par = jnp.concatenate([jnp.zeros((2, c), F32), gamma[None], beta[None], jnp.zeros((4, c), F32)])

        edge = jax.ShapeDtypeStruct((th, 1, c), F32)
        eblk = pl.BlockSpec((rb, 1, c), lambda i: (i, 0, 0))

        def edges(u):
            return u[:, 0:1, :].astype(F32), u[:, tw - 1:, :].astype(F32)

        gt, a, st, *halos = _conv(nh, nw, cnt, x, edges(x), g, edges(g), w1, par)
        xh, gh = halos[:3], halos[3:]
        z, *ze = pl.pallas_call(_z_kernel, grid=(th // rb,), out_shape=[img16, edge, edge], in_specs=[blk, small], out_specs=[blk, eblk, eblk], name="act")(a, st)
        y, dx, t, _, _, d, *zh = _main(nh, nw, cnt, z, *ze, g, gt, gh, x, xh, w1, w2, st, a)
        y, dx, dw1, dw2 = _finish(z, zh, w2, x, y, dx, d)
        return y[None], dx[None], dw1.reshape(w1.shape), dw2.reshape(w2.shape), t[0], t[1]

    return jax.shard_map(body, mesh=mesh3, in_specs=(tile, P(), P(), P(), P(), tile), out_specs=(tile, tile, P(), P(), P(), P()), check_vma=False)
```

```python
import functools

import jax
import jax.numpy as jnp
from jax import lax
from jax.experimental import pallas as pl
from jax.experimental.pallas import tpu as pltpu
from jax.sharding import Mesh
from jax.sharding import PartitionSpec as P

GROUPS = 32
EPS = 1e-5
F32 = jnp.float32
BF16 = jnp.bfloat16
MESH = pl.DeviceIdType.MESH
VMEM_LIMIT = 67043328
ANY = pl.BlockSpec(memory_space=pl.ANY)
VM = pl.BlockSpec(memory_space=pltpu.VMEM)
LAST = 8
GELU_C = 0.7978845608028654
GELU_A = 0.044715


def _whole(*shape, **kw):
    return pl.BlockSpec(shape, lambda i: (0,) * len(shape), **kw)


def _gelu_parts(n):
    n2 = n * n
    t = jnp.tanh(GELU_C * (n + GELU_A * n * n2))
    return n2, t


def _gelu(n):
    _, t = _gelu_parts(n)
    return 0.5 * n * (1.0 + t)


def _gelu_grad(n):
    n2, t = _gelu_parts(n)
    return 0.5 * (1.0 + t) + 0.5 * n * (1.0 - t * t) * (GELU_C * (1.0 + 3.0 * GELU_A * n2))


def _exchange(nh, nw, u, first, last, rows, cl, cr, send, recv):
    th = u.shape[0]
    w = lax.axis_index("w")
    h = lax.axis_index("x") * 2 + lax.axis_index("c")
    dirs = [(dh, dw) for dh in (-1, 0, 1) for dw in (-1, 0, 1) if (dh, dw) != (0, 0)]

    def dev(dh, dw):
        hh = h + dh
        return (w + dw, hh // 2, hh % 2)

    def has(dh, dw):
        ok = None
        for cond in ([h > 0] if dh < 0 else [h < nh - 1] if dh > 0 else []) + ([w > 0] if dw < 0 else [w < nw - 1] if dw > 0 else []):
            ok = cond if ok is None else jnp.logical_and(ok, cond)
        return ok

    def landing(dh, dw):
        side = cr if dw < 0 else cl
        if dw == 0:
            return rows, 1 if dh < 0 else 0
        if dh == 0:
            return side, slice(1, th + 1)
        return side, th + 1 if dh < 0 else 0

    def copy(i, dh, dw):
        r = 0 if dh < 0 else th - 1
        edge = first if dw < 0 else last
        src = u.at[r] if dw == 0 else edge if dh == 0 else edge.at[r]
        ref, at = landing(dh, dw)
        return pltpu.make_async_remote_copy(src_ref=src, dst_ref=ref.at[at], send_sem=send.at[i], recv_sem=recv.at[i],
                                            device_id=dev(dh, dw), device_id_type=MESH)

    def start():
        for i, (dh, dw) in enumerate(dirs):
            @pl.when(has(dh, dw))
            def _(i=i, dh=dh, dw=dw):
                copy(i, dh, dw).start()

    def finish():
        for i, (dh, dw) in enumerate(dirs):
            @pl.when(jnp.logical_not(has(-dh, -dw)))
            def _(dh=dh, dw=dw):
                ref, at = landing(dh, dw)
                ref[at] = jnp.zeros(ref.at[at].shape, ref.dtype)

            @pl.when(has(dh, dw))
            def _(i=i, dh=dh, dw=dw):
                copy(i, dh, dw).wait_send()

            @pl.when(has(-dh, -dw))
            def _(i=i, dh=dh, dw=dw):
                copy(i, dh, dw).wait_recv()

    return start, finish


def _peers(nh, nw):
    n = nh * nw
    me = lax.axis_index("w") * nh + lax.axis_index("x") * 2 + lax.axis_index("c")

    def dev(j):
        hh = lax.rem(j, nh)
        return (lax.div(j, nh), lax.div(hh, 2), lax.rem(hh, 2))

    return me, [dev(lax.rem(me + k, n)) for k in range(1, n)]


def _meet(peers):
    barrier = pltpu.get_barrier_semaphore()
    for d in peers:
        pl.semaphore_signal(barrier, inc=1, device_id=d, device_id_type=MESH)
    pl.semaphore_wait(barrier, len(peers))


def _sum_devices(me, peers, mine, buf, send, recv):
    copies = [pltpu.make_async_remote_copy(src_ref=mine, dst_ref=buf.at[k], send_sem=send.at[k], recv_sem=recv.at[k],
                                           device_id=d, device_id_type=MESH) for k, d in enumerate(peers)]
    for cp in copies:
        cp.start()
    for cp in copies:
        cp.wait()
    n = len(peers) + 1
    vals = [mine[...]] + [buf[k] for k in range(n - 1)]
    total = 0.0
    for j in range(n):
        off = lax.rem(me - j + n, n)
        total = total + sum(jnp.where(off == k, v, 0.0) for k, v in enumerate(vals))
    return total


def _fill_same(same):
    c = same.shape[0]
    gi, gj = [jnp.floor((lax.broadcasted_iota(jnp.int32, (c, c), d).astype(F32) + 0.5) * (GROUPS / c)) for d in range(2)]
    same[...] = jnp.where(gi == gj, 1.0, 0.0).astype(BF16)


def _group_means(v, same, cnt):
    hi = v.astype(BF16)
    rest = v - hi.astype(F32)
    mid = rest.astype(BF16)
    lo = (rest - mid.astype(F32)).astype(BF16)
    return sum(jnp.dot(x, same[...], preferred_element_type=F32) for x in (lo, mid, hi)) / cnt


def _shift_patches(p, cl_ref, cr_ref, r0=0):
    n, tw, c3 = p.shape
    c = c3 // 3
    ck = 128

    def row(r, _):
        idx = lax.broadcasted_iota(jnp.int32, (tw, ck), 0)
        for k in range(c // ck):
            f = p[r, :, c + k * ck:c + (k + 1) * ck].astype(F32)
            lo = cl_ref[r0 + r, :, k * ck:(k + 1) * ck]
            hi = cr_ref[r0 + r, :, k * ck:(k + 1) * ck]
            p[r, :, k * ck:(k + 1) * ck] = jnp.where(idx == 0, lo, pltpu.roll(f, 1, 0)).astype(BF16)
            p[r, :, 2 * c + k * ck:2 * c + (k + 1) * ck] = jnp.where(idx == tw - 1, hi, pltpu.roll(f, tw - 1, 0)).astype(BF16)
        return 0

    lax.fori_loop(0, n, row, 0)


def _transposed(v):
    return v.reshape(v.shape[0] * v.shape[1], v.shape[2]).T


def _put_rows(p, ref):
    th, c = p.shape[0] - 2, ref.shape[2]
    for k in range(2):
        p[k * (th + 1), :, c:2 * c] = ref[k]


def _conv_kernel(nh, nw, cnt, x_ref, x0_ref, x1_ref, g_ref, g0_ref, g1_ref, w_ref, par_ref, gb_ref, gt_ref, a_ref, st_ref, *refs):
    handed, (p, wb, *halo), (sacc, sbuf, same, psem, wsem, hsend, hrecv, ssend, srecv) = refs[:6], refs[6:14], refs[14:]
    i = pl.program_id(0)
    th, tw, c = x_ref.shape
    me, peers = _peers(nh, nw)
    last = th // 2
    x_start, x_finish = _exchange(nh, nw, x_ref, x0_ref, x1_ref, *halo[:3], hsend.at[0], hrecv.at[0])
    g_start, g_finish = _exchange(nh, nw, g_ref, g0_ref, g1_ref, *halo[3:], hsend.at[1], hrecv.at[1])

    @pl.when(i == 0)
    def _():
        xc = pltpu.make_async_copy(x_ref, p.at[1:th + 1, :, c:2 * c], psem)
        wc = pltpu.make_async_copy(w_ref, wb, wsem)
        xc.start()
        wc.start()
        _meet(peers)
        x_start()
        g_start()
        _fill_same(same)
        sacc[...] = jnp.zeros_like(sacc)
        x_finish()
        xc.wait()
        _put_rows(p, halo[0])
        _shift_patches(p, halo[1], halo[2])
        wc.wait()

    @pl.when(i < last)
    def _():
        gt_ref[...] = _transposed(gb_ref[...])
        acc = None
        for a in range(3):
            d = jnp.dot(p[pl.ds(i * 2 + a, 2)].reshape(2 * tw, 3 * c), wb[a], preferred_element_type=F32)
            acc = d if acc is None else acc + d
        a16 = acc.astype(BF16)
        a_ref[...] = a16.reshape(a_ref.shape)
        v = a16.astype(F32)
        row = lax.broadcasted_iota(jnp.int32, sacc.shape, 0)
        sacc[...] += jnp.where(row == 0, v.sum(0, keepdims=True), jnp.where(row == 1, (v * v).sum(0, keepdims=True), 0.0))

    @pl.when(i == last)
    def _():
        g_finish()
        for dst, src in zip(handed, halo):
            dst[...] = src[...]
        m = _group_means(_sum_devices(me, peers, sacc, sbuf, ssend, srecv), same, cnt)
        mean = m[0:1]
        row = lax.broadcasted_iota(jnp.int32, m.shape, 0)
        st_ref[...] = jnp.where(row == 0, mean, jnp.where(row == 1, lax.rsqrt(m[1:2] - mean * mean + EPS), par_ref[...]))


def _conv(nh, nw, cnt, x, xe, g, ge, w, par):
    th, tw, c = x.shape
    n, last = nh * nw - 1, th // 2 - 1
    wshape = (3, 3 * c, c)
    one = _whole(8, c)
    dma = pltpu.SemaphoreType.DMA
    halo = [(2, tw, c), (th + 2, 1, c), (th + 2, 1, c)] * 2
    types = [BF16, F32, F32] * 2
    blk = pl.BlockSpec((2, tw, c), lambda i: (jnp.minimum(i, last), 0, 0))
    return pl.pallas_call(
        functools.partial(_conv_kernel, nh, nw, cnt), grid=(th // 2 + 1,),
        out_shape=[jax.ShapeDtypeStruct((c, th * tw), BF16), jax.ShapeDtypeStruct((th, tw, c), BF16), jax.ShapeDtypeStruct((8, c), F32)]
        + [jax.ShapeDtypeStruct(h, t) for h, t in zip(halo, types)],
        in_specs=[ANY] * 7 + [one, blk], out_specs=[pl.BlockSpec((c, 2 * tw), lambda i: (0, jnp.minimum(i, last))), blk, one] + [_whole(*h) for h in halo],
        scratch_shapes=[pltpu.VMEM((th + 2, tw, 3 * c), BF16), pltpu.VMEM(wshape, BF16)] + [pltpu.VMEM(h, t) for h, t in zip(halo, types)]
        + [pltpu.VMEM((8, c), F32), pltpu.VMEM((n, 8, c), F32), pltpu.VMEM((c, c), BF16), dma, dma, dma((2, 8)), dma((2, 8)), dma((n,)), dma((n,))],
        compiler_params=pltpu.CompilerParams(dimension_semantics=("arbitrary",), vmem_limit_bytes=VMEM_LIMIT, collective_id=1, has_side_effects=True),
        name="conv1",
    )(x, *xe, g, *ge, w.reshape(wshape), par, g)


def _ep_residual(acc, r_ref, o_ref):
    o_ref[...] = (acc + r_ref[...].astype(F32).reshape(acc.shape)).astype(BF16).reshape(o_ref.shape)


def _params(st_ref):
    st = st_ref[...]
    return [st[k:k + 1] for k in range(4)]


def _edges(v, first_ref, last_ref):
    first_ref[...] = v[:, 0:1, :]
    last_ref[...] = v[:, v.shape[1] - 1:, :]


def _z_kernel(a_ref, st_ref, z_ref, first_ref, last_ref):
    mean, rstd, gamma, beta = _params(st_ref)
    xhat = (a_ref[...].astype(F32) - mean) * rstd
    z = _gelu(xhat * gamma + beta).astype(BF16)
    z_ref[...] = z
    _edges(z.astype(F32), first_ref, last_ref)


def _plan(nt, nb):
    starts = [0]
    for n in (nt, nb, nb, nt, nb, nb):
        starts.append(starts[-1] + n)
    late = [*range(2, 9), *range(10, 15, 2), *range(16, 25)]
    return starts, [*range(2, 10), 11, 13, 16, 17, 20, 24, 26] + [starts[3] + s for s in late], 15


def _main_kernel(nh, nw, cnt, z_ref, z0_ref, z1_ref, g_ref, gt_ref, grows, gcl, gcr, x_ref, xrows, xcl, xcr, w1_ref, w2_ref, st_ref, xb_ref, gb_ref, ab_ref,
                 y_ref, dx_ref, t_ref, dn_ref, da_ref, dw_ref, hrows, hcl, hcr,
                 p, vt, wb, dsend, hown, recv0, recv1, recv2, zrows, zcl, zcr, arows, acl, acr, e0, e1, dnb, dab, sacc, sbuf, same,
                 psem, wsem, vsem, send, recv, lsem, zsend, zrecv, asend, arecv, ssend, srecv, dsem):
    i = pl.program_id(0)
    th, tw, c = x_ref.shape
    nt, nb = w1_ref.shape[0], th // 2
    (_, s_z, s_a, s_w, s_x, s_y, _), ticks, second = _plan(nt, nb)
    half, q, e, sub = c // 2, c // 4, c // 8, c // 16
    wi, xi, ci = lax.axis_index("w"), lax.axis_index("x"), lax.axis_index("c")
    mate, xn, yn = (wi, xi, 1 - ci), (wi, 1 - xi, ci), (1 - wi, xi, ci)
    pa, pb = xi * e, q + wi * e
    fa, fb = pa + wi * sub, pb + xi * sub
    me, peers = _peers(nh, nw)

    def slot(t):
        return jnp.where(t < nt, t, t - second)

    def sem_of(t):
        return jnp.where(t < nt, t, t - second + nt)

    def rows(start, n):
        return pl.ds(pl.multiple_of(start, 8), n)

    def rc(stage, t, src, dst, dev):
        return pltpu.make_async_remote_copy(src_ref=src, dst_ref=dst, send_sem=send.at[stage, sem_of(t)], recv_sem=recv.at[stage, sem_of(t)],
                                            device_id=dev, device_id_type=MESH)

    def tap(k):
        return lax.rem(2 * lax.rem(k, 3) + 1, 3), lax.rem(2 * lax.div(k, 3) + 1, 3)

    def base(t):
        a, b = tap(slot(t))
        return (jnp.where(t < nt, 0, nt) + a * 3 + b) * c + ci * half

    def s0(t):
        return [rc(0, t, dsend.at[lax.rem(slot(t), 2)], recv0.at[lax.rem(slot(t), 2)], mate)]

    def s1(t):
        return [rc(1, t, hown.at[slot(t), rows((1 - xi) * e, e)], recv1.at[slot(t), 0], xn),
                rc(2, t, hown.at[slot(t), rows(q + (1 - wi) * e, e)], recv1.at[slot(t), 1], yn)]

    def s2(t):
        return [rc(3, t, hown.at[slot(t), rows(pa + (1 - wi) * sub, sub)], recv2.at[slot(t), 0], yn),
                rc(4, t, hown.at[slot(t), rows(pb + (1 - xi) * sub, sub)], recv2.at[slot(t), 1], xn)]

    def s3(t):
        return [rc(5, t, hown.at[slot(t), rows(fa, sub)], dw_ref.at[rows(base(t) + fa, sub)], yn),
                rc(6, t, hown.at[slot(t), rows(fb, sub)], dw_ref.at[rows(base(t) + fb, sub)], xn)]

    def keep(t):
        return [pltpu.make_async_copy(hown.at[slot(t), rows(fa, sub)], dw_ref.at[rows(base(t) + fa, sub)], lsem.at[0, sem_of(t)]),
                pltpu.make_async_copy(hown.at[slot(t), rows(fb, sub)], dw_ref.at[rows(base(t) + fb, sub)], lsem.at[1, sem_of(t)])]

    def s4(t):
        return [rc(7, t, dw_ref.at[rows(base(t) + pa, e)], dw_ref.at[rows(base(t) + pa, e)], xn),
                rc(8, t, dw_ref.at[rows(base(t) + pb, e)], dw_ref.at[rows(base(t) + pb, e)], yn)]

    def s5(t):
        return [rc(9, t, dw_ref.at[rows(base(t), half)], dw_ref.at[rows(base(t), half)], mate)]

    def start(cps):
        for cp in cps:
            cp.start()

    def when_chunk(j, stages, f):
        for first, lag in ((0, 2), (second, 2)):
            t = j - stages * lag

            @pl.when(jnp.logical_and(t >= first, t < first + nt))
            def _(t=t):
                f(t)

    def tick(j):
        def t2(t):
            for cp in s1(t):
                cp.wait_recv()
            hown[slot(t), rows(pa, e), :] += recv1[slot(t), 0]
            hown[slot(t), rows(pb, e), :] += recv1[slot(t), 1]

        def t3(t):
            for cp in s2(t):
                cp.wait_recv()
            hown[slot(t), rows(fa, sub), :] += recv2[slot(t), 0]
            hown[slot(t), rows(fb, sub), :] += recv2[slot(t), 1]

        def t4(t):
            for cp in s3(t):
                cp.wait_recv()
            for cp in keep(t):
                cp.wait()
            for cp in s1(t) + s2(t) + s3(t):
                cp.wait_send()
            start(s4(t))

        def t5(t):
            for cp in s4(t):
                cp.wait_recv()
            start(s5(t))

        def t6(t):
            for cp in s5(t):
                cp.wait_recv()
            for cp in s4(t) + s5(t):
                cp.wait_send()

        when_chunk(j, 0, lambda t: start(s1(t)))
        for stages, f in enumerate((t2, t3, t4, t5)):
            when_chunk(j, stages + 1, f)
        when_chunk(j, 1, lambda t: start(s2(t)))
        when_chunk(j, 2, lambda t: start(s3(t) + keep(t)))
        when_chunk(j, 5, t6)

    z_start, z_finish = _exchange(nh, nw, z_ref, z0_ref, z1_ref, zrows, zcl, zcr, zsend, zrecv)
    a_start, a_finish = _exchange(nh, nw, da_ref, e0, e1, arows, acl, acr, asend, arecv)

    def wcp(ref):
        return pltpu.make_async_copy(ref, wb, wsem)

    def middle(src):
        return pltpu.make_async_copy(src, p.at[1:th + 1, :, c:2 * c], psem.at[2])

    def given(ref):
        return [pltpu.make_async_copy(ref.at[k], p.at[k * (th + 1), :, c:2 * c], psem.at[k]) for k in range(2)]

    def run(cps):
        start(cps)
        for cp in cps:
            cp.wait()

    def at(step):
        return pl.when(i == step)

    def within(a, b):
        return pl.when(jnp.logical_and(i >= a, i < b))

    @at(0)
    def _():
        cps = [pltpu.make_async_copy(gt_ref, vt, vsem), middle(z_ref)]
        start(cps)
        _meet(peers)
        z_start()
        wcp(w2_ref).start()
        _fill_same(same)
        sacc[...] = jnp.zeros_like(sacc)
        for cp in cps:
            cp.wait()

    @at(1)
    def _():
        z_finish()
        _put_rows(p, zrows)

    @at(3)
    def _():
        run([pltpu.make_async_copy(src, dst, psem.at[k]) for k, (src, dst) in enumerate(zip((zrows, zcl, zcr), (hrows, hcl, hcr)))])
        _shift_patches(p, zcl, zcr)

    @at(s_z)
    def _():
        run([middle(g_ref)] + given(grows))
        _shift_patches(p, gcl, gcr)
        wcp(w2_ref).wait()

    @at(s_w + 3)
    def _():
        _shift_patches(p, xcl, xcr)

    def dn_out(k):
        return pltpu.make_async_copy(dnb.at[lax.rem(k, 2)], dn_ref.at[pl.ds(2 * k, 2)], dsem.at[0, lax.rem(k, 2)])

    def dn_in(k):
        return pltpu.make_async_copy(dn_ref.at[pl.ds(2 * k, 2)], dnb.at[lax.rem(k, 2)], dsem.at[1, lax.rem(k, 2)])

    def da_out(k):
        return pltpu.make_async_copy(dab.at[lax.rem(k, 2)], da_ref.at[pl.ds(2 * k, 2)], dsem.at[2, lax.rem(k, 2)])

    @at(s_a)
    def _():
        for k in range(2):
            dn_out(nb - 2 + k).wait()
        start([dn_in(0), dn_in(1), middle(x_ref), wcp(w1_ref)] + given(xrows))
        total = _sum_devices(me, peers, sacc, sbuf, ssend, srecv)
        u = _group_means(total * _params(st_ref)[2], same, cnt)
        row = lax.broadcasted_iota(jnp.int32, total.shape, 0)
        t_ref[...] = jnp.where(row < 2, total, jnp.where(row == 2, u[0:1], u[1:2]))

    @at(s_w)
    def _():
        for k in range(2):
            da_out(nb - 2 + k).wait()
        a_start()
        for cp in [middle(x_ref)] + given(xrows):
            cp.wait()

    @at(s_x)
    def _():
        start([middle(da_ref)])
        a_finish()
        middle(da_ref).wait()
        _put_rows(p, arows)
        _shift_patches(p, acl, acr)
        wcp(w1_ref).wait()

    @at(s_y)
    def _():
        cps = [middle(z_ref), wcp(w2_ref)]
        start(cps)
        _put_rows(p, zrows)
        for cp in cps:
            cp.wait()
        _shift_patches(p, zcl, zcr)

    later = i >= s_w
    step = jnp.where(later, i - s_w, i)
    chunk0 = jnp.where(later, second, 0)

    @pl.when(jnp.logical_and(step >= 2, step < nt + 2))
    def _():
        k = step - 2
        for cp in s0(chunk0 + k):
            cp.wait()
        hown[k] += recv0[lax.rem(k, 2)]

    @pl.when(jnp.logical_and(step >= 1, step < nt + 1))
    def _():
        start(s0(chunk0 + step - 1))

    j = jnp.int32(-1)
    now = jnp.int32(0)
    for s in ticks:
        j = j + jnp.where(i >= s, 1, 0)
        now = now + jnp.where(i == s, 1, 0)

    @pl.when(now > 0)
    def _():
        tick(j)

    @pl.when(step < nt)
    def _():
        a, b = tap(step)
        rhs = p[pl.ds(a, th), :, pl.ds(pl.multiple_of(b * c, 128), c)].reshape(th * tw, c)
        d = jnp.dot(vt[...], rhs, preferred_element_type=F32).T
        hown[step] = jnp.where(ci == 0, d[:half], d[half:])
        dsend[lax.rem(step, 2)] = jnp.where(ci == 0, d[half:], d[:half])

    def conv(ib, transposed):
        acc = None
        for a in range(3):
            lhs = p[pl.ds(ib * 2 + a, 2)].reshape(2 * tw, 3 * c)
            if transposed:
                k = nt - 1 - 3 * a
                rhs = jnp.concatenate([wb[k], wb[k - 1], wb[k - 2]], axis=1)
                d = lax.dot_general(lhs, rhs, (((1,), (1,)), ((), ())), preferred_element_type=F32)
            else:
                d = jnp.dot(lhs, wb[3 * a:3 * a + 3].reshape(3 * c, c), preferred_element_type=F32)
            acc = d if acc is None else acc + d
        return acc

    @within(s_z, s_a)
    def _():
        k = i - s_z

        @pl.when(k > 1)
        def _():
            dn_out(k - 2).wait()

        acc = conv(k, True)
        mean, rstd, gamma, beta = _params(st_ref)
        xhat = (ab_ref[...].astype(F32).reshape(acc.shape) - mean) * rstd
        dn = acc * _gelu_grad(xhat * gamma + beta)
        dnb[lax.rem(k, 2)] = dn.reshape(2, tw, c)
        dn_out(k).start()
        row = lax.broadcasted_iota(jnp.int32, sacc.shape, 0)
        sacc[...] += jnp.where(row == 0, (dn * xhat).sum(0, keepdims=True), jnp.where(row == 1, dn.sum(0, keepdims=True), 0.0))

    @within(s_a, s_w)
    def _():
        k = i - s_a

        @pl.when(k > 1)
        def _():
            da_out(k - 2).wait()

        dn_in(k).wait()
        mean, rstd, gamma, _ = _params(st_ref)
        _, _, u0, u1 = _params(t_ref)
        xhat = (ab_ref[...].astype(F32) - mean) * rstd
        da = (rstd * (dnb[lax.rem(k, 2)] * gamma - u1 - xhat * u0)).astype(BF16)
        dab[lax.rem(k, 2)] = da

        @pl.when(k + 2 < nb)
        def _():
            dn_in(k + 2).start()

        _edges(da.astype(F32), e0.at[pl.ds(2 * k, 2)], e1.at[pl.ds(2 * k, 2)])
        vt[:, pl.ds(pl.multiple_of(2 * k * tw, 2 * tw), 2 * tw)] = _transposed(da)
        da_out(k).start()

    @within(s_x, s_y)
    def _():
        _ep_residual(conv(i - s_x, True), gb_ref, dx_ref)

    @within(s_y, s_y + (th - LAST) // 2)
    def _():
        _ep_residual(conv(i - s_y, False), xb_ref, y_ref)


def _main(nh, nw, cnt, z, z0, z1, g, gt, gh, x, xh, w1, w2, st, a):
    th, tw, c = x.shape
    nt, nb, half = 9, th // 2, c // 2
    (_, s_z, _, _, s_x, s_y, end), _, _ = _plan(nt, nb)
    full = _whole(th + 2, 1, c, pipeline_mode=pl.Buffered(1))
    one = _whole(8, c)

    def blocks(first, count=nb):
        return pl.BlockSpec((2, tw, c), lambda i: (lax.rem(jnp.minimum(jnp.maximum(i - first, 0), count - 1), nb), 0, 0))

    dma = pltpu.SemaphoreType.DMA
    img16, img32 = jax.ShapeDtypeStruct((th, tw, c), BF16), jax.ShapeDtypeStruct((th, tw, c), F32)
    side, edge, hrow = pltpu.VMEM((th + 2, 1, c), F32), pltpu.VMEM((th, 1, c), F32), pltpu.VMEM((2, tw, c), BF16)
    n = nh * nw - 1
    return pl.pallas_call(
        functools.partial(_main_kernel, nh, nw, cnt), grid=(end,),
        out_shape=[jax.ShapeDtypeStruct((th - LAST, tw, c), BF16), img16, jax.ShapeDtypeStruct((8, c), F32), img32, img16, jax.ShapeDtypeStruct((2 * nt * c, c), F32)]
        + [jax.ShapeDtypeStruct(h.shape, h.dtype) for h in gh],
        in_specs=[ANY] * 6 + [full, full, ANY, ANY, full, full, ANY, ANY, one, blocks(s_y, (th - LAST) // 2), blocks(s_x), blocks(s_z, 2 * nb)],
        out_specs=[blocks(s_y, (th - LAST) // 2), blocks(s_x), one] + [ANY] * 6,
        scratch_shapes=[pltpu.VMEM((th + 2, tw, 3 * c), BF16), pltpu.VMEM((c, th * tw), BF16), pltpu.VMEM((nt, c, c), BF16),
                        pltpu.VMEM((2, half, c), F32), pltpu.VMEM((nt, half, c), F32), pltpu.VMEM((2, half, c), F32),
                        pltpu.VMEM((nt, 2, c // 8, c), F32), pltpu.VMEM((nt, 2, c // 16, c), F32),
                        hrow, side, side, hrow, side, side, edge, edge, pltpu.VMEM((2, 2, tw, c), F32), pltpu.VMEM((2, 2, tw, c), BF16),
                        pltpu.VMEM((8, c), F32), pltpu.VMEM((n, 8, c), F32), pltpu.VMEM((c, c), BF16),
                        dma((3,)), dma, dma, dma((10, 2 * nt)), dma((10, 2 * nt)), dma((2, 2 * nt)), dma((8,)), dma((8,)), dma((8,)), dma((8,)), dma((n,)), dma((n,)), dma((3, 2))],
        compiler_params=pltpu.CompilerParams(dimension_semantics=("arbitrary",), vmem_limit_bytes=VMEM_LIMIT, collective_id=5, has_side_effects=True),
        name="main",
    )(z, z0, z1, g, gt, *gh, x, *xh, w1.reshape(nt, c, c), w2.reshape(nt, c, c), st, x, g, a)


def _finish_kernel(z_ref, rows_ref, cl_ref, cr_ref, w_ref, xb_ref, y0_ref, dx0_ref, d1_ref, d2_ref, y_ref, dx_ref, dw1_ref, dw2_ref,
                   p, wb, yb, psem, wsem, ysem, csem):
    i = pl.program_id(0)
    steps = pl.num_programs(0)
    th, tw, c = z_ref.shape
    r0 = th - LAST
    n = LAST + 1

    def yout(k):
        return pltpu.make_async_copy(yb.at[lax.rem(k, 2)], y_ref.at[r0 + k], ysem.at[lax.rem(k, 2)])

    ycopy = pltpu.make_async_copy(y0_ref.at[0], y_ref.at[i], csem)
    ycopy.start()

    @pl.when(i == 0)
    def _():
        cps = [pltpu.make_async_copy(z_ref.at[r0 - 1:], p.at[:n, :, c:2 * c], psem.at[0]),
               pltpu.make_async_copy(rows_ref.at[1], p.at[n, :, c:2 * c], psem.at[1])]
        wc = pltpu.make_async_copy(w_ref, wb, wsem)
        for cp in cps + [wc]:
            cp.start()
        for cp in cps:
            cp.wait()
        _shift_patches(p, cl_ref, cr_ref, r0)
        wc.wait()

    @pl.when(i > 1)
    def _():
        yout(i - 2).wait()

    for src, dst in ((dx0_ref, dx_ref), (d1_ref, dw1_ref), (d2_ref, dw2_ref)):
        dst[...] = src[...]
    acc = None
    for a in range(3):
        d = jnp.dot(p[i + a], wb[a], preferred_element_type=F32)
        acc = d if acc is None else acc + d
    yb[lax.rem(i, 2)] = (acc + xb_ref[0].astype(F32)).astype(BF16)
    yout(i).start()
    ycopy.wait()

    @pl.when(i == steps - 1)
    def _():
        yout(i - 1).wait()
        yout(i).wait()


def _finish(z, zh, w, x, y0, dx0, d):
    th, tw, c = x.shape
    steps = LAST
    rows = d.shape[0] // 2 // steps
    wshape = (3, 3 * c, c)
    dma = pltpu.SemaphoreType.DMA
    full = _whole(th + 2, 1, c)

    def part(k):
        return pl.BlockSpec((rows, c), lambda i: (i + k, 0))

    def img(n, k=0):
        return pl.BlockSpec((n, tw, c), lambda i: (i + k, 0, 0))

    wout = jax.ShapeDtypeStruct((d.shape[0] // 2, c), F32)
    iout = jax.ShapeDtypeStruct((th, tw, c), BF16)
    return pl.pallas_call(
        _finish_kernel, grid=(steps,), out_shape=[iout, iout, wout, wout],
        in_specs=[ANY, ANY, full, full, ANY, img(1, steps), img(1), img(2), part(steps), part(0)], out_specs=[ANY, img(2), part(0), part(0)],
        scratch_shapes=[pltpu.VMEM((steps + 2, tw, 3 * c), BF16), pltpu.VMEM(wshape, BF16), pltpu.VMEM((2, tw, c), BF16), dma((2,)), dma, dma((2,)), dma],
        compiler_params=pltpu.CompilerParams(dimension_semantics=("arbitrary",), vmem_limit_bytes=VMEM_LIMIT), name="finish",
    )(z, *zh, w.reshape(wshape), x, y0, dx0, d, d)


def solution(mesh):
    nh, nw = mesh.shape["h"], mesh.shape["w"]
    mesh3 = Mesh(mesh.devices.reshape(nw, nh // 2, 2), ("w", "x", "c"))
    tile = P(None, ("x", "c"), "w", None)

    def body(x, w1, gamma, beta, w2, g):
        _, th, tw, c = x.shape
        x, g = x[0], g[0]
        cnt = float(th * nh * tw * nw * (c // GROUPS))
        rb = 2
        blk = pl.BlockSpec((rb, tw, c), lambda i: (i, 0, 0))
        small = _whole(8, c)
        img16 = jax.ShapeDtypeStruct((th, tw, c), BF16)
        par = jnp.concatenate([jnp.zeros((2, c), F32), gamma[None], beta[None], jnp.zeros((4, c), F32)])

        edge = jax.ShapeDtypeStruct((th, 1, c), F32)
        eblk = pl.BlockSpec((rb, 1, c), lambda i: (i, 0, 0))

        def edges(u):
            return u[:, 0:1, :].astype(F32), u[:, tw - 1:, :].astype(F32)

        gt, a, st, *halos = _conv(nh, nw, cnt, x, edges(x), g, edges(g), w1, par)
        xh, gh = halos[:3], halos[3:]
        z, *ze = pl.pallas_call(_z_kernel, grid=(th // rb,), out_shape=[img16, edge, edge], in_specs=[blk, small], out_specs=[blk, eblk, eblk], name="act")(a, st)
        y, dx, t, _, _, d, *zh = _main(nh, nw, cnt, z, *ze, g, gt, gh, x, xh, w1, w2, st, a)
        y, dx, dw1, dw2 = _finish(z, zh, w2, x, y, dx, d)
        return y[None], dx[None], dw1.reshape(w1.shape), dw2.reshape(w2.shape), t[0], t[1]

    return jax.shard_map(body, mesh=mesh3, in_specs=(tile, P(), P(), P(), P(), tile), out_specs=(tile, tile, P(), P(), P(), P()), check_vma=False)
```
